128 devices in a mesh: section: 4 (over x), chan: 32 (over y, z, core).
Axes of the slice: x: 4, y: 4, z: 4, core: 2. Of those that a mesh axis runs over, the one named last changes fastest.
Arguments:
- voltages: bfloat16 [2, 512, 524288], P(None, 'chan', 'section'), may hold values from -6 to 6
- usable: int32 [4096, 512], P(('section', 'chan')), may hold values 0 or 1
- auto_power: float32 [4096, 512], P(('section', 'chan')), may hold values from 0.5 to 4
Outputs:
- gains: float32 [2, 4096, 512], P(None, ('section', 'chan'))
The draws below stay inside these ranges and needn't reach their ends.
Inputs may be any that keep to these rules, and one draw needn't show every extreme that they name: 1 marks a feed as usable in that channel, 0 as flagged.
All inputs are finite; a program needn't handle non-finite values. No bound on the sum of `usable` on one device may be relied on, other than what follows from the above.
Results may differ from the reference program's by a relative error of at most 0.0046.
Values may be sent and summed in bfloat16 or wider, within the bound.
A program may use at most 256 MiB of HBM per device.

```python
import math
import jax
import jax.numpy as jnp
from jax import lax

FEEDS = 512
CHANNELS = 4096
TAPS = 4
ITERS = 5
SPECTRA = 128
SAMPLES = 524288
N_SECTION = 4
N_CHAN = 32


def with_ends(array, rng, low, top_value):
    longest = array.shape.index(max(array.shape))
    spots = []
    for shift in (0, 1):
        where = [jax.random.randint(jax.random.fold_in(rng, axis), (), 0, length) for axis, length in enumerate(array.shape)]
        where[longest] = (where[longest] + shift) % array.shape[longest]
        spots.append(tuple(where))
    return array.at[spots[0]].set(low).at[spots[1]].set(top_value)


def levels(own_key, dims, cuts, least, top_value):
    level = 1.0
    for axis_at, parts in cuts:
        steps = jax.random.uniform(jax.random.fold_in(jax.random.fold_in(own_key, 6), axis_at), (parts,), jnp.float32, least / len(cuts), top_value / len(cuts))
        level = level * jnp.repeat(jnp.exp(steps), dims[axis_at] // parts).reshape((-1,) + (1,) * (len(dims) - 1 - axis_at))
    return level


def normal_values(stream_key, dims, spread, bound, cuts=(), held_as=jnp.bfloat16):
    values = jax.random.normal(stream_key, dims, jnp.float32) * spread
    if len(cuts) > 0:
        values = levels(stream_key, dims, cuts, -0.22, 0.18) * values
    return jnp.clip(values, min=-bound, max=bound).astype(held_as)


def setup_inputs(seed: int = 0) -> dict:
    arg_keys = jax.random.split(jax.random.key(seed), 4)
    return {
        "voltages": normal_values(arg_keys[0], (2, FEEDS, SAMPLES), 1.0, 6.0, ((1, 32), (2, 4))),
        "usable": with_ends((jax.random.randint(arg_keys[1], (CHANNELS, FEEDS), 0, 8) < 7).astype(jnp.int32), jax.random.fold_in(arg_keys[1], 1), 0, 1),
        "auto_power": jnp.clip(jnp.exp(math.log(4.0) - 2.0794415 * jax.random.uniform(arg_keys[2], (CHANNELS, FEEDS), jnp.float32) ** levels(arg_keys[2], (CHANNELS, FEEDS), ((0, 128),), -0.2, 0.2)), 0.5, 4.0),
    }


def prototype(tap_count, channels):
    position = lax.iota(jnp.float32, tap_count * channels)
    offset = (position - 0.5 * tap_count * channels + 0.5) / channels
    window = 0.5 - 0.5 * jnp.cos(2.0 * jnp.pi * (position + 0.5) / (tap_count * channels))
    return (jnp.sin(jnp.pi * offset) / (jnp.pi * offset) * window).reshape(tap_count, channels)

def channelize(group_volts):
    samples = group_volts.astype(jnp.float32)
    count_here = samples.shape[1]
    leading = jnp.zeros((2, count_here, (TAPS - 1) * CHANNELS), jnp.float32)
    extended = jnp.concatenate([leading, samples], axis=2)
    extended = extended.reshape(2, count_here, SPECTRA + TAPS - 1, CHANNELS)
    coeffs = prototype(TAPS, CHANNELS)
    filtered = coeffs[0] * extended[:, :, 0:SPECTRA]
    for tap_index in range(1, TAPS):
        filtered = filtered + coeffs[tap_index] * extended[:, :, tap_index:tap_index + SPECTRA]
    spectrum = jnp.fft.fft(lax.complex(filtered[0], filtered[1]), axis=-1) / math.sqrt(CHANNELS)
    return jnp.stack([jnp.real(spectrum), jnp.imag(spectrum)]).astype(jnp.bfloat16)

def solve_group(pieces):
    spectra, usable, auto_power = pieces
    values = spectra.astype(jnp.float32)
    rotated = jnp.stack([values[:, 1], -values[:, 0]], axis=1)
    stacked = jnp.stack([values, rotated], axis=1)
    visibility = jnp.einsum('cqpit,cpjt->cqij', stacked, values, precision=lax.Precision.HIGHEST)
    weight = usable.astype(jnp.float32)
    diagonal = jnp.diagonal(visibility[:, 0], axis1=1, axis2=2)
    shifted = SPECTRA * auto_power - diagonal
    current = jnp.stack([weight, jnp.zeros_like(weight)], axis=1)
    result = current
    length = jnp.ones((weight.shape[0],), jnp.float32)
    for iteration in range(ITERS):
        masked = weight[:, None] * current
        product = jnp.einsum('cqij,cpj->cqpi', visibility, masked, precision=lax.Precision.HIGHEST)
        real_part = product[:, 0, 0] - product[:, 1, 1]
        imag_part = product[:, 0, 1] + product[:, 1, 0]
        result = weight[:, None] * (jnp.stack([real_part, imag_part], axis=1) + shifted[:, None] * masked)
        length = jnp.sqrt(lax.optimization_barrier(jnp.sum(result * result, axis=(1, 2))) + 1e-06)
        current = result / length[:, None, None]
    return result / jnp.sqrt(length)[:, None, None]

def reference(voltages, usable, auto_power):
    per_group = FEEDS // N_CHAN
    grouped = voltages.reshape(2, N_CHAN, per_group, SAMPLES).transpose(1, 0, 2, 3)
    spectra = lax.map(channelize, grouped)
    spectra = spectra.transpose(1, 0, 2, 3, 4).reshape(2, FEEDS, SPECTRA, CHANNELS)
    group_size = math.gcd(CHANNELS // (N_SECTION * N_CHAN), 8)
    group_count = CHANNELS // group_size
    ordered = spectra.reshape(2, FEEDS, SPECTRA, group_count, group_size).transpose(3, 4, 0, 1, 2)
    gains = lax.map(solve_group, (ordered, usable.reshape(group_count, group_size, FEEDS), auto_power.reshape(group_count, group_size, FEEDS)))
    return gains.reshape(CHANNELS, 2, FEEDS).transpose(1, 0, 2)
```

```python
import functools
import math

import jax
import jax.numpy as jnp
import numpy as np
from jax import lax
from jax.experimental import pallas as pl
from jax.experimental.pallas import tpu as pltpu
from jax.sharding import PartitionSpec as P

CHANNELS = 4096
TAPS = 4
ITERS = 5
EPSILON = 1e-06

COARSE = 32
FINE = 128
FEEDS_HERE = 16
BLOCKS_HERE = 32
GROUP = 8
GROUPS = BLOCKS_HERE // GROUP
PACKS = 4
OWNERS = 128
SECTIONS = 4
FEED_SETS = 32
STRIDE = 17
MARGIN = (TAPS - 1) * CHANNELS
LENGTH = BLOCKS_HERE * CHANNELS


def tables():
    position = np.arange(TAPS * CHANNELS, dtype=np.float64)
    offset = (position - 0.5 * TAPS * CHANNELS + 0.5) / CHANNELS
    window = 0.5 - 0.5 * np.cos(2.0 * np.pi * (position + 0.5) / (TAPS * CHANNELS))
    taps = np.sin(np.pi * offset) / (np.pi * offset) * window
    taps = taps.reshape(TAPS * COARSE, FINE).astype(np.float32)
    angle = 2.0 * np.pi * np.outer(np.arange(COARSE), np.arange(FINE)) / CHANNELS
    twiddle = np.concatenate([np.cos(angle), np.sin(angle)], axis=0).astype(np.float32)
    angle = 2.0 * np.pi * (np.outer(np.arange(FINE), np.arange(FINE)) % FINE) / FINE
    cosine = np.cos(angle) / math.sqrt(CHANNELS)
    sine = np.sin(angle) / math.sqrt(CHANNELS)
    fine = np.block([[cosine, sine], [-sine, cosine]]).astype(np.float32)
    lane = np.arange(128)
    share = (lane[:, None] // FEEDS_HERE == lane[None, :] // FEEDS_HERE).astype(np.float32)
    return taps, twiddle, fine, share


def butterfly_4(x):
    (ar, ai), (br, bi), (cr, ci), (dr, di) = x
    pr, pi, qr, qi = ar + cr, ai + ci, ar - cr, ai - ci
    sr, si, tr, ti = br + dr, bi + di, br - dr, bi - di
    return [(pr + sr, pi + si), (qr + ti, qi - tr), (pr - sr, pi - si), (qr - ti, qi + tr)]


def turn(x, eighths_of_32):
    n = eighths_of_32 % 32
    re, im = x
    if n == 0:
        return re, im
    if n == 8:
        return im, -re
    if n == 16:
        return -re, -im
    if n == 24:
        return -im, re
    cosine, sine = math.cos(2 * math.pi * n / 32), math.sin(2 * math.pi * n / 32)
    if n % 4 == 0:
        h = math.sqrt(0.5)
        if n == 4:
            return (re + im) * h, (im - re) * h
        if n == 12:
            return (im - re) * h, (re + im) * -h
    return re * cosine + im * sine, im * cosine - re * sine


def butterfly_8(x):
    even = butterfly_4([x[0], x[2], x[4], x[6]])
    odd = butterfly_4([x[1], x[3], x[5], x[7]])
    low, high = [], []
    for k in range(4):
        er, ei = even[k]
        tr, ti = turn(odd[k], 4 * k)
        low.append((er + tr, ei + ti))
        high.append((er - tr, ei - ti))
    return low + high


def first_transform(block, ext, taps, halfway):
    start = block * CHANNELS
    for low in range(8):
        points = []
        for high in range(4):
            tile = 8 * high + low
            pair = []
            for part in range(2):
                total = None
                for tap in range(TAPS):
                    at = pl.multiple_of(start + (tap * COARSE + tile) * FINE, FINE)
                    row = tap * COARSE + tile
                    term = taps[row : row + 1, :] * ext[part, :, pl.ds(at, FINE)].astype(jnp.float32)
                    total = term if total is None else total + term
                pair.append(total)
            points.append(tuple(pair))
        for q, point in enumerate(butterfly_4(points)):
            re, im = turn(point, low * q)
            halfway[q, low, 0] = re
            halfway[q, low, 1] = im


def second_transform(twiddle, halfway, upper, lower):
    for q1 in range(4):
        points = [(halfway[q1, low, 0], halfway[q1, low, 1]) for low in range(8)]
        for q2, (re, im) in enumerate(butterfly_8(points)):
            q = q1 + 4 * q2
            if q > 0:
                cosine = twiddle[q : q + 1, :]
                sine = twiddle[COARSE + q : COARSE + q + 1, :]
                re, im = re * cosine + im * sine, im * cosine - re * sine
            for part, value in enumerate((re, im)):
                high = value.astype(jnp.bfloat16)
                low = (value - high.astype(jnp.float32)).astype(jnp.bfloat16)
                rows = slice(q * FEEDS_HERE, (q + 1) * FEEDS_HERE)
                lanes = slice(part * FINE, (part + 1) * FINE)
                upper[rows, lanes] = high
                lower[rows, lanes] = low


def fine_transform(at, fine_upper, fine_lower, upper, lower, stage):
    dims = (((1,), (1,)), ((), ()))
    for half in range(2):
        rows = slice(half * 256, (half + 1) * 256)
        high = upper[rows, :]
        low = lower[rows, :]
        out = lax.dot_general(fine_upper[...], high, dims, preferred_element_type=jnp.float32)
        out += lax.dot_general(fine_lower[...], high, dims, preferred_element_type=jnp.float32)
        out += lax.dot_general(fine_upper[...], low, dims, preferred_element_type=jnp.float32)
        for pack in range(2):
            for part in range(2):
                piece = out[part * FINE : (part + 1) * FINE, pack * 128 : (pack + 1) * 128]
                stage[2 * half + pack, pl.ds(part * GROUP + at, OWNERS, stride=STRIDE), :] = piece


def channel_kernel(
    volt, tail, taps, twiddle, fine_upper, fine_lower, out, ext, halfway, upper, lower, stage, loads
):
    def load(group):
        width = GROUP * CHANNELS
        return pltpu.make_async_copy(
            volt.at[:, :, pl.ds(group * width, width)],
            ext.at[:, :, pl.ds(MARGIN + group * width, width)],
            loads.at[1 + group],
        )

    group = pl.program_id(0)
    edge = pltpu.make_async_copy(tail, ext.at[:, :, pl.ds(0, MARGIN)], loads.at[0])

    @pl.when(group == 0)
    def _():
        edge.start()
        for g in range(GROUPS):
            load(g).start()
        edge.wait()

    for g in range(GROUPS):

        @pl.when(group == g)
        def _():
            load(g).wait()

    def step(at, carry):
        first_transform(group * GROUP + at, ext, taps, halfway)
        second_transform(twiddle, halfway, upper, lower)
        fine_transform(at, fine_upper, fine_lower, upper, lower, stage)
        return carry

    lax.fori_loop(0, GROUP, step, 0)

    def emit(owner, carry):
        for pack in range(PACKS):
            out[owner, pack, 0] = stage[pack, pl.ds(owner * STRIDE, 16), :].astype(jnp.bfloat16)
        return carry

    lax.fori_loop(0, OWNERS, emit, 0, unroll=8)


def channelize(voltages, history):
    taps, twiddle, fine, _ = tables()
    upper = fine.astype(jnp.bfloat16)
    lower = (fine - upper.astype(np.float32)).astype(jnp.bfloat16)
    whole = lambda shape: pl.BlockSpec(shape, lambda g: (0,) * len(shape))
    return pl.pallas_call(
        channel_kernel,
        grid=(GROUPS,),
        out_shape=jax.ShapeDtypeStruct((OWNERS, PACKS, GROUPS, 16, 128), jnp.bfloat16),
        in_specs=[
            pl.BlockSpec(memory_space=pl.ANY),
            pl.BlockSpec(memory_space=pl.ANY),
            whole((TAPS * COARSE, FINE)),
            whole((2 * COARSE, FINE)),
            whole((256, 256)),
            whole((256, 256)),
        ],
        out_specs=pl.BlockSpec((OWNERS, PACKS, 1, 16, 128), lambda g: (0, 0, g, 0, 0)),
        scratch_shapes=[
            pltpu.VMEM((2, FEEDS_HERE, MARGIN + LENGTH), jnp.bfloat16),
            pltpu.VMEM((4, 8, 2, FEEDS_HERE, FINE), jnp.float32),
            pltpu.VMEM((COARSE * FEEDS_HERE, 256), jnp.bfloat16),
            pltpu.VMEM((COARSE * FEEDS_HERE, 256), jnp.bfloat16),
            pltpu.VMEM((PACKS, OWNERS * STRIDE + 8, 128), jnp.float32),
            pltpu.SemaphoreType.DMA((1 + GROUPS,)),
        ],
        compiler_params=pltpu.CompilerParams(
            dimension_semantics=("arbitrary",), vmem_limit_bytes=56 * 1024 * 1024
        ),
        cost_estimate=pl.CostEstimate(flops=10**10, bytes_accessed=2 * 10**7, transcendentals=0),
    )(voltages, history, taps, twiddle, upper, lower)


def solve_kernel(spectra, weight, power, share, out, held, x, y, coeff, fold, diag, load):
    copy = pltpu.make_async_copy(spectra, held, load)
    copy.start()
    copy.wait()
    rows = PACKS * FEED_SETS
    slots = SECTIONS * GROUPS
    exact = dict(precision=lax.Precision.HIGHEST, preferred_element_type=jnp.float32)

    def tile(pack, slot, feed_set):
        source = (slot // GROUPS) * FEED_SETS + feed_set
        value = held[source, pack, slot % GROUPS].astype(jnp.float32)
        return value[0:GROUP], value[GROUP:]

    def spread(value, count):
        column = lax.broadcasted_iota(jnp.int32, (count, count * 8), 1) // 8
        row = lax.broadcasted_iota(jnp.int32, (count, count * 8), 0)
        pick = jnp.where(column == row, 1.0, 0.0).astype(jnp.float32)
        return jnp.dot(pick, value, **exact)

    def diagonal(feed_set, carry):
        for pack in range(PACKS):
            total = jnp.zeros((GROUP, 128), jnp.float32)
            for slot in range(slots):
                re, im = tile(pack, slot, feed_set)
                total = total + (re * re + im * im)
            fold[pack, 0, pl.ds(pl.multiple_of(feed_set * 8, 8), 8), :] = total
        return carry

    lax.fori_loop(0, FEED_SETS, diagonal, 0)
    for pack in range(PACKS):
        own = slice(pack * FEED_SETS, (pack + 1) * FEED_SETS)
        total = spread(fold[pack, 0], FEED_SETS)
        diag[own, :] = float(slots * GROUP) * power[own, :] - total
    x[0] = weight[...]
    x[1] = jnp.zeros((rows, 128), jnp.float32)

    def iterate(iteration, carry):
        def forward(index, inner):
            pack = index // slots
            slot = index % slots
            pr = [jnp.zeros((GROUP, 128), jnp.float32) for _ in range(2)]
            pi = [jnp.zeros((GROUP, 128), jnp.float32) for _ in range(2)]
            for feed_set in range(FEED_SETS):
                re, im = tile(pack, slot, feed_set)
                xr = x[0, pl.ds(pack * FEED_SETS + feed_set, 1), :]
                xi = x[1, pl.ds(pack * FEED_SETS + feed_set, 1), :]
                pr[0] = pr[0] + re * xr
                pr[1] = pr[1] + im * xi
                pi[0] = pi[0] + re * xi
                pi[1] = pi[1] - im * xr
            at = pl.multiple_of(index * GROUP, GROUP)
            coeff[0, pl.ds(at, GROUP), :] = pr[0] + pr[1]
            coeff[1, pl.ds(at, GROUP), :] = pi[0] + pi[1]
            return inner

        lax.fori_loop(0, PACKS * slots, forward, 0)
        for part in range(2):
            coeff[part] = jnp.dot(coeff[part], share[...], **exact)

        def backward(index, inner):
            pack = index // FEED_SETS
            feed_set = index % FEED_SETS
            yr = [jnp.zeros((GROUP, 128), jnp.float32) for _ in range(2)]
            yi = [jnp.zeros((GROUP, 128), jnp.float32) for _ in range(2)]
            for slot in range(slots):
                re, im = tile(pack, slot, feed_set)
                at = pl.multiple_of((pack * slots + slot) * GROUP, GROUP)
                pr = coeff[0, pl.ds(at, GROUP), :]
                pi = coeff[1, pl.ds(at, GROUP), :]
                yr[0] = yr[0] + re * pr
                yr[1] = yr[1] - im * pi
                yi[0] = yi[0] + re * pi
                yi[1] = yi[1] + im * pr
            at = pl.multiple_of(feed_set * 8, 8)
            fold[pack, 0, pl.ds(at, 8), :] = yr[0] + yr[1]
            fold[pack, 1, pl.ds(at, 8), :] = yi[0] + yi[1]
            return inner

        lax.fori_loop(0, rows, backward, 0)
        for pack in range(PACKS):
            own = slice(pack * FEED_SETS, (pack + 1) * FEED_SETS)
            w = weight[own, :]
            power_here = jnp.zeros((1, 128), jnp.float32)
            parts = []
            for part in range(2):
                total = spread(fold[pack, part], FEED_SETS)
                value = w * (total + diag[own, :] * (w * x[part, own, :]))
                y[part, own, :] = value
                parts.append(value)
                power_here = power_here + jnp.sum(value * value, axis=0, keepdims=True)
            squares = jnp.dot(jnp.broadcast_to(power_here, (8, 128)), share[...], **exact)
            length = jnp.sqrt(squares[0:1] + EPSILON)
            last = iteration == ITERS - 1
            scale = jnp.where(last, jnp.sqrt(length), length)
            for part in range(2):
                x[part, own, :] = parts[part] / scale
        return carry

    lax.fori_loop(0, ITERS, iterate, 0)
    out[...] = x[...]


def solve(spectra, usable, auto_power):
    _, _, _, share = tables()
    rows = PACKS * FEED_SETS

    def arrange(array):
        array = array.reshape(PACKS, 8, FEED_SETS, FEEDS_HERE)
        return array.transpose(0, 2, 1, 3).reshape(rows, 128)

    vmem = pl.BlockSpec(memory_space=pltpu.VMEM)
    gains = pl.pallas_call(
        solve_kernel,
        out_shape=jax.ShapeDtypeStruct((2, rows, 128), jnp.float32),
        in_specs=[pl.BlockSpec(memory_space=pl.ANY), vmem, vmem, vmem],
        out_specs=vmem,
        scratch_shapes=[
            pltpu.VMEM((OWNERS, PACKS, GROUPS, 16, 128), jnp.bfloat16),
            pltpu.VMEM((2, rows, 128), jnp.float32),
            pltpu.VMEM((2, rows, 128), jnp.float32),
            pltpu.VMEM((2, PACKS * SECTIONS * GROUPS * GROUP, 128), jnp.float32),
            pltpu.VMEM((PACKS, 2, FEED_SETS * 8, 128), jnp.float32),
            pltpu.VMEM((rows, 128), jnp.float32),
            pltpu.SemaphoreType.DMA,
        ],
        compiler_params=pltpu.CompilerParams(vmem_limit_bytes=48 * 1024 * 1024),
        cost_estimate=pl.CostEstimate(flops=10**10, bytes_accessed=2 * 10**7, transcendentals=0),
    )(spectra, arrange(usable.astype(jnp.float32)), arrange(auto_power), share)
    gains = gains.reshape(2, PACKS, FEED_SETS, 8, FEEDS_HERE).transpose(0, 1, 3, 2, 4)
    return gains.reshape(2, PACKS * 8, FEED_SETS * FEEDS_HERE)


def local(voltages, usable, auto_power):
    tail_samples = voltages[:, :, voltages.shape[2] - MARGIN :]
    route = [(i, i + 1) for i in range(SECTIONS - 1)]
    history = lax.ppermute(tail_samples, "section", route)
    spectra = channelize(voltages, history)
    turned = lax.all_to_all(spectra, ("section", "chan"), split_axis=0, concat_axis=0, tiled=True)
    return solve(turned, usable, auto_power)


def solution(mesh):
    in_specs = (
        P(None, "chan", "section"),
        P(("section", "chan"), None),
        P(("section", "chan"), None),
    )
    out_specs = P(None, ("section", "chan"), None)
    return jax.shard_map(local, mesh=mesh, in_specs=in_specs, out_specs=out_specs, check_vma=False)
```

```python
import functools
import math

import jax
import jax.numpy as jnp
import numpy as np
from jax import lax
from jax.experimental import pallas as pl
from jax.experimental.pallas import tpu as pltpu
from jax.sharding import PartitionSpec as P

CHANNELS = 4096
TAPS = 4
ITERS = 5
EPSILON = 1e-06

COARSE = 32
FINE = 128
FEEDS_HERE = 16
BLOCKS_HERE = 32
GROUP = 8
GROUPS = BLOCKS_HERE // GROUP
PACKS = 4
OWNERS = 128
SECTIONS = 4
FEED_SETS = 32
SLOTS = SECTIONS * GROUPS
STEP = 45
STRIDE = 17
MARGIN = (TAPS - 1) * CHANNELS
LENGTH = BLOCKS_HERE * CHANNELS


def tables():
    position = np.arange(TAPS * CHANNELS, dtype=np.float64)
    offset = (position - 0.5 * TAPS * CHANNELS + 0.5) / CHANNELS
    window = 0.5 - 0.5 * np.cos(2.0 * np.pi * (position + 0.5) / (TAPS * CHANNELS))
    taps = np.sin(np.pi * offset) / (np.pi * offset) * window
    taps = taps.reshape(TAPS * COARSE, FINE).astype(np.float32)
    angle = 2.0 * np.pi * np.outer(np.arange(COARSE), np.arange(FINE)) / CHANNELS
    twiddle = np.concatenate([np.cos(angle), np.sin(angle)], axis=0).astype(np.float32)
    angle = 2.0 * np.pi * (np.outer(np.arange(FINE), np.arange(FINE)) % FINE) / FINE
    cosine = np.cos(angle) / math.sqrt(CHANNELS)
    sine = np.sin(angle) / math.sqrt(CHANNELS)
    fine = np.block([[cosine, sine], [-sine, cosine]]).astype(np.float32)
    lane = np.arange(128)
    share = (lane[:, None] // FEEDS_HERE == lane[None, :] // FEEDS_HERE).astype(np.float32)
    return taps, twiddle, fine, share


def butterfly_4(x):
    (ar, ai), (br, bi), (cr, ci), (dr, di) = x
    pr, pi, qr, qi = ar + cr, ai + ci, ar - cr, ai - ci
    sr, si, tr, ti = br + dr, bi + di, br - dr, bi - di
    return [(pr + sr, pi + si), (qr + ti, qi - tr), (pr - sr, pi - si), (qr - ti, qi + tr)]


def turn(x, eighths_of_32):
    n = eighths_of_32 % 32
    re, im = x
    if n == 0:
        return re, im
    if n == 8:
        return im, -re
    if n == 16:
        return -re, -im
    if n == 24:
        return -im, re
    cosine, sine = math.cos(2 * math.pi * n / 32), math.sin(2 * math.pi * n / 32)
    if n % 4 == 0:
        h = math.sqrt(0.5)
        if n == 4:
            return (re + im) * h, (im - re) * h
        if n == 12:
            return (im - re) * h, (re + im) * -h
    return re * cosine + im * sine, im * cosine - re * sine


def butterfly_8(x):
    even = butterfly_4([x[0], x[2], x[4], x[6]])
    odd = butterfly_4([x[1], x[3], x[5], x[7]])
    low, high = [], []
    for k in range(4):
        er, ei = even[k]
        tr, ti = turn(odd[k], 4 * k)
        low.append((er + tr, ei + ti))
        high.append((er - tr, ei - ti))
    return low + high


def first_transform(block, ext, taps, halfway):
    start = block * CHANNELS
    for low in range(8):
        points = []
        for high in range(4):
            tile = 8 * high + low
            pair = []
            for part in range(2):
                total = None
                for tap in range(TAPS):
                    at = pl.multiple_of(start + (tap * COARSE + tile) * FINE, FINE)
                    row = tap * COARSE + tile
                    term = taps[row : row + 1, :] * ext[part, :, pl.ds(at, FINE)].astype(jnp.float32)
                    total = term if total is None else total + term
                pair.append(total)
            points.append(tuple(pair))
        for q, point in enumerate(butterfly_4(points)):
            re, im = turn(point, low * q)
            halfway[q, low, 0] = re
            halfway[q, low, 1] = im


def second_transform(twiddle, halfway, upper, lower):
    for q1 in range(4):
        points = [(halfway[q1, low, 0], halfway[q1, low, 1]) for low in range(8)]
        for q2, (re, im) in enumerate(butterfly_8(points)):
            q = q1 + 4 * q2
            if q > 0:
                cosine = twiddle[q : q + 1, :]
                sine = twiddle[COARSE + q : COARSE + q + 1, :]
                re, im = re * cosine + im * sine, im * cosine - re * sine
            for part, value in enumerate((re, im)):
                high = value.astype(jnp.bfloat16)
                low = (value - high.astype(jnp.float32)).astype(jnp.bfloat16)
                rows = slice(q * FEEDS_HERE, (q + 1) * FEEDS_HERE)
                lanes = slice(part * FINE, (part + 1) * FINE)
                upper[rows, lanes] = high
                lower[rows, lanes] = low


def fine_transform(at, fine_upper, fine_lower, upper, lower, stage):
    dims = (((1,), (1,)), ((), ()))
    for half in range(2):
        rows = slice(half * 256, (half + 1) * 256)
        high = upper[rows, :]
        low = lower[rows, :]
        out = lax.dot_general(fine_upper[...], high, dims, preferred_element_type=jnp.float32)
        out += lax.dot_general(fine_lower[...], high, dims, preferred_element_type=jnp.float32)
        out += lax.dot_general(fine_upper[...], low, dims, preferred_element_type=jnp.float32)
        for pack in range(2):
            for part in range(2):
                piece = out[part * FINE : (part + 1) * FINE, pack * 128 : (pack + 1) * 128]
                stage[2 * half + pack, pl.ds(part * GROUP + at, OWNERS, stride=STRIDE), :] = piece


def copy_at(source, target, sems, at, peer):
    return pltpu.make_async_remote_copy(
        src_ref=source,
        dst_ref=target,
        send_sem=sems[0].at[at],
        recv_sem=sems[1].at[at],
        device_id=(lax.div(peer, FEED_SETS), lax.rem(peer, FEED_SETS)),
        device_id_type=pl.DeviceIdType.MESH,
    )


def exact_dot(left, right, split_left):
    value = left if split_left else right
    high = value.astype(jnp.bfloat16)
    low = (value - high.astype(jnp.float32)).astype(jnp.bfloat16)
    if split_left:
        return jnp.dot(high, right, preferred_element_type=jnp.float32) + jnp.dot(
            low, right, preferred_element_type=jnp.float32
        )
    return jnp.dot(left, high, preferred_element_type=jnp.float32) + jnp.dot(
        left, low, preferred_element_type=jnp.float32
    )


def solve_packs(tile, first, count, weight, power, share, x, coeff, fold, diag):
    feeds = FEED_SETS * 8
    own = pl.ds(pl.multiple_of(first * FEED_SETS, FEED_SETS), count * FEED_SETS)
    column = lax.broadcasted_iota(jnp.int32, (FEED_SETS, feeds), 1)
    row = lax.broadcasted_iota(jnp.int32, (FEED_SETS, feeds), 0)
    near = (column >= row * 8) & (column < row * 8 + 8)
    pick = jnp.where(near, 1.0, 0.0).astype(jnp.bfloat16)

    def diagonal(feed_set, carry):
        for pack in range(count):
            total = [jnp.zeros((GROUP, 128), jnp.float32) for _ in range(2)]
            for slot in range(SLOTS):
                re, im = tile(pack, slot, feed_set)
                total[0] = total[0] + re * re
                total[1] = total[1] + im * im
            fold[pack, 0, pl.ds(pl.multiple_of(feed_set * 8, 8), 8), :] = total[0] + total[1]
        return carry

    lax.fori_loop(0, FEED_SETS, diagonal, 0)
    w_all = weight[own, :]
    p_all = power[own, :]
    for pack in range(count):
        here = slice(pack * FEED_SETS, (pack + 1) * FEED_SETS)
        total = exact_dot(pick, fold[pack, 0], False)
        diag[here, :] = float(SLOTS * GROUP) * p_all[here] - total
    x[0, 0 : count * FEED_SETS, :] = w_all
    x[1, 0 : count * FEED_SETS, :] = jnp.zeros_like(w_all)

    def iterate(iteration, carry):
        for pack in range(count):

            def forward(index, inner):
                pr = [jnp.zeros((GROUP, 128), jnp.float32) for _ in range(4)]
                pi = [jnp.zeros((GROUP, 128), jnp.float32) for _ in range(4)]
                for feed_set in range(FEED_SETS):
                    at = pack * FEED_SETS + feed_set
                    xr = x[0, at : at + 1, :]
                    xi = x[1, at : at + 1, :]
                    for two in range(2):
                        re, im = tile(pack, index * 2 + two, feed_set)
                        pr[two] = pr[two] + re * xr
                        pr[2 + two] = pr[2 + two] + im * xi
                        pi[two] = pi[two] + re * xi
                        pi[2 + two] = pi[2 + two] - im * xr
                at = pl.multiple_of((pack * SLOTS + index * 2) * GROUP, 2 * GROUP)
                for two in range(2):
                    coeff[0, pl.ds(at + two * GROUP, GROUP), :] = pr[two] + pr[2 + two]
                    coeff[1, pl.ds(at + two * GROUP, GROUP), :] = pi[two] + pi[2 + two]
                return inner

            lax.fori_loop(0, SLOTS // 2, forward, 0)
        for part in range(2):
            rows = slice(0, count * SLOTS * GROUP)
            coeff[part, rows, :] = exact_dot(coeff[part, rows, :], share[...], True)

        for pack in range(count):

            def backward(index, inner):
                yr = [jnp.zeros((GROUP, 128), jnp.float32) for _ in range(8)]
                yi = [jnp.zeros((GROUP, 128), jnp.float32) for _ in range(8)]
                for slot in range(SLOTS):
                    at = (pack * SLOTS + slot) * GROUP
                    pr = coeff[0, at : at + GROUP, :]
                    pi = coeff[1, at : at + GROUP, :]
                    for two in range(4):
                        re, im = tile(pack, slot, index * 4 + two)
                        yr[two] = yr[two] + re * pr
                        yr[4 + two] = yr[4 + two] - im * pi
                        yi[two] = yi[two] + re * pi
                        yi[4 + two] = yi[4 + two] + im * pr
                for two in range(4):
                    at = pl.multiple_of((index * 4 + two) * 8, 8)
                    fold[pack, 0, pl.ds(at, 8), :] = yr[two] + yr[4 + two]
                    fold[pack, 1, pl.ds(at, 8), :] = yi[two] + yi[4 + two]
                return inner

            lax.fori_loop(0, FEED_SETS // 4, backward, 0)
        for pack in range(count):
            here = slice(pack * FEED_SETS, (pack + 1) * FEED_SETS)
            w = w_all[here]
            squares = jnp.zeros((1, 128), jnp.float32)
            parts = []
            for part in range(2):
                total = exact_dot(pick, fold[pack, part], False)
                value = w * (total + diag[here, :] * (w * x[part, here, :]))
                parts.append(value)
                squares = squares + jnp.sum(value * value, axis=0, keepdims=True)
            squares = jnp.broadcast_to(squares, (8, 128))
            total = jnp.dot(
                squares,
                share[...].astype(jnp.float32),
                precision=lax.Precision.HIGHEST,
                preferred_element_type=jnp.float32,
            )
            length = jnp.sqrt(total[0:1] + EPSILON)
            scale = jnp.where(iteration == ITERS - 1, jnp.sqrt(length), length)
            for part in range(2):
                x[part, here, :] = parts[part] / scale
        return carry

    lax.fori_loop(0, ITERS, iterate, 0)


def kernel(
    volt, taps, twiddle, fine_upper, fine_lower, weight, power, share, out,
    ext, halfway, upper, lower, stage, sent_pair, sent_one, held_pair, held_one,
    x, coeff, fold, diag, loads, send_sems, recv_sems, edge_sems,
):
    section = lax.axis_index("section")
    me = section * FEED_SETS + lax.axis_index("chan")
    sems = (send_sems, recv_sems)
    barrier = pltpu.get_barrier_semaphore()

    def greet(step, carry):
        peer = lax.rem(me + lax.rem(step * STEP, OWNERS), OWNERS)
        pl.semaphore_signal(
            barrier,
            inc=1,
            device_id=(lax.div(peer, FEED_SETS), lax.rem(peer, FEED_SETS)),
            device_id_type=pl.DeviceIdType.MESH,
        )
        return carry

    lax.fori_loop(1, OWNERS, greet, 0)

    def load(group):
        width = GROUP * CHANNELS
        start = pl.multiple_of(group * width, width)
        return pltpu.make_async_copy(
            volt.at[:, :, pl.ds(start, width)],
            ext.at[:, :, pl.ds(MARGIN + start, width)],
            loads.at[group],
        )

    edge = pltpu.make_async_remote_copy(
        src_ref=volt.at[:, :, pl.ds(LENGTH - MARGIN, MARGIN)],
        dst_ref=ext.at[:, :, pl.ds(0, MARGIN)],
        send_sem=edge_sems.at[0],
        recv_sem=edge_sems.at[1],
        device_id=(lax.rem(section + 1, SECTIONS), lax.axis_index("chan")),
        device_id_type=pl.DeviceIdType.MESH,
    )
    for position in range(GROUPS):
        load((position) % GROUPS).start()
    load(0).wait()

    def grouped(position, carry):
        group = lax.rem(position + 1, GROUPS)

        @pl.when(position < GROUPS - 1)
        def _():
            load(group).wait()

        @pl.when(position == GROUPS - 1)
        def _():
            edge.wait()

            @pl.when(section == 0)
            def _():
                def clear(at, inner):
                    where = pl.ds(pl.multiple_of(at * FINE, FINE), FINE)
                    for part in range(2):
                        ext[part, :, where] = jnp.zeros((FEEDS_HERE, FINE), jnp.bfloat16)
                    return inner

                lax.fori_loop(0, MARGIN // FINE, clear, 0)

        def step(at, inner):
            first_transform(group * GROUP + at, ext, taps, halfway)
            second_transform(twiddle, halfway, upper, lower)
            fine_transform(at, fine_upper, fine_lower, upper, lower, stage)
            return inner

        lax.fori_loop(0, GROUP, step, 0)

        def emit(owner, inner):
            rows = pl.ds(owner * STRIDE, 16)
            for pack in range(2):
                sent_pair[owner, group, pack] = stage[pack, rows, :].astype(jnp.bfloat16)
                sent_one[pack, owner, group] = stage[2 + pack, rows, :].astype(jnp.bfloat16)
            return inner

        lax.fori_loop(0, OWNERS, emit, 0, unroll=8)

        @pl.when(position == 0)
        def _():
            pl.semaphore_wait(barrier, OWNERS - 1)
            edge.start()

        def send(step, inner):
            peer = lax.rem(me + lax.rem(step * STEP, OWNERS), OWNERS)
            copy_at(sent_pair.at[peer, group], held_pair.at[me, group], sems, 0, peer).start()
            return inner

        lax.fori_loop(1, OWNERS, send, 0)
        return carry

    lax.fori_loop(0, GROUPS, grouped, 0)
    for pack in range(2):

        def send(step, inner):
            peer = lax.rem(me + lax.rem(step * STEP, OWNERS), OWNERS)
            copy_at(
                sent_one.at[pack, peer], held_one.at[pack, me], sems, 1 + pack, peer
            ).start()
            return inner

        lax.fori_loop(1, OWNERS, send, 0)

    for group in range(GROUPS):
        for pack in range(2):
            held_pair[me, group, pack] = sent_pair[me, group, pack]
            held_one[pack, me, group] = sent_one[pack, me, group]

    others = pl.ds(0, OWNERS - 1)
    pltpu.make_async_copy(sent_pair.at[others], held_pair.at[others], recv_sems.at[0]).wait()

    def tile_pair(pack, slot, feed_set):
        source = lax.div(slot, GROUPS) * FEED_SETS + feed_set
        value = held_pair[source, lax.rem(slot, GROUPS), pack].astype(jnp.float32)
        return value[0:GROUP], value[GROUP:]

    solve_packs(tile_pair, 0, 2, weight, power, share, x, coeff, fold, diag)
    out[:, 0 : 2 * FEED_SETS, :] = x[...]

    def single(index, carry):
        pltpu.make_async_copy(
            sent_one.at[0, others], held_one.at[index, others], recv_sems.at[1 + index]
        ).wait()

        def tile_one(pack, slot, feed_set):
            source = lax.div(slot, GROUPS) * FEED_SETS + feed_set
            value = held_one[index, source, lax.rem(slot, GROUPS)].astype(jnp.float32)
            return value[0:GROUP], value[GROUP:]

        solve_packs(tile_one, 2 + index, 1, weight, power, share, x, coeff, fold, diag)
        at = pl.multiple_of((2 + index) * FEED_SETS, FEED_SETS)
        out[:, pl.ds(at, FEED_SETS), :] = x[:, 0:FEED_SETS, :]
        return carry

    lax.fori_loop(0, 2, single, 0)
    pltpu.make_async_copy(sent_pair.at[others], held_pair.at[others], send_sems.at[0]).wait()
    for pack in range(2):
        pltpu.make_async_copy(
            sent_one.at[pack, others], held_one.at[pack, others], send_sems.at[1 + pack]
        ).wait()


def local(voltages, usable, auto_power):
    taps, twiddle, fine, share = tables()
    upper = fine.astype(jnp.bfloat16)
    lower = (fine - upper.astype(np.float32)).astype(jnp.bfloat16)
    rows = PACKS * FEED_SETS

    def arrange(array):
        array = array.reshape(PACKS, 8, FEED_SETS, FEEDS_HERE)
        return array.transpose(0, 2, 1, 3).reshape(rows, 128)

    vmem = pl.BlockSpec(memory_space=pltpu.VMEM)
    pair = pltpu.VMEM((OWNERS, GROUPS, 2, 16, 128), jnp.bfloat16)
    one = pltpu.VMEM((2, OWNERS, GROUPS, 16, 128), jnp.bfloat16)
    gains = pl.pallas_call(
        kernel,
        out_shape=jax.ShapeDtypeStruct((2, rows, 128), jnp.float32),
        in_specs=[pl.BlockSpec(memory_space=pl.ANY)] + [vmem] * 7,
        out_specs=vmem,
        scratch_shapes=[
            pltpu.VMEM((2, FEEDS_HERE, MARGIN + LENGTH), jnp.bfloat16),
            pltpu.VMEM((4, 8, 2, FEEDS_HERE, FINE), jnp.float32),
            pltpu.VMEM((COARSE * FEEDS_HERE, 256), jnp.bfloat16),
            pltpu.VMEM((COARSE * FEEDS_HERE, 256), jnp.bfloat16),
            pltpu.VMEM((PACKS, OWNERS * STRIDE + 8, 128), jnp.float32),
            pair,
            one,
            pair,
            one,
            pltpu.VMEM((2, 2 * FEED_SETS, 128), jnp.float32),
            pltpu.VMEM((2, 2 * SLOTS * GROUP, 128), jnp.float32),
            pltpu.VMEM((2, 2, FEED_SETS * 8, 128), jnp.float32),
            pltpu.VMEM((2 * FEED_SETS, 128), jnp.float32),
            pltpu.SemaphoreType.DMA((GROUPS,)),
            pltpu.SemaphoreType.DMA((3,)),
            pltpu.SemaphoreType.DMA((3,)),
            pltpu.SemaphoreType.DMA((2,)),
        ],
        compiler_params=pltpu.CompilerParams(
            collective_id=0, has_side_effects=True, vmem_limit_bytes=56 * 1024 * 1024
        ),
        cost_estimate=pl.CostEstimate(flops=10**10, bytes_accessed=2 * 10**7, transcendentals=0),
    )(
        voltages, taps, twiddle, upper, lower,
        arrange(usable.astype(jnp.float32)), arrange(auto_power), share.astype(jnp.bfloat16),
    )
    gains = gains.reshape(2, PACKS, FEED_SETS, 8, FEEDS_HERE).transpose(0, 1, 3, 2, 4)
    return gains.reshape(2, PACKS * 8, FEED_SETS * FEEDS_HERE)


def solution(mesh):
    in_specs = (
        P(None, "chan", "section"),
        P(("section", "chan"), None),
        P(("section", "chan"), None),
    )
    out_specs = P(None, ("section", "chan"), None)
    return jax.shard_map(local, mesh=mesh, in_specs=in_specs, out_specs=out_specs, check_vma=False)
```

```python
import functools
import math

import jax
import jax.numpy as jnp
import numpy as np
from jax import lax
from jax.experimental import pallas as pl
from jax.experimental.pallas import tpu as pltpu
from jax.sharding import PartitionSpec as P

CHANNELS = 4096
TAPS = 4
ITERS = 5
EPSILON = 1e-06

COARSE = 32
FINE = 128
FEEDS_HERE = 16
BLOCKS_HERE = 32
GROUP = 8
GROUPS = BLOCKS_HERE // GROUP
PACKS = 4
OWNERS = 128
SECTIONS = 4
FEED_SETS = 32
SLOTS = SECTIONS * GROUPS
STRIDE = 17
LENGTH = BLOCKS_HERE * CHANNELS
EARLY = 2 * CHANNELS
LATE = CHANNELS


def tables():
    position = np.arange(TAPS * CHANNELS, dtype=np.float64)
    offset = (position - 0.5 * TAPS * CHANNELS + 0.5) / CHANNELS
    window = 0.5 - 0.5 * np.cos(2.0 * np.pi * (position + 0.5) / (TAPS * CHANNELS))
    taps = np.sin(np.pi * offset) / (np.pi * offset) * window
    taps = taps.reshape(TAPS * COARSE, FINE).astype(np.float32)
    angle = 2.0 * np.pi * np.outer(np.arange(COARSE), np.arange(FINE)) / CHANNELS
    twiddle = np.concatenate([np.cos(angle), np.sin(angle)], axis=0).astype(np.float32)
    angle = 2.0 * np.pi * (np.outer(np.arange(FINE), np.arange(FINE)) % FINE) / FINE
    cosine = np.cos(angle) / math.sqrt(CHANNELS)
    sine = np.sin(angle) / math.sqrt(CHANNELS)
    fine = np.block([[cosine, sine], [-sine, cosine]]).astype(np.float32)
    lane = np.arange(128)
    share = (lane[:, None] // FEEDS_HERE == lane[None, :] // FEEDS_HERE).astype(np.float32)
    return taps, twiddle, fine, share


def butterfly_4(x):
    (ar, ai), (br, bi), (cr, ci), (dr, di) = x
    pr, pi, qr, qi = ar + cr, ai + ci, ar - cr, ai - ci
    sr, si, tr, ti = br + dr, bi + di, br - dr, bi - di
    return [(pr + sr, pi + si), (qr + ti, qi - tr), (pr - sr, pi - si), (qr - ti, qi + tr)]


def turn(x, eighths_of_32):
    n = eighths_of_32 % 32
    re, im = x
    if n == 0:
        return re, im
    if n == 8:
        return im, -re
    if n == 16:
        return -re, -im
    if n == 24:
        return -im, re
    cosine, sine = math.cos(2 * math.pi * n / 32), math.sin(2 * math.pi * n / 32)
    if n % 4 == 0:
        h = math.sqrt(0.5)
        if n == 4:
            return (re + im) * h, (im - re) * h
        if n == 12:
            return (im - re) * h, (re + im) * -h
    return re * cosine + im * sine, im * cosine - re * sine


def butterfly_8(x):
    even = butterfly_4([x[0], x[2], x[4], x[6]])
    odd = butterfly_4([x[1], x[3], x[5], x[7]])
    low, high = [], []
    for k in range(4):
        er, ei = even[k]
        tr, ti = turn(odd[k], 4 * k)
        low.append((er + tr, ei + ti))
        high.append((er - tr, ei - ti))
    return low + high


def first_transform(block, ext, taps, halfway):
    start = block * CHANNELS
    for low in range(8):
        points = []
        for high in range(4):
            tile = 8 * high + low
            pair = []
            for part in range(2):
                total = None
                for tap in range(TAPS):
                    at = pl.multiple_of(start + (tap * COARSE + tile) * FINE, FINE)
                    row = tap * COARSE + tile
                    term = taps[row : row + 1, :] * ext[part, :, pl.ds(at, FINE)].astype(jnp.float32)
                    total = term if total is None else total + term
                pair.append(total)
            points.append(tuple(pair))
        for q, point in enumerate(butterfly_4(points)):
            re, im = turn(point, low * q)
            halfway[q, low, 0] = re
            halfway[q, low, 1] = im


def second_transform(twiddle, halfway, upper, lower):
    for q1 in range(4):
        points = [(halfway[q1, low, 0], halfway[q1, low, 1]) for low in range(8)]
        for q2, (re, im) in enumerate(butterfly_8(points)):
            q = q1 + 4 * q2
            if q > 0:
                cosine = twiddle[q : q + 1, :]
                sine = twiddle[COARSE + q : COARSE + q + 1, :]
                re, im = re * cosine + im * sine, im * cosine - re * sine
            for part, value in enumerate((re, im)):
                high = value.astype(jnp.bfloat16)
                low = (value - high.astype(jnp.float32)).astype(jnp.bfloat16)
                rows = slice(q * FEEDS_HERE, (q + 1) * FEEDS_HERE)
                lanes = slice(part * FINE, (part + 1) * FINE)
                upper[rows, lanes] = high
                lower[rows, lanes] = low


def fine_transform(at, fine_upper, fine_lower, upper, lower, stage):
    dims = (((1,), (1,)), ((), ()))
    for half in range(2):
        rows = slice(half * 256, (half + 1) * 256)
        high = upper[rows, :]
        low = lower[rows, :]
        out = lax.dot_general(fine_upper[...], high, dims, preferred_element_type=jnp.float32)
        out += lax.dot_general(fine_lower[...], high, dims, preferred_element_type=jnp.float32)
        out += lax.dot_general(fine_upper[...], low, dims, preferred_element_type=jnp.float32)
        for pack in range(2):
            for part in range(2):
                piece = out[part * FINE : (part + 1) * FINE, pack * 128 : (pack + 1) * 128]
                stage[2 * half + pack, pl.ds(part * GROUP + at, OWNERS, stride=STRIDE), :] = piece


def partner(step, section, chan):
    def bit(at):
        return lax.rem(lax.div(step, 2**at), 2)

    there = lax.rem(section + bit(0) * 2 + bit(3), SECTIONS)
    y = lax.rem(lax.div(chan, 8) + bit(1) * 2 + bit(4), 4)
    z = lax.rem(lax.div(chan, 2) + bit(2) * 2 + bit(5), 4)
    core = lax.rem(chan + bit(6), 2)
    return there, y * 8 + z * 2 + core


def copy_at(source, target, sems, at, device):
    return pltpu.make_async_remote_copy(
        src_ref=source,
        dst_ref=target,
        send_sem=sems[0].at[at],
        recv_sem=sems[1].at[at],
        device_id=device,
        device_id_type=pl.DeviceIdType.MESH,
    )


def share_dot(value, share):
    high = value.astype(jnp.bfloat16)
    low = (value - high.astype(jnp.float32)).astype(jnp.bfloat16)
    total = jnp.dot(high, share, preferred_element_type=jnp.float32)
    return total + jnp.dot(low, share, preferred_element_type=jnp.float32)


def solve_packs(tile, first, count, weight, power, share, x, y, coeff, squares, diag):
    own = pl.ds(pl.multiple_of(first * FEED_SETS, FEED_SETS), count * FEED_SETS)

    def diagonal(feed_set, carry):
        for pack in range(count):
            total = [jnp.zeros((GROUP, 128), jnp.float32) for _ in range(4)]
            for slot in range(SLOTS):
                re, im = tile(pack, slot, feed_set)
                at = slot % 2
                total[at] = total[at] + re * re
                total[2 + at] = total[2 + at] + im * im
            total = (total[0] + total[1]) + (total[2] + total[3])
            at = pl.ds(pack * FEED_SETS + feed_set, 1)
            diag[at, :] = jnp.sum(total, axis=0, keepdims=True)
        return carry

    lax.fori_loop(0, FEED_SETS, diagonal, 0)
    span = slice(0, count * FEED_SETS)
    diag[span, :] = float(SLOTS * GROUP) * power[own, :] - diag[span, :]
    x[0, span, :] = weight[own, :]
    x[1, span, :] = jnp.zeros((count * FEED_SETS, 128), jnp.float32)
    squares[...] = jnp.zeros_like(squares)

    def lengths():
        total = share_dot(squares[...], share[...])
        return [jnp.sqrt(total[8 * pack : 8 * pack + 1] + EPSILON) for pack in range(count)]

    def iterate(iteration, carry):
        for pack in range(count):

            def forward(index, inner):
                pr = [jnp.zeros((GROUP, 128), jnp.float32) for _ in range(4)]
                pi = [jnp.zeros((GROUP, 128), jnp.float32) for _ in range(4)]
                for feed_set in range(FEED_SETS):
                    at = pack * FEED_SETS + feed_set
                    xr = x[0, at : at + 1, :]
                    xi = x[1, at : at + 1, :]
                    for two in range(2):
                        re, im = tile(pack, index * 2 + two, feed_set)
                        pr[two] = pr[two] + re * xr
                        pr[2 + two] = pr[2 + two] + im * xi
                        pi[two] = pi[two] + re * xi
                        pi[2 + two] = pi[2 + two] - im * xr
                at = pl.multiple_of((pack * SLOTS + index * 2) * GROUP, 2 * GROUP)
                for two in range(2):
                    coeff[0, pl.ds(at + two * GROUP, GROUP), :] = pr[two] + pr[2 + two]
                    coeff[1, pl.ds(at + two * GROUP, GROUP), :] = pi[two] + pi[2 + two]
                return inner

            lax.fori_loop(0, SLOTS // 2, forward, 0)
        inverse = [jnp.where(iteration == 0, 1.0, 1.0 / length) for length in lengths()]
        for pack in range(count):
            rows = slice(pack * SLOTS * GROUP, (pack + 1) * SLOTS * GROUP)
            for part in range(2):
                coeff[part, rows, :] = share_dot(coeff[part, rows, :], share[...]) * inverse[pack]
        for pack in range(count):

            def backward(index, inner):
                yr = [jnp.zeros((GROUP, 128), jnp.float32) for _ in range(8)]
                yi = [jnp.zeros((GROUP, 128), jnp.float32) for _ in range(8)]
                for slot in range(SLOTS):
                    at = (pack * SLOTS + slot) * GROUP
                    pr = coeff[0, at : at + GROUP, :]
                    pi = coeff[1, at : at + GROUP, :]
                    for two in range(4):
                        re, im = tile(pack, slot, index * 4 + two)
                        yr[two] = yr[two] + re * pr
                        yr[4 + two] = yr[4 + two] - im * pi
                        yi[two] = yi[two] + re * pi
                        yi[4 + two] = yi[4 + two] + im * pr
                for two in range(4):
                    at = pl.ds(pack * FEED_SETS + index * 4 + two, 1)
                    y[0, at, :] = jnp.sum(yr[two] + yr[4 + two], axis=0, keepdims=True)
                    y[1, at, :] = jnp.sum(yi[two] + yi[4 + two], axis=0, keepdims=True)
                return inner

            lax.fori_loop(0, FEED_SETS // 4, backward, 0)
        for pack in range(count):
            here = slice(pack * FEED_SETS, (pack + 1) * FEED_SETS)
            at = pl.ds(pl.multiple_of((first + pack) * FEED_SETS, FEED_SETS), FEED_SETS)
            w = weight[at, :]
            scaled = w * (diag[here, :] * (w * inverse[pack]))
            total = jnp.zeros((8, 128), jnp.float32)
            for part in range(2):
                value = w * y[part, here, :] + scaled * x[part, here, :]
                x[part, here, :] = value
                for row in range(0, FEED_SETS, 8):
                    total = total + value[row : row + 8] * value[row : row + 8]
            total = jnp.sum(total, axis=0, keepdims=True)
            squares[8 * pack : 8 * pack + 8, :] = jnp.broadcast_to(total, (8, 128))
        return carry

    lax.fori_loop(0, ITERS, iterate, 0)
    for pack, length in enumerate(lengths()):
        here = slice(pack * FEED_SETS, (pack + 1) * FEED_SETS)
        for part in range(2):
            x[part, here, :] = x[part, here, :] / jnp.sqrt(length)


def kernel(
    volt, taps, twiddle, fine_upper, fine_lower, usable, auto_power, share, repeat, out,
    weight, power, lined, ext, halfway, upper, lower, stage, sent_pair, sent_one, held_pair, held_one,
    x, y, coeff, squares, diag, loads, send_sems, recv_sems, edge_sems,
):
    def arrange(source, target, split):
        feeds = FEED_SETS * FEEDS_HERE
        lane = lax.broadcasted_iota(jnp.int32, (FEED_SETS, feeds), 1)
        first = lax.broadcasted_iota(jnp.int32, (FEED_SETS, feeds), 0) * FEEDS_HERE
        mine = (lane >= first) & (lane < first + FEEDS_HERE)
        place = lax.broadcasted_iota(jnp.int32, (FEED_SETS, 128), 1)

        def body(pack, carry):
            for q in range(8):
                row = source[pl.ds(pack * 8 + q, 1), :].astype(jnp.float32)
                lined[q * FEED_SETS : (q + 1) * FEED_SETS, :] = jnp.where(mine, row, 0.0)
            value = lined[...]
            high = value.astype(jnp.bfloat16)
            wide = jnp.dot(high, repeat[...], preferred_element_type=jnp.float32)
            if split:
                rest = value - high.astype(jnp.float32)
                middle = rest.astype(jnp.bfloat16)
                low = (rest - middle.astype(jnp.float32)).astype(jnp.bfloat16)
                wide = wide + jnp.dot(middle, repeat[...], preferred_element_type=jnp.float32)
                wide = wide + jnp.dot(low, repeat[...], preferred_element_type=jnp.float32)
            total = jnp.zeros((FEED_SETS, 128), jnp.float32)
            for q in range(8):
                part = wide[q * FEED_SETS : (q + 1) * FEED_SETS]
                own = (place >= q * FEEDS_HERE) & (place < (q + 1) * FEEDS_HERE)
                total = total + jnp.where(own, part, 0.0)
            target[pl.ds(pl.multiple_of(pack * FEED_SETS, FEED_SETS), FEED_SETS), :] = total
            return carry

        lax.fori_loop(0, PACKS, body, 0)

    section = lax.axis_index("section")
    chan = lax.axis_index("chan")
    me = section * FEED_SETS + chan
    sems = (send_sems, recv_sems)
    load = pltpu.make_async_copy(volt, ext.at[:, :, pl.ds(EARLY, LENGTH)], loads)
    load.start()
    barrier = pltpu.get_barrier_semaphore()

    def greet(step, carry):
        pl.semaphore_signal(
            barrier,
            inc=1,
            device_id=partner(step, section, chan),
            device_id_type=pl.DeviceIdType.MESH,
        )
        return carry

    lax.fori_loop(1, OWNERS, greet, 0)
    early = copy_at(
        volt.at[:, :, pl.ds(LENGTH - EARLY, EARLY)],
        ext.at[:, :, pl.ds(0, EARLY)],
        (edge_sems, edge_sems.at[pl.ds(2, 2)]),
        0,
        (lax.rem(section + 1, SECTIONS), chan),
    )
    late = copy_at(
        volt.at[:, :, pl.ds(0, LATE)],
        ext.at[:, :, pl.ds(EARLY + LENGTH, LATE)],
        (edge_sems, edge_sems.at[pl.ds(2, 2)]),
        1,
        (lax.rem(section + SECTIONS - 1, SECTIONS), chan),
    )
    pl.semaphore_wait(barrier, OWNERS - 1)
    early.start()
    late.start()
    arrange(usable, weight, False)
    load.wait()

    def clear(first, count):
        def body(at, inner):
            where = pl.ds(pl.multiple_of(first * CHANNELS + at * FINE, FINE), FINE)
            for part in range(2):
                ext[part, :, where] = jnp.zeros((FEEDS_HERE, FINE), jnp.bfloat16)
            return inner

        lax.fori_loop(0, count * COARSE, body, 0)

    def grouped(position, carry):
        group = lax.rem(position + 1, GROUPS)

        @pl.when(position == 2)
        def _():
            late.wait()

        @pl.when(position == 3)
        def _():
            early.wait()

            @pl.when(section == 0)
            def _():
                clear(0, 2)

        def step(at, inner):
            @pl.when((section == SECTIONS - 1) & (position == 2) & (at == GROUP - 1))
            def _():
                clear(BLOCKS_HERE - 1, TAPS - 1)

            first_transform(group * GROUP + at, ext, taps, halfway)
            second_transform(twiddle, halfway, upper, lower)
            fine_transform(at, fine_upper, fine_lower, upper, lower, stage)
            return inner

        lax.fori_loop(0, GROUP, step, 0)

        def emit(owner, inner):
            rows = pl.ds(owner * STRIDE, 16)
            for pack in range(2):
                sent_pair[owner, group, pack] = stage[pack, rows, :].astype(jnp.bfloat16)
                sent_one[pack, owner, group] = stage[2 + pack, rows, :].astype(jnp.bfloat16)
            return inner

        lax.fori_loop(0, OWNERS, emit, 0, unroll=8)

        def send(step, inner):
            there, column = partner(step, section, chan)
            source = sent_pair.at[there * FEED_SETS + column, group]
            copy_at(source, held_pair.at[me, group], sems, 0, (there, column)).start()
            return inner

        lax.fori_loop(1, OWNERS, send, 0)
        return carry

    lax.fori_loop(0, GROUPS, grouped, 0)

    def rest(pack, carry):
        def send(step, inner):
            there, column = partner(step, section, chan)
            source = sent_one.at[pack, there * FEED_SETS + column]
            copy_at(source, held_one.at[pack, me], sems, 1 + pack, (there, column)).start()
            return inner

        lax.fori_loop(1, OWNERS, send, 0)
        return carry

    lax.fori_loop(0, 2, rest, 0)
    arrange(auto_power, power, True)

    for group in range(GROUPS):
        for pack in range(2):
            held_pair[me, group, pack] = sent_pair[me, group, pack]
            held_one[pack, me, group] = sent_one[pack, me, group]

    others = pl.ds(0, OWNERS - 1)
    pltpu.make_async_copy(sent_pair.at[others], held_pair.at[others], recv_sems.at[0]).wait()

    def tile_pair(pack, slot, feed_set):
        source = lax.div(slot, GROUPS) * FEED_SETS + feed_set
        value = held_pair[source, lax.rem(slot, GROUPS), pack].astype(jnp.float32)
        return value[0:GROUP], value[GROUP:]

    solve_packs(tile_pair, 0, 2, weight, power, share, x, y, coeff, squares, diag)
    out[:, 0 : 2 * FEED_SETS, :] = x[...]

    def single(index, carry):
        pltpu.make_async_copy(
            sent_one.at[0, others], held_one.at[index, others], recv_sems.at[1 + index]
        ).wait()

        def tile_one(pack, slot, feed_set):
            source = lax.div(slot, GROUPS) * FEED_SETS + feed_set
            value = held_one[index, source, lax.rem(slot, GROUPS)].astype(jnp.float32)
            return value[0:GROUP], value[GROUP:]

        solve_packs(tile_one, 2 + index, 1, weight, power, share, x, y, coeff, squares, diag)
        at = pl.multiple_of((2 + index) * FEED_SETS, FEED_SETS)
        out[:, pl.ds(at, FEED_SETS), :] = x[:, 0:FEED_SETS, :]
        return carry

    lax.fori_loop(0, 2, single, 0)
    pltpu.make_async_copy(sent_pair.at[others], held_pair.at[others], send_sems.at[0]).wait()
    for pack in range(2):
        pltpu.make_async_copy(
            sent_one.at[pack, others], held_one.at[pack, others], send_sems.at[1 + pack]
        ).wait()


def local(voltages, usable, auto_power):
    taps, twiddle, fine, share = tables()
    upper = fine.astype(jnp.bfloat16)
    lower = (fine - upper.astype(np.float32)).astype(jnp.bfloat16)
    rows = PACKS * FEED_SETS

    lane = np.arange(FEED_SETS * FEEDS_HERE)[:, None] % FEEDS_HERE
    repeat = (lane == np.arange(128)[None, :] % FEEDS_HERE).astype(jnp.bfloat16)
    vmem = pl.BlockSpec(memory_space=pltpu.VMEM)
    pair = pltpu.VMEM((OWNERS, GROUPS, 2, 16, 128), jnp.bfloat16)
    one = pltpu.VMEM((2, OWNERS, GROUPS, 16, 128), jnp.bfloat16)
    gains = pl.pallas_call(
        kernel,
        out_shape=jax.ShapeDtypeStruct((2, rows, 128), jnp.float32),
        in_specs=[pl.BlockSpec(memory_space=pl.ANY)] + [vmem] * 8,
        out_specs=vmem,
        scratch_shapes=[
            pltpu.VMEM((rows, 128), jnp.float32),
            pltpu.VMEM((rows, 128), jnp.float32),
            pltpu.VMEM((8 * FEED_SETS, FEED_SETS * FEEDS_HERE), jnp.float32),
            pltpu.VMEM((2, FEEDS_HERE, EARLY + LENGTH + LATE), jnp.bfloat16),
            pltpu.VMEM((4, 8, 2, FEEDS_HERE, FINE), jnp.float32),
            pltpu.VMEM((COARSE * FEEDS_HERE, 256), jnp.bfloat16),
            pltpu.VMEM((COARSE * FEEDS_HERE, 256), jnp.bfloat16),
            pltpu.VMEM((PACKS, OWNERS * STRIDE + 8, 128), jnp.float32),
            pair,
            one,
            pair,
            one,
            pltpu.VMEM((2, 2 * FEED_SETS, 128), jnp.float32),
            pltpu.VMEM((2, 2 * FEED_SETS, 128), jnp.float32),
            pltpu.VMEM((2, 2 * SLOTS * GROUP, 128), jnp.float32),
            pltpu.VMEM((16, 128), jnp.float32),
            pltpu.VMEM((2 * FEED_SETS, 128), jnp.float32),
            pltpu.SemaphoreType.DMA,
            pltpu.SemaphoreType.DMA((3,)),
            pltpu.SemaphoreType.DMA((3,)),
            pltpu.SemaphoreType.DMA((4,)),
        ],
        compiler_params=pltpu.CompilerParams(
            collective_id=0, has_side_effects=True, vmem_limit_bytes=56 * 1024 * 1024
        ),
        cost_estimate=pl.CostEstimate(flops=10**10, bytes_accessed=2 * 10**7, transcendentals=0),
    )(
        voltages, taps, twiddle, upper, lower,
        usable, auto_power, share.astype(jnp.bfloat16), repeat,
    )
    gains = gains.reshape(2, PACKS, FEED_SETS, 8, FEEDS_HERE).transpose(0, 1, 3, 2, 4)
    return gains.reshape(2, PACKS * 8, FEED_SETS * FEEDS_HERE)


def solution(mesh):
    in_specs = (
        P(None, "chan", "section"),
        P(("section", "chan"), None),
        P(("section", "chan"), None),
    )
    out_specs = P(None, ("section", "chan"), None)
    return jax.shard_map(local, mesh=mesh, in_specs=in_specs, out_specs=out_specs, check_vma=False)
```

```python
import functools
import math

import jax
import jax.numpy as jnp
import numpy as np
from jax import lax
from jax.experimental import pallas as pl
from jax.experimental.pallas import tpu as pltpu
from jax.sharding import PartitionSpec as P

CHANNELS = 4096
TAPS = 4
ITERS = 5
EPSILON = 1e-06

COARSE = 32
FINE = 128
FEEDS_HERE = 16
BLOCKS_HERE = 32
GROUP = 8
GROUPS = BLOCKS_HERE // GROUP
PACKS = 4
OWNERS = 128
SECTIONS = 4
FEED_SETS = 32
SLOTS = SECTIONS * GROUPS
STRIDE = 17
LENGTH = BLOCKS_HERE * CHANNELS
EARLY = 2 * CHANNELS
LATE = CHANNELS


def tables():
    position = np.arange(TAPS * CHANNELS, dtype=np.float64)
    offset = (position - 0.5 * TAPS * CHANNELS + 0.5) / CHANNELS
    window = 0.5 - 0.5 * np.cos(2.0 * np.pi * (position + 0.5) / (TAPS * CHANNELS))
    taps = np.sin(np.pi * offset) / (np.pi * offset) * window
    taps = taps.reshape(TAPS * COARSE, FINE).astype(np.float32)
    angle = 2.0 * np.pi * np.outer(np.arange(COARSE), np.arange(FINE)) / CHANNELS
    twiddle = np.concatenate([np.cos(angle), np.sin(angle)], axis=0).astype(np.float32)
    angle = 2.0 * np.pi * (np.outer(np.arange(FINE), np.arange(FINE)) % FINE) / FINE
    cosine = np.cos(angle) / math.sqrt(CHANNELS)
    sine = np.sin(angle) / math.sqrt(CHANNELS)
    fine = np.block([[cosine, sine], [-sine, cosine]]).astype(np.float32)
    lane = np.arange(128)
    share = (lane[:, None] // FEEDS_HERE == lane[None, :] // FEEDS_HERE).astype(np.float32)
    return taps, twiddle, fine, share


def butterfly_4(x):
    (ar, ai), (br, bi), (cr, ci), (dr, di) = x
    pr, pi, qr, qi = ar + cr, ai + ci, ar - cr, ai - ci
    sr, si, tr, ti = br + dr, bi + di, br - dr, bi - di
    return [(pr + sr, pi + si), (qr + ti, qi - tr), (pr - sr, pi - si), (qr - ti, qi + tr)]


def turn(x, eighths_of_32):
    n = eighths_of_32 % 32
    re, im = x
    if n == 0:
        return re, im
    if n == 8:
        return im, -re
    if n == 16:
        return -re, -im
    if n == 24:
        return -im, re
    cosine, sine = math.cos(2 * math.pi * n / 32), math.sin(2 * math.pi * n / 32)
    if n % 4 == 0:
        h = math.sqrt(0.5)
        if n == 4:
            return (re + im) * h, (im - re) * h
        if n == 12:
            return (im - re) * h, (re + im) * -h
    return re * cosine + im * sine, im * cosine - re * sine


def butterfly_8(x):
    even = butterfly_4([x[0], x[2], x[4], x[6]])
    odd = butterfly_4([x[1], x[3], x[5], x[7]])
    low, high = [], []
    for k in range(4):
        er, ei = even[k]
        tr, ti = turn(odd[k], 4 * k)
        low.append((er + tr, ei + ti))
        high.append((er - tr, ei - ti))
    return low + high


def first_transform(block, ext, taps, halfway):
    start = block * CHANNELS
    for low in range(8):
        points = []
        for high in range(4):
            tile = 8 * high + low
            pair = []
            for part in range(2):
                total = None
                for tap in range(TAPS):
                    at = pl.multiple_of(start + (tap * COARSE + tile) * FINE, FINE)
                    row = tap * COARSE + tile
                    term = taps[row : row + 1, :] * ext[part, :, pl.ds(at, FINE)].astype(jnp.float32)
                    total = term if total is None else total + term
                pair.append(total)
            points.append(tuple(pair))
        for q, point in enumerate(butterfly_4(points)):
            re, im = turn(point, low * q)
            halfway[q, low, 0] = re
            halfway[q, low, 1] = im


def second_transform(twiddle, halfway, upper, lower):
    for q1 in range(4):
        points = [(halfway[q1, low, 0], halfway[q1, low, 1]) for low in range(8)]
        for q2, (re, im) in enumerate(butterfly_8(points)):
            q = q1 + 4 * q2
            if q > 0:
                cosine = twiddle[q : q + 1, :]
                sine = twiddle[COARSE + q : COARSE + q + 1, :]
                re, im = re * cosine + im * sine, im * cosine - re * sine
            for part, value in enumerate((re, im)):
                high = value.astype(jnp.bfloat16)
                low = (value - high.astype(jnp.float32)).astype(jnp.bfloat16)
                rows = slice(q * FEEDS_HERE, (q + 1) * FEEDS_HERE)
                lanes = slice(part * FINE, (part + 1) * FINE)
                upper[rows, lanes] = high
                lower[rows, lanes] = low


def fine_transform(at, fine_upper, fine_lower, upper, lower, stage):
    dims = (((1,), (1,)), ((), ()))
    for half in range(2):
        rows = slice(half * 256, (half + 1) * 256)
        high = upper[rows, :]
        low = lower[rows, :]
        out = lax.dot_general(fine_upper[...], high, dims, preferred_element_type=jnp.float32)
        out += lax.dot_general(fine_lower[...], high, dims, preferred_element_type=jnp.float32)
        out += lax.dot_general(fine_upper[...], low, dims, preferred_element_type=jnp.float32)
        for pack in range(2):
            for part in range(2):
                piece = out[part * FINE : (part + 1) * FINE, pack * 128 : (pack + 1) * 128]
                stage[2 * half + pack, pl.ds(part * GROUP + at, OWNERS, stride=STRIDE), :] = piece


def visit(section, chan, action):
    row, column = lax.div(chan, 8), lax.rem(lax.div(chan, 2), 4)

    def turns(near, core):
        x = [lax.rem(section + near[0] + 2 * far, SECTIONS) for far in range(2)]
        y = [lax.rem(row + near[1] + 2 * far, 4) * 8 for far in range(2)]
        z = [lax.rem(column + near[2] + 2 * far, 4) * 2 + core for far in range(2)]
        return x, y, z

    def several(x, y, z, skip):
        for step in range(skip, 8):
            action(x[step % 2], y[step // 2 % 2] + z[step // 4])

    same = lax.rem(chan, 2)
    several(*turns((0, 0, 0), same), 1)

    def body(step, carry):
        near = [lax.rem(step, 2), lax.rem(lax.div(step, 2), 2), lax.rem(lax.div(step, 4), 2)]
        core = lax.rem(same + lax.div(step, 8), 2)
        several(*turns(near, core), 0)
        return carry

    lax.fori_loop(1, 16, body, 0)


def copy_at(source, target, sems, at, device):
    return pltpu.make_async_remote_copy(
        src_ref=source,
        dst_ref=target,
        send_sem=sems[0].at[at],
        recv_sem=sems[1].at[at],
        device_id=device,
        device_id_type=pl.DeviceIdType.MESH,
    )


def share_dot(value, share):
    high = value.astype(jnp.bfloat16)
    low = (value - high.astype(jnp.float32)).astype(jnp.bfloat16)
    total = jnp.dot(high, share, preferred_element_type=jnp.float32)
    return total + jnp.dot(low, share, preferred_element_type=jnp.float32)


def solve_packs(tile, first, count, weight, power, share, x, y, coeff, squares, diag):
    own = pl.ds(pl.multiple_of(first * FEED_SETS, FEED_SETS), count * FEED_SETS)

    def diagonal(feed_set, carry):
        for pack in range(count):
            total = [jnp.zeros((GROUP, 128), jnp.float32) for _ in range(4)]
            for slot in range(SLOTS):
                re, im = tile(pack, slot, feed_set)
                at = slot % 2
                total[at] = total[at] + re * re
                total[2 + at] = total[2 + at] + im * im
            total = (total[0] + total[1]) + (total[2] + total[3])
            at = pl.ds(pack * FEED_SETS + feed_set, 1)
            diag[at, :] = jnp.sum(total, axis=0, keepdims=True)
        return carry

    lax.fori_loop(0, FEED_SETS, diagonal, 0)
    span = slice(0, count * FEED_SETS)
    diag[span, :] = float(SLOTS * GROUP) * power[own, :] - diag[span, :]
    x[0, span, :] = weight[own, :]
    x[1, span, :] = jnp.zeros((count * FEED_SETS, 128), jnp.float32)
    squares[...] = jnp.zeros_like(squares)

    def lengths():
        total = share_dot(squares[...], share[...])
        return [jnp.sqrt(total[8 * pack : 8 * pack + 1] + EPSILON) for pack in range(count)]

    def iterate(iteration, carry):
        for pack in range(count):

            def forward(index, inner):
                pr = [jnp.zeros((GROUP, 128), jnp.float32) for _ in range(4)]
                pi = [jnp.zeros((GROUP, 128), jnp.float32) for _ in range(4)]
                for feed_set in range(FEED_SETS):
                    at = pack * FEED_SETS + feed_set
                    xr = x[0, at : at + 1, :]
                    xi = x[1, at : at + 1, :]
                    for two in range(2):
                        re, im = tile(pack, index * 2 + two, feed_set)
                        pr[two] = pr[two] + re * xr
                        pr[2 + two] = pr[2 + two] + im * xi
                        pi[two] = pi[two] + re * xi
                        pi[2 + two] = pi[2 + two] - im * xr
                at = pl.multiple_of((pack * SLOTS + index * 2) * GROUP, 2 * GROUP)
                for two in range(2):
                    coeff[0, pl.ds(at + two * GROUP, GROUP), :] = pr[two] + pr[2 + two]
                    coeff[1, pl.ds(at + two * GROUP, GROUP), :] = pi[two] + pi[2 + two]
                return inner

            lax.fori_loop(0, SLOTS // 2, forward, 0)
        inverse = [jnp.where(iteration == 0, 1.0, 1.0 / length) for length in lengths()]
        for pack in range(count):
            rows = slice(pack * SLOTS * GROUP, (pack + 1) * SLOTS * GROUP)
            for part in range(2):
                coeff[part, rows, :] = share_dot(coeff[part, rows, :], share[...]) * inverse[pack]
        for pack in range(count):

            def backward(index, inner):
                yr = [jnp.zeros((GROUP, 128), jnp.float32) for _ in range(8)]
                yi = [jnp.zeros((GROUP, 128), jnp.float32) for _ in range(8)]
                for slot in range(SLOTS):
                    at = (pack * SLOTS + slot) * GROUP
                    pr = coeff[0, at : at + GROUP, :]
                    pi = coeff[1, at : at + GROUP, :]
                    for two in range(4):
                        re, im = tile(pack, slot, index * 4 + two)
                        yr[two] = yr[two] + re * pr
                        yr[4 + two] = yr[4 + two] - im * pi
                        yi[two] = yi[two] + re * pi
                        yi[4 + two] = yi[4 + two] + im * pr
                for two in range(4):
                    at = pl.ds(pack * FEED_SETS + index * 4 + two, 1)
                    y[0, at, :] = jnp.sum(yr[two] + yr[4 + two], axis=0, keepdims=True)
                    y[1, at, :] = jnp.sum(yi[two] + yi[4 + two], axis=0, keepdims=True)
                return inner

            lax.fori_loop(0, FEED_SETS // 4, backward, 0)
        for pack in range(count):
            here = slice(pack * FEED_SETS, (pack + 1) * FEED_SETS)
            at = pl.ds(pl.multiple_of((first + pack) * FEED_SETS, FEED_SETS), FEED_SETS)
            w = weight[at, :]
            scaled = w * (diag[here, :] * (w * inverse[pack]))
            total = jnp.zeros((8, 128), jnp.float32)
            for part in range(2):
                value = w * y[part, here, :] + scaled * x[part, here, :]
                x[part, here, :] = value
                for row in range(0, FEED_SETS, 8):
                    total = total + value[row : row + 8] * value[row : row + 8]
            total = jnp.sum(total, axis=0, keepdims=True)
            squares[8 * pack : 8 * pack + 8, :] = jnp.broadcast_to(total, (8, 128))
        return carry

    lax.fori_loop(0, ITERS, iterate, 0)
    for pack, length in enumerate(lengths()):
        here = slice(pack * FEED_SETS, (pack + 1) * FEED_SETS)
        for part in range(2):
            x[part, here, :] = x[part, here, :] / jnp.sqrt(length)


def kernel(
    volt, taps, twiddle, fine_upper, fine_lower, usable, auto_power, share, repeat, out,
    weight, power, lined, ext, halfway, upper, lower, stage, sent_pair, sent_one, held_pair, held_one,
    x, y, coeff, squares, diag, loads, send_sems, recv_sems, edge_sems,
):
    def arrange(source, target, split):
        feeds = FEED_SETS * FEEDS_HERE
        lane = lax.broadcasted_iota(jnp.int32, (FEED_SETS, feeds), 1)
        first = lax.broadcasted_iota(jnp.int32, (FEED_SETS, feeds), 0) * FEEDS_HERE
        mine = (lane >= first) & (lane < first + FEEDS_HERE)
        place = lax.broadcasted_iota(jnp.int32, (FEED_SETS, 128), 1)

        def body(pack, carry):
            for q in range(8):
                row = source[pl.ds(pack * 8 + q, 1), :].astype(jnp.float32)
                lined[q * FEED_SETS : (q + 1) * FEED_SETS, :] = jnp.where(mine, row, 0.0)
            value = lined[...]
            high = value.astype(jnp.bfloat16)
            wide = jnp.dot(high, repeat[...], preferred_element_type=jnp.float32)
            if split:
                rest = value - high.astype(jnp.float32)
                middle = rest.astype(jnp.bfloat16)
                low = (rest - middle.astype(jnp.float32)).astype(jnp.bfloat16)
                wide = wide + jnp.dot(middle, repeat[...], preferred_element_type=jnp.float32)
                wide = wide + jnp.dot(low, repeat[...], preferred_element_type=jnp.float32)
            total = jnp.zeros((FEED_SETS, 128), jnp.float32)
            for q in range(8):
                part = wide[q * FEED_SETS : (q + 1) * FEED_SETS]
                own = (place >= q * FEEDS_HERE) & (place < (q + 1) * FEEDS_HERE)
                total = total + jnp.where(own, part, 0.0)
            target[pl.ds(pl.multiple_of(pack * FEED_SETS, FEED_SETS), FEED_SETS), :] = total
            return carry

        lax.fori_loop(0, PACKS, body, 0)

    section = lax.axis_index("section")
    chan = lax.axis_index("chan")
    me = section * FEED_SETS + chan
    sems = (send_sems, recv_sems)
    load = pltpu.make_async_copy(volt, ext.at[:, :, pl.ds(EARLY, LENGTH)], loads)
    load.start()
    barrier = pltpu.get_barrier_semaphore()

    def greet(there, column):
        pl.semaphore_signal(
            barrier, inc=1, device_id=(there, column), device_id_type=pl.DeviceIdType.MESH
        )

    visit(section, chan, greet)
    early = copy_at(
        volt.at[:, :, pl.ds(LENGTH - EARLY, EARLY)],
        ext.at[:, :, pl.ds(0, EARLY)],
        (edge_sems, edge_sems.at[pl.ds(2, 2)]),
        0,
        (lax.rem(section + 1, SECTIONS), chan),
    )
    late = copy_at(
        volt.at[:, :, pl.ds(0, LATE)],
        ext.at[:, :, pl.ds(EARLY + LENGTH, LATE)],
        (edge_sems, edge_sems.at[pl.ds(2, 2)]),
        1,
        (lax.rem(section + SECTIONS - 1, SECTIONS), chan),
    )
    pl.semaphore_wait(barrier, OWNERS - 1)
    early.start()
    late.start()
    arrange(usable, weight, False)
    load.wait()

    def clear(first, count):
        def body(at, inner):
            where = pl.ds(pl.multiple_of(first * CHANNELS + at * FINE, FINE), FINE)
            for part in range(2):
                ext[part, :, where] = jnp.zeros((FEEDS_HERE, FINE), jnp.bfloat16)
            return inner

        lax.fori_loop(0, count * COARSE, body, 0)

    def grouped(position, carry):
        group = lax.rem(position + 1, GROUPS)

        @pl.when(position == 2)
        def _():
            late.wait()

        @pl.when(position == 3)
        def _():
            early.wait()

            @pl.when(section == 0)
            def _():
                clear(0, 2)

        def step(at, inner):
            @pl.when((section == SECTIONS - 1) & (position == 2) & (at == GROUP - 1))
            def _():
                clear(BLOCKS_HERE - 1, TAPS - 1)

            first_transform(group * GROUP + at, ext, taps, halfway)
            second_transform(twiddle, halfway, upper, lower)
            fine_transform(at, fine_upper, fine_lower, upper, lower, stage)
            return inner

        lax.fori_loop(0, GROUP, step, 0)

        def emit(owner, inner):
            rows = pl.ds(owner * STRIDE, 16)
            for pack in range(2):
                sent_pair[owner, group, pack] = stage[pack, rows, :].astype(jnp.bfloat16)
                sent_one[pack, owner, group] = stage[2 + pack, rows, :].astype(jnp.bfloat16)
            return inner

        lax.fori_loop(0, OWNERS, emit, 0, unroll=8)

        def send(there, column):
            source = sent_pair.at[there * FEED_SETS + column, group]
            copy_at(source, held_pair.at[me, group], sems, 0, (there, column)).start()

        visit(section, chan, send)
        return carry

    lax.fori_loop(0, GROUPS, grouped, 0)

    def rest(pack, carry):
        def send(there, column):
            source = sent_one.at[pack, there * FEED_SETS + column]
            copy_at(source, held_one.at[pack, me], sems, 1 + pack, (there, column)).start()

        visit(section, chan, send)
        return carry

    lax.fori_loop(0, 2, rest, 0)
    arrange(auto_power, power, True)

    for group in range(GROUPS):
        for pack in range(2):
            held_pair[me, group, pack] = sent_pair[me, group, pack]
            held_one[pack, me, group] = sent_one[pack, me, group]

    others = pl.ds(0, OWNERS - 1)
    pltpu.make_async_copy(sent_pair.at[others], held_pair.at[others], recv_sems.at[0]).wait()

    def tile_pair(pack, slot, feed_set):
        source = lax.div(slot, GROUPS) * FEED_SETS + feed_set
        value = held_pair[source, lax.rem(slot, GROUPS), pack].astype(jnp.float32)
        return value[0:GROUP], value[GROUP:]

    solve_packs(tile_pair, 0, 2, weight, power, share, x, y, coeff, squares, diag)
    out[:, 0 : 2 * FEED_SETS, :] = x[...]

    def single(index, carry):
        pltpu.make_async_copy(
            sent_one.at[0, others], held_one.at[index, others], recv_sems.at[1 + index]
        ).wait()

        def tile_one(pack, slot, feed_set):
            source = lax.div(slot, GROUPS) * FEED_SETS + feed_set
            value = held_one[index, source, lax.rem(slot, GROUPS)].astype(jnp.float32)
            return value[0:GROUP], value[GROUP:]

        solve_packs(tile_one, 2 + index, 1, weight, power, share, x, y, coeff, squares, diag)
        at = pl.multiple_of((2 + index) * FEED_SETS, FEED_SETS)
        out[:, pl.ds(at, FEED_SETS), :] = x[:, 0:FEED_SETS, :]
        return carry

    lax.fori_loop(0, 2, single, 0)
    pltpu.make_async_copy(sent_pair.at[others], held_pair.at[others], send_sems.at[0]).wait()
    for pack in range(2):
        pltpu.make_async_copy(
            sent_one.at[pack, others], held_one.at[pack, others], send_sems.at[1 + pack]
        ).wait()


def local(voltages, usable, auto_power):
    taps, twiddle, fine, share = tables()
    upper = fine.astype(jnp.bfloat16)
    lower = (fine - upper.astype(np.float32)).astype(jnp.bfloat16)
    rows = PACKS * FEED_SETS

    lane = np.arange(FEED_SETS * FEEDS_HERE)[:, None] % FEEDS_HERE
    repeat = (lane == np.arange(128)[None, :] % FEEDS_HERE).astype(jnp.bfloat16)
    vmem = pl.BlockSpec(memory_space=pltpu.VMEM)
    pair = pltpu.VMEM((OWNERS, GROUPS, 2, 16, 128), jnp.bfloat16)
    one = pltpu.VMEM((2, OWNERS, GROUPS, 16, 128), jnp.bfloat16)
    gains = pl.pallas_call(
        kernel,
        out_shape=jax.ShapeDtypeStruct((2, rows, 128), jnp.float32),
        in_specs=[pl.BlockSpec(memory_space=pl.ANY)] + [vmem] * 8,
        out_specs=vmem,
        scratch_shapes=[
            pltpu.VMEM((rows, 128), jnp.float32),
            pltpu.VMEM((rows, 128), jnp.float32),
            pltpu.VMEM((8 * FEED_SETS, FEED_SETS * FEEDS_HERE), jnp.float32),
            pltpu.VMEM((2, FEEDS_HERE, EARLY + LENGTH + LATE), jnp.bfloat16),
            pltpu.VMEM((4, 8, 2, FEEDS_HERE, FINE), jnp.float32),
            pltpu.VMEM((COARSE * FEEDS_HERE, 256), jnp.bfloat16),
            pltpu.VMEM((COARSE * FEEDS_HERE, 256), jnp.bfloat16),
            pltpu.VMEM((PACKS, OWNERS * STRIDE + 8, 128), jnp.float32),
            pair,
            one,
            pair,
            one,
            pltpu.VMEM((2, 2 * FEED_SETS, 128), jnp.float32),
            pltpu.VMEM((2, 2 * FEED_SETS, 128), jnp.float32),
            pltpu.VMEM((2, 2 * SLOTS * GROUP, 128), jnp.float32),
            pltpu.VMEM((16, 128), jnp.float32),
            pltpu.VMEM((2 * FEED_SETS, 128), jnp.float32),
            pltpu.SemaphoreType.DMA,
            pltpu.SemaphoreType.DMA((3,)),
            pltpu.SemaphoreType.DMA((3,)),
            pltpu.SemaphoreType.DMA((4,)),
        ],
        compiler_params=pltpu.CompilerParams(
            collective_id=0, has_side_effects=True, vmem_limit_bytes=56 * 1024 * 1024
        ),
        cost_estimate=pl.CostEstimate(flops=10**10, bytes_accessed=2 * 10**7, transcendentals=0),
    )(
        voltages, taps, twiddle, upper, lower,
        usable, auto_power, share.astype(jnp.bfloat16), repeat,
    )
    gains = gains.reshape(2, PACKS, FEED_SETS, 8, FEEDS_HERE).transpose(0, 1, 3, 2, 4)
    return gains.reshape(2, PACKS * 8, FEED_SETS * FEEDS_HERE)


def solution(mesh):
    in_specs = (
        P(None, "chan", "section"),
        P(("section", "chan"), None),
        P(("section", "chan"), None),
    )
    out_specs = P(None, ("section", "chan"), None)
    return jax.shard_map(local, mesh=mesh, in_specs=in_specs, out_specs=out_specs, check_vma=False)
```

```python
import functools
import math

import jax
import jax.numpy as jnp
import numpy as np
from jax import lax
from jax.experimental import pallas as pl
from jax.experimental.pallas import tpu as pltpu
from jax.sharding import PartitionSpec as P

CHANNELS = 4096
TAPS = 4
ITERS = 5
EPSILON = 1e-06

COARSE = 32
FINE = 128
FEEDS_HERE = 16
BLOCKS_HERE = 32
GROUP = 8
GROUPS = BLOCKS_HERE // GROUP
PACKS = 4
OWNERS = 128
SECTIONS = 4
FEED_SETS = 32
SLOTS = SECTIONS * GROUPS
STRIDE = 17
LENGTH = BLOCKS_HERE * CHANNELS
HALO = TAPS - 1


def tables():
    position = np.arange(TAPS * CHANNELS, dtype=np.float64)
    offset = (position - 0.5 * TAPS * CHANNELS + 0.5) / CHANNELS
    window = 0.5 - 0.5 * np.cos(2.0 * np.pi * (position + 0.5) / (TAPS * CHANNELS))
    taps = np.sin(np.pi * offset) / (np.pi * offset) * window
    taps = taps.reshape(TAPS * COARSE, FINE).astype(np.float32)
    angle = 2.0 * np.pi * np.outer(np.arange(COARSE), np.arange(FINE)) / CHANNELS
    twiddle = np.concatenate([np.cos(angle), np.sin(angle)], axis=0).astype(np.float32)
    angle = 2.0 * np.pi * (np.outer(np.arange(FINE), np.arange(FINE)) % FINE) / FINE
    cosine = np.cos(angle) / math.sqrt(CHANNELS)
    sine = np.sin(angle) / math.sqrt(CHANNELS)
    fine = np.block([[cosine, sine], [-sine, cosine]]).astype(np.float32)
    lane = np.arange(128)
    share = (lane[:, None] // FEEDS_HERE == lane[None, :] // FEEDS_HERE).astype(np.float32)
    return taps, twiddle, fine, share


def butterfly_4(x):
    (ar, ai), (br, bi), (cr, ci), (dr, di) = x
    pr, pi, qr, qi = ar + cr, ai + ci, ar - cr, ai - ci
    sr, si, tr, ti = br + dr, bi + di, br - dr, bi - di
    return [(pr + sr, pi + si), (qr + ti, qi - tr), (pr - sr, pi - si), (qr - ti, qi + tr)]


def turn(x, eighths_of_32):
    n = eighths_of_32 % 32
    re, im = x
    if n == 0:
        return re, im
    if n == 8:
        return im, -re
    if n == 16:
        return -re, -im
    if n == 24:
        return -im, re
    cosine, sine = math.cos(2 * math.pi * n / 32), math.sin(2 * math.pi * n / 32)
    if n % 4 == 0:
        h = math.sqrt(0.5)
        if n == 4:
            return (re + im) * h, (im - re) * h
        if n == 12:
            return (im - re) * h, (re + im) * -h
    return re * cosine + im * sine, im * cosine - re * sine


def butterfly_8(x):
    even = butterfly_4([x[0], x[2], x[4], x[6]])
    odd = butterfly_4([x[1], x[3], x[5], x[7]])
    low, high = [], []
    for k in range(4):
        er, ei = even[k]
        tr, ti = turn(odd[k], 4 * k)
        low.append((er + tr, ei + ti))
        high.append((er - tr, ei - ti))
    return low + high


def first_transform(block, ext, taps, halfway):
    start = block * CHANNELS
    for low in range(8):
        points = []
        for high in range(4):
            tile = 8 * high + low
            pair = []
            for part in range(2):
                total = None
                for tap in range(TAPS):
                    at = pl.multiple_of(start + (tap * COARSE + tile) * FINE, FINE)
                    row = tap * COARSE + tile
                    term = taps[row : row + 1, :] * ext[part, :, pl.ds(at, FINE)].astype(jnp.float32)
                    total = term if total is None else total + term
                pair.append(total)
            points.append(tuple(pair))
        for q, point in enumerate(butterfly_4(points)):
            re, im = turn(point, low * q)
            halfway[q, low, 0] = re
            halfway[q, low, 1] = im


def second_transform(twiddle, halfway, upper, lower):
    for q1 in range(4):
        points = [(halfway[q1, low, 0], halfway[q1, low, 1]) for low in range(8)]
        for q2, (re, im) in enumerate(butterfly_8(points)):
            q = q1 + 4 * q2
            if q > 0:
                cosine = twiddle[q : q + 1, :]
                sine = twiddle[COARSE + q : COARSE + q + 1, :]
                re, im = re * cosine + im * sine, im * cosine - re * sine
            for part, value in enumerate((re, im)):
                high = value.astype(jnp.bfloat16)
                low = (value - high.astype(jnp.float32)).astype(jnp.bfloat16)
                rows = slice(q * FEEDS_HERE, (q + 1) * FEEDS_HERE)
                lanes = slice(part * FINE, (part + 1) * FINE)
                upper[rows, lanes] = high
                lower[rows, lanes] = low


def fine_transform(at, fine_upper, fine_lower, upper, lower, stage):
    dims = (((1,), (1,)), ((), ()))
    for half in range(2):
        rows = slice(half * 256, (half + 1) * 256)
        high = upper[rows, :]
        low = lower[rows, :]
        out = lax.dot_general(fine_upper[...], high, dims, preferred_element_type=jnp.float32)
        out += lax.dot_general(fine_lower[...], high, dims, preferred_element_type=jnp.float32)
        out += lax.dot_general(fine_upper[...], low, dims, preferred_element_type=jnp.float32)
        for pack in range(2):
            for part in range(2):
                piece = out[part * FINE : (part + 1) * FINE, pack * 128 : (pack + 1) * 128]
                stage[2 * half + pack, pl.ds(part * GROUP + at, OWNERS, stride=STRIDE), :] = piece


def visit(section, chan, action):
    row, column = lax.div(chan, 8), lax.rem(lax.div(chan, 2), 4)

    def turns(near, core):
        x = [lax.rem(section + near[0] + 2 * far, SECTIONS) for far in range(2)]
        y = [lax.rem(row + near[1] + 2 * far, 4) * 8 for far in range(2)]
        z = [lax.rem(column + near[2] + 2 * far, 4) * 2 + core for far in range(2)]
        return x, y, z

    def several(x, y, z, skip):
        for step in range(skip, 8):
            action(x[step % 2], y[step // 2 % 2] + z[step // 4])

    same = lax.rem(chan, 2)
    several(*turns((0, 0, 0), same), 1)

    def body(step, carry):
        near = [lax.rem(step, 2), lax.rem(lax.div(step, 2), 2), lax.rem(lax.div(step, 4), 2)]
        core = lax.rem(same + lax.div(step, 8), 2)
        several(*turns(near, core), 0)
        return carry

    lax.fori_loop(1, 16, body, 0)


def copy_at(source, target, sems, at, device):
    return pltpu.make_async_remote_copy(
        src_ref=source,
        dst_ref=target,
        send_sem=sems[0].at[at],
        recv_sem=sems[1].at[at],
        device_id=device,
        device_id_type=pl.DeviceIdType.MESH,
    )


def share_dot(value, share):
    high = value.astype(jnp.bfloat16)
    low = (value - high.astype(jnp.float32)).astype(jnp.bfloat16)
    total = jnp.dot(high, share, preferred_element_type=jnp.float32)
    return total + jnp.dot(low, share, preferred_element_type=jnp.float32)


def own_rows(pack, count=1):
    return pl.ds(pl.multiple_of(pack * FEED_SETS, FEED_SETS), count * FEED_SETS)


def forward_pass(tile, count, x, coeff):
    for pack in range(count):

        def forward(index, inner):
            pr = [jnp.zeros((GROUP, 128), jnp.float32) for _ in range(8)]
            pi = [jnp.zeros((GROUP, 128), jnp.float32) for _ in range(8)]
            for feed_set in range(FEED_SETS):
                at = pack * FEED_SETS + feed_set
                xr = x[0, at : at + 1, :]
                xi = x[1, at : at + 1, :]
                for two in range(4):
                    re, im = tile(pack, index * 4 + two, feed_set)
                    pr[two] = pr[two] + re * xr
                    pr[4 + two] = pr[4 + two] + im * xi
                    pi[two] = pi[two] + re * xi
                    pi[4 + two] = pi[4 + two] - im * xr
            at = pl.multiple_of((pack * SLOTS + index * 4) * GROUP, 4 * GROUP)
            for two in range(4):
                coeff[0, pl.ds(at + two * GROUP, GROUP), :] = pr[two] + pr[4 + two]
                coeff[1, pl.ds(at + two * GROUP, GROUP), :] = pi[two] + pi[4 + two]
            return inner

        lax.fori_loop(0, SLOTS // 4, forward, 0)


def start_x(first, count, weight, x):
    span = slice(0, count * FEED_SETS)
    x[0, span, :] = weight[own_rows(first, count), :]
    x[1, span, :] = jnp.zeros((count * FEED_SETS, 128), jnp.float32)


def start_packs(tile, first, count, weight, x, coeff, diag):
    def diagonal(feed_set, carry):
        for pack in range(count):
            total = [jnp.zeros((GROUP, 128), jnp.float32) for _ in range(4)]
            for slot in range(SLOTS):
                re, im = tile(pack, slot, feed_set)
                at = slot % 2
                total[at] = total[at] + re * re
                total[2 + at] = total[2 + at] + im * im
            total = (total[0] + total[1]) + (total[2] + total[3])
            at = pl.ds(pack * FEED_SETS + feed_set, 1)
            diag[at, :] = jnp.sum(total, axis=0, keepdims=True)
        return carry

    lax.fori_loop(0, FEED_SETS, diagonal, 0)
    start_x(first, count, weight, x)
    forward_pass(tile, count, x, coeff)


def solve_packs(tile, first, count, weight, power, share, x, y, coeff, squares, diag):
    span = slice(0, count * FEED_SETS)
    diag[span, :] = float(SLOTS * GROUP) * power[own_rows(first, count), :] - diag[span, :]
    squares[...] = jnp.zeros_like(squares)

    def lengths():
        total = share_dot(squares[...], share[...])
        return [jnp.sqrt(total[8 * pack : 8 * pack + 1] + EPSILON) for pack in range(count)]

    def iterate(iteration, carry):
        inverse = [jnp.where(iteration == 0, 1.0, 1.0 / length) for length in lengths()]
        for pack in range(count):
            rows = slice(pack * SLOTS * GROUP, (pack + 1) * SLOTS * GROUP)
            for part in range(2):
                coeff[part, rows, :] = share_dot(coeff[part, rows, :], share[...]) * inverse[pack]
        for pack in range(count):

            def backward(index, inner):
                yr = [jnp.zeros((GROUP, 128), jnp.float32) for _ in range(8)]
                yi = [jnp.zeros((GROUP, 128), jnp.float32) for _ in range(8)]
                for slot in range(SLOTS):
                    at = (pack * SLOTS + slot) * GROUP
                    pr = coeff[0, at : at + GROUP, :]
                    pi = coeff[1, at : at + GROUP, :]
                    for two in range(4):
                        re, im = tile(pack, slot, index * 4 + two)
                        yr[two] = yr[two] + re * pr
                        yr[4 + two] = yr[4 + two] - im * pi
                        yi[two] = yi[two] + re * pi
                        yi[4 + two] = yi[4 + two] + im * pr
                for two in range(4):
                    at = pl.ds(pack * FEED_SETS + index * 4 + two, 1)
                    y[0, at, :] = jnp.sum(yr[two] + yr[4 + two], axis=0, keepdims=True)
                    y[1, at, :] = jnp.sum(yi[two] + yi[4 + two], axis=0, keepdims=True)
                return inner

            lax.fori_loop(0, FEED_SETS // 4, backward, 0)
        for pack in range(count):
            here = slice(pack * FEED_SETS, (pack + 1) * FEED_SETS)
            w = weight[own_rows(first + pack), :]
            scaled = w * (diag[here, :] * (w * inverse[pack]))
            total = jnp.zeros((8, 128), jnp.float32)
            for part in range(2):
                value = w * y[part, here, :] + scaled * x[part, here, :]
                x[part, here, :] = value
                for row in range(0, FEED_SETS, 8):
                    total = total + value[row : row + 8] * value[row : row + 8]
            total = jnp.sum(total, axis=0, keepdims=True)
            squares[8 * pack : 8 * pack + 8, :] = jnp.broadcast_to(total, (8, 128))

        @pl.when(iteration < ITERS - 1)
        def _():
            forward_pass(tile, count, x, coeff)

        return carry

    lax.fori_loop(0, ITERS, iterate, 0)
    for pack, length in enumerate(lengths()):
        here = slice(pack * FEED_SETS, (pack + 1) * FEED_SETS)
        for part in range(2):
            x[part, here, :] = x[part, here, :] / jnp.sqrt(length)


def kernel(
    volt, taps, twiddle, fine_upper, fine_lower, usable, auto_power, share, repeat, out,
    weight, power, lined, lined_back, wide, ext, halfway, upper, lower, stage, sent_pair, sent_one, held_pair, held_one,
    x, y, coeff, squares, diag, loads, send_sems, recv_sems, edge_sems,
):
    def arrange(source, target, split):
        feeds = FEED_SETS * FEEDS_HERE
        lane = lax.broadcasted_iota(jnp.int32, (FEED_SETS, feeds), 1)
        first = lax.broadcasted_iota(jnp.int32, (FEED_SETS, feeds), 0) * FEEDS_HERE
        mine = (lane >= first) & (lane < first + FEEDS_HERE)
        place = lax.broadcasted_iota(jnp.int32, (FEED_SETS, 128), 1)

        def body(pack, carry):
            for q in range(8):
                row = source[pl.ds(pack * 8 + q, 1), :].astype(jnp.float32)
                lined[q * FEED_SETS : (q + 1) * FEED_SETS, :] = jnp.where(mine, row, 0.0)
            value = lined[...]
            high = value.astype(jnp.bfloat16)
            wide = jnp.dot(high, repeat[...], preferred_element_type=jnp.float32)
            if split:
                rest = value - high.astype(jnp.float32)
                middle = rest.astype(jnp.bfloat16)
                low = (rest - middle.astype(jnp.float32)).astype(jnp.bfloat16)
                wide = wide + jnp.dot(middle, repeat[...], preferred_element_type=jnp.float32)
                wide = wide + jnp.dot(low, repeat[...], preferred_element_type=jnp.float32)
            total = jnp.zeros((FEED_SETS, 128), jnp.float32)
            for q in range(8):
                part = wide[q * FEED_SETS : (q + 1) * FEED_SETS]
                own = (place >= q * FEEDS_HERE) & (place < (q + 1) * FEEDS_HERE)
                total = total + jnp.where(own, part, 0.0)
            target[pl.ds(pl.multiple_of(pack * FEED_SETS, FEED_SETS), FEED_SETS), :] = total
            return carry

        lax.fori_loop(0, PACKS, body, 0)

    def arrange_back(pack, rows):
        feeds = FEED_SETS * FEEDS_HERE
        lane = lax.broadcasted_iota(jnp.int32, (FEED_SETS, feeds), 1)
        first = lax.broadcasted_iota(jnp.int32, (FEED_SETS, feeds), 0) * FEEDS_HERE
        mine = (lane >= first) & (lane < first + FEEDS_HERE)
        place = lax.broadcasted_iota(jnp.int32, (FEED_SETS, 128), 1)
        dims = (((1,), (1,)), ((), ()))
        for part in range(2):
            value = x[part, rows, :]
            for q in range(8):
                own = (place >= q * FEEDS_HERE) & (place < (q + 1) * FEEDS_HERE)
                lined_back[q * FEED_SETS : (q + 1) * FEED_SETS, :] = jnp.where(own, value, 0.0)
            rest = lined_back[...]
            total = jnp.zeros((8 * FEED_SETS, feeds), jnp.float32)
            for _ in range(3):
                piece = rest.astype(jnp.bfloat16)
                rest = rest - piece.astype(jnp.float32)
                total = total + lax.dot_general(
                    piece, repeat[...], dims, preferred_element_type=jnp.float32
                )
            for q in range(8):
                line = jnp.where(mine, total[q * FEED_SETS : (q + 1) * FEED_SETS], 0.0)
                out[part, pl.ds(pack * 8 + q, 1), :] = jnp.sum(line, axis=0, keepdims=True)

    section = lax.axis_index("section")
    chan = lax.axis_index("chan")
    core = lax.rem(chan, 2)
    before = 2 - core
    me = section * FEED_SETS + chan
    sems = (send_sems, recv_sems)
    load = pltpu.make_async_copy(
        volt, ext.at[:, :, pl.ds(pl.multiple_of(before * CHANNELS, CHANNELS), LENGTH)], loads
    )
    load.start()
    barrier = pltpu.get_barrier_semaphore()

    def greet(there, column):
        pl.semaphore_signal(
            barrier, inc=1, device_id=(there, column), device_id_type=pl.DeviceIdType.MESH
        )

    visit(section, chan, greet)
    edges = []
    for kind in range(2):
        early, late = (2 - kind) * CHANNELS, (1 + kind) * CHANNELS
        pair = (edge_sems, edge_sems.at[pl.ds(2, 2)])
        edges.append((
            copy_at(
                volt.at[:, :, pl.ds(LENGTH - early, early)],
                ext.at[:, :, pl.ds(0, early)],
                pair,
                0,
                (lax.rem(section + 1, SECTIONS), chan),
            ),
            copy_at(
                volt.at[:, :, pl.ds(0, late)],
                ext.at[:, :, pl.ds(early + LENGTH, late)],
                pair,
                1,
                (lax.rem(section + SECTIONS - 1, SECTIONS), chan),
            ),
        ))
    pl.semaphore_wait(barrier, OWNERS - 1)
    for kind in range(2):

        @pl.when(core == kind)
        def _():
            edges[kind][0].start()
            edges[kind][1].start()

    load.wait()

    def clear(first, count):
        def body(at, inner):
            where = pl.ds(pl.multiple_of(first * CHANNELS + at * FINE, FINE), FINE)
            for part in range(2):
                ext[part, :, where] = jnp.zeros((FEEDS_HERE, FINE), jnp.bfloat16)
            return inner

        lax.fori_loop(0, count * COARSE, body, 0)

    def grouped(position, carry):
        group = lax.rem(position + 1, GROUPS)

        for kind in range(2):

            @pl.when((position == 2) & (core == kind))
            def _():
                edges[kind][1].wait()

            @pl.when((position == 3) & (core == kind))
            def _():
                edges[kind][0].wait()

        @pl.when((position == 3) & (section == 0))
        def _():
            clear(0, before)

        def step(at, inner):
            @pl.when((section == SECTIONS - 1) & (position == 2) & (at == GROUP - 1))
            def _():
                clear(BLOCKS_HERE - HALO + before, HALO)

            block = lax.rem(group * GROUP + at + core * (BLOCKS_HERE - 1), BLOCKS_HERE)
            first_transform(block, ext, taps, halfway)
            second_transform(twiddle, halfway, upper, lower)
            fine_transform(at, fine_upper, fine_lower, upper, lower, stage)
            return inner

        lax.fori_loop(0, GROUP, step, 0)

        def emit(owner, inner):
            rows = pl.ds(owner * STRIDE, 16)
            for pack in range(2):
                sent_pair[owner, group, pack] = stage[pack, rows, :].astype(jnp.bfloat16)
                sent_one[pack, owner, group] = stage[2 + pack, rows, :].astype(jnp.bfloat16)
            return inner

        lax.fori_loop(0, OWNERS, emit, 0, unroll=8)

        def send(there, column):
            source = sent_pair.at[there * FEED_SETS + column, group]
            copy_at(source, held_pair.at[me, group], sems, 0, (there, column)).start()

        visit(section, chan, send)
        return carry

    lax.fori_loop(0, GROUPS, grouped, 0)

    def send_third(there, column):
        source = sent_one.at[0, there * FEED_SETS + column]
        copy_at(source, held_one.at[0, me], sems, 1, (there, column)).start()

    visit(section, chan, send_third)

    def rest(group, carry):
        def send(there, column):
            pltpu.make_async_remote_copy(
                src_ref=sent_one.at[1, there * FEED_SETS + column, group],
                dst_ref=held_one.at[1, me, group],
                send_sem=send_sems.at[2],
                recv_sem=recv_sems.at[2 + group],
                device_id=(there, column),
                device_id_type=pl.DeviceIdType.MESH,
            ).start()

        visit(section, chan, send)
        return carry

    lax.fori_loop(0, GROUPS, rest, 0)
    arrange(usable, weight, False)
    arrange(auto_power, power, True)

    for group in range(GROUPS):
        for pack in range(2):
            held_pair[me, group, pack] = sent_pair[me, group, pack]
            held_one[pack, me, group] = sent_one[pack, me, group]

    others = pl.ds(0, OWNERS - 1)
    pltpu.make_async_copy(sent_pair.at[others], held_pair.at[others], recv_sems.at[0]).wait()

    def tile_pair(pack, slot, feed_set):
        source = lax.div(slot, GROUPS) * FEED_SETS + feed_set
        value = held_pair[source, lax.rem(slot, GROUPS), pack].astype(jnp.float32)
        return value[0:GROUP], value[GROUP:]

    first_row = lax.broadcasted_iota(jnp.int32, (16, 128), 0)
    first_row = (first_row == 0) | (first_row == GROUP)

    def mend(read, write):
        def body(index, carry):
            values = [read(at * FEED_SETS + 2 * index + 1).astype(jnp.float32) for at in range(4)]
            for at in range(4):
                value = jnp.where(first_row, values[at - 1], values[at])
                write(at * FEED_SETS + 2 * index + 1, value.astype(jnp.bfloat16))
            return carry

        lax.fori_loop(0, FEED_SETS // 2, body, 0)

    for pack in range(2):

        def write_pair(source, value):
            held_pair[source, 0, pack] = value

        mend(lambda source: held_pair[source, 0, pack], write_pair)
    scratch = (weight, power, share, x, y, coeff, squares, diag)
    start_packs(tile_pair, 0, 2, weight, x, coeff, diag)
    solve_packs(tile_pair, 0, 2, *scratch)
    for pack in range(2):
        arrange_back(pack, slice(pack * FEED_SETS, (pack + 1) * FEED_SETS))

    def tile_third(pack, slot, feed_set):
        source = lax.div(slot, GROUPS) * FEED_SETS + feed_set
        value = held_one[0, source, lax.rem(slot, GROUPS)].astype(jnp.float32)
        return value[0:GROUP], value[GROUP:]

    def write_third(source, value):
        held_one[0, source, 0] = value

    pltpu.make_async_copy(
        sent_one.at[0, others], held_one.at[0, others], recv_sems.at[1]
    ).wait()
    mend(lambda source: held_one[0, source, 0], write_third)
    start_packs(tile_third, 2, 1, weight, x, coeff, diag)
    solve_packs(tile_third, 2, 1, *scratch)
    arrange_back(2, slice(0, FEED_SETS))

    def tile_last(pack, slot, feed_set):
        at = slot * FEED_SETS + feed_set
        return wide[at, 0], wide[at, 1]

    start_x(3, 1, weight, x)
    diag[0:FEED_SETS, :] = jnp.zeros((FEED_SETS, 128), jnp.float32)
    top_row = lax.broadcasted_iota(jnp.int32, (GROUP, 128), 0) == 0
    for group in range(GROUPS):
        pltpu.make_async_copy(
            sent_one.at[1, others, group], held_one.at[1, others, group], recv_sems.at[2 + group]
        ).wait()

        def arrive(index, sums):
            sums = list(sums)
            for near in range(2):
                feed_set = index * 2 + near
                weight_row = x[0, pl.ds(feed_set, 1), :]
                values = []
                for at in range(SECTIONS):
                    value = held_one[1, at * FEED_SETS + feed_set, group].astype(jnp.float32)
                    values.append((value[0:GROUP], value[GROUP:]))
                if group == 0 and near == 1:
                    values = [
                        tuple(jnp.where(top_row, values[at - 1][c], values[at][c]) for c in range(2))
                        for at in range(SECTIONS)
                    ]
                total = jnp.zeros((GROUP, 128), jnp.float32)
                for at, (re, im) in enumerate(values):
                    place = (at * GROUPS + group) * FEED_SETS + feed_set
                    wide[place, 0] = re
                    wide[place, 1] = im
                    total = total + (re * re + im * im)
                    sums[2 * at] = sums[2 * at] + re * weight_row
                    sums[2 * at + 1] = sums[2 * at + 1] - im * weight_row
                row = pl.ds(feed_set, 1)
                diag[row, :] = diag[row, :] + jnp.sum(total, axis=0, keepdims=True)
            return tuple(sums)

        zero = jnp.zeros((GROUP, 128), jnp.float32)
        sums = lax.fori_loop(0, FEED_SETS // 2, arrive, (zero,) * (2 * SECTIONS))
        for at in range(SECTIONS):
            rows = slice((at * GROUPS + group) * GROUP, (at * GROUPS + group + 1) * GROUP)
            coeff[0, rows, :] = sums[2 * at]
            coeff[1, rows, :] = sums[2 * at + 1]
    solve_packs(tile_last, 3, 1, *scratch)
    arrange_back(3, slice(0, FEED_SETS))
    pltpu.make_async_copy(sent_pair.at[others], held_pair.at[others], send_sems.at[0]).wait()
    for pack in range(2):
        pltpu.make_async_copy(
            sent_one.at[pack, others], held_one.at[pack, others], send_sems.at[1 + pack]
        ).wait()


def local(voltages, usable, auto_power):
    taps, twiddle, fine, share = tables()
    upper = fine.astype(jnp.bfloat16)
    lower = (fine - upper.astype(np.float32)).astype(jnp.bfloat16)
    rows = PACKS * FEED_SETS

    lane = np.arange(FEED_SETS * FEEDS_HERE)[:, None] % FEEDS_HERE
    repeat = (lane == np.arange(128)[None, :] % FEEDS_HERE).astype(jnp.bfloat16)
    vmem = pl.BlockSpec(memory_space=pltpu.VMEM)
    pair = pltpu.VMEM((OWNERS, GROUPS, 2, 16, 128), jnp.bfloat16)
    one = pltpu.VMEM((2, OWNERS, GROUPS, 16, 128), jnp.bfloat16)
    return pl.pallas_call(
        kernel,
        out_shape=jax.ShapeDtypeStruct((2, PACKS * 8, FEED_SETS * FEEDS_HERE), jnp.float32),
        in_specs=[pl.BlockSpec(memory_space=pl.ANY)] + [vmem] * 8,
        out_specs=vmem,
        scratch_shapes=[
            pltpu.VMEM((rows, 128), jnp.float32),
            pltpu.VMEM((rows, 128), jnp.float32),
            pltpu.VMEM((8 * FEED_SETS, FEED_SETS * FEEDS_HERE), jnp.float32),
            pltpu.VMEM((8 * FEED_SETS, 128), jnp.float32),
            pltpu.VMEM((SLOTS * FEED_SETS, 2, GROUP, 128), jnp.float32),
            pltpu.VMEM((2, FEEDS_HERE, LENGTH + HALO * CHANNELS), jnp.bfloat16),
            pltpu.VMEM((4, 8, 2, FEEDS_HERE, FINE), jnp.float32),
            pltpu.VMEM((COARSE * FEEDS_HERE, 256), jnp.bfloat16),
            pltpu.VMEM((COARSE * FEEDS_HERE, 256), jnp.bfloat16),
            pltpu.VMEM((PACKS, OWNERS * STRIDE + 8, 128), jnp.float32),
            pair,
            one,
            pair,
            one,
            pltpu.VMEM((2, 2 * FEED_SETS, 128), jnp.float32),
            pltpu.VMEM((2, 2 * FEED_SETS, 128), jnp.float32),
            pltpu.VMEM((2, 2 * SLOTS * GROUP, 128), jnp.float32),
            pltpu.VMEM((16, 128), jnp.float32),
            pltpu.VMEM((2 * FEED_SETS, 128), jnp.float32),
            pltpu.SemaphoreType.DMA,
            pltpu.SemaphoreType.DMA((3,)),
            pltpu.SemaphoreType.DMA((2 + GROUPS,)),
            pltpu.SemaphoreType.DMA((4,)),
        ],
        compiler_params=pltpu.CompilerParams(
            collective_id=0, has_side_effects=True, vmem_limit_bytes=56 * 1024 * 1024
        ),
        cost_estimate=pl.CostEstimate(flops=10**10, bytes_accessed=2 * 10**7, transcendentals=0),
    )(
        voltages, taps, twiddle, upper, lower,
        usable, auto_power, share.astype(jnp.bfloat16), repeat,
    )


def solution(mesh):
    in_specs = (
        P(None, "chan", "section"),
        P(("section", "chan"), None),
        P(("section", "chan"), None),
    )
    out_specs = P(None, ("section", "chan"), None)
    return jax.shard_map(local, mesh=mesh, in_specs=in_specs, out_specs=out_specs, check_vma=False)
```

```python
import functools
import math

import jax
import jax.numpy as jnp
import numpy as np
from jax import lax
from jax.experimental import pallas as pl
from jax.experimental.pallas import tpu as pltpu
from jax.sharding import PartitionSpec as P

CHANNELS = 4096
TAPS = 4
ITERS = 5
EPSILON = 1e-06

COARSE = 32
FINE = 128
FEEDS_HERE = 16
BLOCKS_HERE = 32
GROUP = 8
GROUPS = BLOCKS_HERE // GROUP
PACKS = 4
OWNERS = 128
SECTIONS = 4
FEED_SETS = 32
SLOTS = SECTIONS * GROUPS
STRIDE = 17
LENGTH = BLOCKS_HERE * CHANNELS
HALO = TAPS - 1


def tables():
    position = np.arange(TAPS * CHANNELS, dtype=np.float64)
    offset = (position - 0.5 * TAPS * CHANNELS + 0.5) / CHANNELS
    window = 0.5 - 0.5 * np.cos(2.0 * np.pi * (position + 0.5) / (TAPS * CHANNELS))
    taps = np.sin(np.pi * offset) / (np.pi * offset) * window
    taps = taps.reshape(TAPS * COARSE, FINE).astype(np.float32)
    angle = 2.0 * np.pi * np.outer(np.arange(COARSE), np.arange(FINE)) / CHANNELS
    twiddle = np.concatenate([np.cos(angle), np.sin(angle)], axis=0).astype(np.float32)
    angle = 2.0 * np.pi * (np.outer(np.arange(FINE), np.arange(FINE)) % FINE) / FINE
    cosine = np.cos(angle) / math.sqrt(CHANNELS)
    sine = np.sin(angle) / math.sqrt(CHANNELS)
    fine = np.block([[cosine, sine], [-sine, cosine]]).astype(np.float32)
    lane = np.arange(128)
    share = (lane[:, None] // FEEDS_HERE == lane[None, :] // FEEDS_HERE).astype(np.float32)
    return taps, twiddle, fine, share


def butterfly_4(x):
    (ar, ai), (br, bi), (cr, ci), (dr, di) = x
    pr, pi, qr, qi = ar + cr, ai + ci, ar - cr, ai - ci
    sr, si, tr, ti = br + dr, bi + di, br - dr, bi - di
    return [(pr + sr, pi + si), (qr + ti, qi - tr), (pr - sr, pi - si), (qr - ti, qi + tr)]


def turn(x, eighths_of_32):
    n = eighths_of_32 % 32
    re, im = x
    if n == 0:
        return re, im
    if n == 8:
        return im, -re
    if n == 16:
        return -re, -im
    if n == 24:
        return -im, re
    cosine, sine = math.cos(2 * math.pi * n / 32), math.sin(2 * math.pi * n / 32)
    if n % 4 == 0:
        h = math.sqrt(0.5)
        if n == 4:
            return (re + im) * h, (im - re) * h
        if n == 12:
            return (im - re) * h, (re + im) * -h
    return re * cosine + im * sine, im * cosine - re * sine


def butterfly_8(x):
    even = butterfly_4([x[0], x[2], x[4], x[6]])
    odd = butterfly_4([x[1], x[3], x[5], x[7]])
    low, high = [], []
    for k in range(4):
        er, ei = even[k]
        tr, ti = turn(odd[k], 4 * k)
        low.append((er + tr, ei + ti))
        high.append((er - tr, ei - ti))
    return low + high


def first_transform(block, ext, taps, halfway):
    start = block * CHANNELS
    for low in range(8):
        points = []
        for high in range(4):
            tile = 8 * high + low
            pair = []
            for part in range(2):
                total = None
                for tap in range(TAPS):
                    at = pl.multiple_of(start + (tap * COARSE + tile) * FINE, FINE)
                    row = tap * COARSE + tile
                    term = taps[row : row + 1, :] * ext[part, :, pl.ds(at, FINE)].astype(jnp.float32)
                    total = term if total is None else total + term
                pair.append(total)
            points.append(tuple(pair))
        for q, point in enumerate(butterfly_4(points)):
            re, im = turn(point, low * q)
            halfway[q, low, 0] = re
            halfway[q, low, 1] = im


def second_transform(twiddle, halfway, upper, lower):
    for q1 in range(4):
        points = [(halfway[q1, low, 0], halfway[q1, low, 1]) for low in range(8)]
        for q2, (re, im) in enumerate(butterfly_8(points)):
            q = q1 + 4 * q2
            if q > 0:
                cosine = twiddle[q : q + 1, :]
                sine = twiddle[COARSE + q : COARSE + q + 1, :]
                re, im = re * cosine + im * sine, im * cosine - re * sine
            for part, value in enumerate((re, im)):
                high = value.astype(jnp.bfloat16)
                low = (value - high.astype(jnp.float32)).astype(jnp.bfloat16)
                rows = slice(q * FEEDS_HERE, (q + 1) * FEEDS_HERE)
                lanes = slice(part * FINE, (part + 1) * FINE)
                upper[rows, lanes] = high
                lower[rows, lanes] = low


def fine_transform(at, fine_upper, fine_lower, upper, lower, stage):
    dims = (((1,), (1,)), ((), ()))
    for half in range(2):
        rows = slice(half * 256, (half + 1) * 256)
        high = upper[rows, :]
        low = lower[rows, :]
        out = lax.dot_general(fine_upper[...], high, dims, preferred_element_type=jnp.float32)
        out += lax.dot_general(fine_lower[...], high, dims, preferred_element_type=jnp.float32)
        out += lax.dot_general(fine_upper[...], low, dims, preferred_element_type=jnp.float32)
        for pack in range(2):
            for part in range(2):
                piece = out[part * FINE : (part + 1) * FINE, pack * 128 : (pack + 1) * 128]
                stage[2 * half + pack, pl.ds(part * GROUP + at, OWNERS, stride=STRIDE), :] = piece


def visit(section, chan, action):
    row, column = lax.div(chan, 8), lax.rem(lax.div(chan, 2), 4)

    def turns(near, core):
        x = [lax.rem(section + near[0] + 2 * far, SECTIONS) for far in range(2)]
        y = [lax.rem(row + near[1] + 2 * far, 4) * 8 for far in range(2)]
        z = [lax.rem(column + near[2] + 2 * far, 4) * 2 + core for far in range(2)]
        return x, y, z

    def several(x, y, z, skip):
        for step in range(skip, 8):
            action(x[step % 2], y[step // 2 % 2] + z[step // 4])

    same = lax.rem(chan, 2)
    several(*turns((0, 0, 0), same), 1)

    def body(step, carry):
        near = [lax.rem(step, 2), lax.rem(lax.div(step, 2), 2), lax.rem(lax.div(step, 4), 2)]
        core = lax.rem(same + lax.div(step, 8), 2)
        several(*turns(near, core), 0)
        return carry

    lax.fori_loop(1, 16, body, 0)


def copy_at(source, target, sems, at, device):
    return pltpu.make_async_remote_copy(
        src_ref=source,
        dst_ref=target,
        send_sem=sems[0].at[at],
        recv_sem=sems[1].at[at],
        device_id=device,
        device_id_type=pl.DeviceIdType.MESH,
    )


def share_dot(value, share):
    high = value.astype(jnp.bfloat16)
    low = (value - high.astype(jnp.float32)).astype(jnp.bfloat16)
    total = jnp.dot(high, share, preferred_element_type=jnp.float32)
    return total + jnp.dot(low, share, preferred_element_type=jnp.float32)


def own_rows(pack, count=1):
    return pl.ds(pl.multiple_of(pack * FEED_SETS, FEED_SETS), count * FEED_SETS)


def forward_pass(tile, count, x, coeff):
    for pack in range(count):

        def forward(index, inner):
            pr = [jnp.zeros((GROUP, 128), jnp.float32) for _ in range(8)]
            pi = [jnp.zeros((GROUP, 128), jnp.float32) for _ in range(8)]
            for feed_set in range(FEED_SETS):
                at = pack * FEED_SETS + feed_set
                xr = x[0, at : at + 1, :]
                xi = x[1, at : at + 1, :]
                for two in range(4):
                    re, im = tile(pack, index * 4 + two, feed_set)
                    pr[two] = pr[two] + re * xr
                    pr[4 + two] = pr[4 + two] + im * xi
                    pi[two] = pi[two] + re * xi
                    pi[4 + two] = pi[4 + two] - im * xr
            at = pl.multiple_of((pack * SLOTS + index * 4) * GROUP, 4 * GROUP)
            for two in range(4):
                coeff[0, pl.ds(at + two * GROUP, GROUP), :] = pr[two] + pr[4 + two]
                coeff[1, pl.ds(at + two * GROUP, GROUP), :] = pi[two] + pi[4 + two]
            return inner

        lax.fori_loop(0, SLOTS // 4, forward, 0)


def start_x(first, count, weight, x):
    span = slice(0, count * FEED_SETS)
    x[0, span, :] = weight[own_rows(first, count), :]
    x[1, span, :] = jnp.zeros((count * FEED_SETS, 128), jnp.float32)


def solve_packs(tile, first, count, weight, power, share, x, y, coeff, squares, diag):
    span = slice(0, count * FEED_SETS)
    diag[span, :] = float(SLOTS * GROUP) * power[own_rows(first, count), :] - diag[span, :]
    squares[...] = jnp.zeros_like(squares)

    def lengths():
        total = share_dot(squares[...], share[...])
        return [jnp.sqrt(total[8 * pack : 8 * pack + 1] + EPSILON) for pack in range(count)]

    def iterate(iteration, carry):
        inverse = [jnp.where(iteration == 0, 1.0, 1.0 / length) for length in lengths()]
        for pack in range(count):
            rows = slice(pack * SLOTS * GROUP, (pack + 1) * SLOTS * GROUP)
            for part in range(2):
                coeff[part, rows, :] = share_dot(coeff[part, rows, :], share[...]) * inverse[pack]
        for pack in range(count):

            def backward(index, inner):
                yr = [jnp.zeros((GROUP, 128), jnp.float32) for _ in range(8)]
                yi = [jnp.zeros((GROUP, 128), jnp.float32) for _ in range(8)]
                for slot in range(SLOTS):
                    at = (pack * SLOTS + slot) * GROUP
                    pr = coeff[0, at : at + GROUP, :]
                    pi = coeff[1, at : at + GROUP, :]
                    for two in range(4):
                        re, im = tile(pack, slot, index * 4 + two)
                        yr[two] = yr[two] + re * pr
                        yr[4 + two] = yr[4 + two] - im * pi
                        yi[two] = yi[two] + re * pi
                        yi[4 + two] = yi[4 + two] + im * pr
                for two in range(4):
                    at = pl.ds(pack * FEED_SETS + index * 4 + two, 1)
                    y[0, at, :] = jnp.sum(yr[two] + yr[4 + two], axis=0, keepdims=True)
                    y[1, at, :] = jnp.sum(yi[two] + yi[4 + two], axis=0, keepdims=True)
                return inner

            lax.fori_loop(0, FEED_SETS // 4, backward, 0)
        for pack in range(count):
            here = slice(pack * FEED_SETS, (pack + 1) * FEED_SETS)
            w = weight[own_rows(first + pack), :]
            scaled = w * (diag[here, :] * (w * inverse[pack]))
            total = jnp.zeros((8, 128), jnp.float32)
            for part in range(2):
                value = w * y[part, here, :] + scaled * x[part, here, :]
                x[part, here, :] = value
                for row in range(0, FEED_SETS, 8):
                    total = total + value[row : row + 8] * value[row : row + 8]
            total = jnp.sum(total, axis=0, keepdims=True)
            squares[8 * pack : 8 * pack + 8, :] = jnp.broadcast_to(total, (8, 128))

        @pl.when(iteration < ITERS - 1)
        def _():
            forward_pass(tile, count, x, coeff)

        return carry

    lax.fori_loop(0, ITERS, iterate, 0)
    for pack, length in enumerate(lengths()):
        here = slice(pack * FEED_SETS, (pack + 1) * FEED_SETS)
        for part in range(2):
            x[part, here, :] = x[part, here, :] / jnp.sqrt(length)


def kernel(
    volt, taps, twiddle, fine_upper, fine_lower, usable, auto_power, share, repeat, out,
    weight, power, lined, lined_back, wide, ext, halfway, upper, lower, stage, sent_pair, sent_one, held_pair, held_one,
    x, y, coeff, squares, diag, loads, send_sems, recv_sems, edge_sems,
):
    def arrange(source, target, split):
        feeds = FEED_SETS * FEEDS_HERE
        lane = lax.broadcasted_iota(jnp.int32, (FEED_SETS, feeds), 1)
        first = lax.broadcasted_iota(jnp.int32, (FEED_SETS, feeds), 0) * FEEDS_HERE
        mine = (lane >= first) & (lane < first + FEEDS_HERE)
        place = lax.broadcasted_iota(jnp.int32, (FEED_SETS, 128), 1)

        def body(pack, carry):
            for q in range(8):
                row = source[pl.ds(pack * 8 + q, 1), :].astype(jnp.float32)
                lined[q * FEED_SETS : (q + 1) * FEED_SETS, :] = jnp.where(mine, row, 0.0)
            value = lined[...]
            high = value.astype(jnp.bfloat16)
            wide = jnp.dot(high, repeat[...], preferred_element_type=jnp.float32)
            if split:
                rest = value - high.astype(jnp.float32)
                middle = rest.astype(jnp.bfloat16)
                low = (rest - middle.astype(jnp.float32)).astype(jnp.bfloat16)
                wide = wide + jnp.dot(middle, repeat[...], preferred_element_type=jnp.float32)
                wide = wide + jnp.dot(low, repeat[...], preferred_element_type=jnp.float32)
            total = jnp.zeros((FEED_SETS, 128), jnp.float32)
            for q in range(8):
                part = wide[q * FEED_SETS : (q + 1) * FEED_SETS]
                own = (place >= q * FEEDS_HERE) & (place < (q + 1) * FEEDS_HERE)
                total = total + jnp.where(own, part, 0.0)
            target[pl.ds(pl.multiple_of(pack * FEED_SETS, FEED_SETS), FEED_SETS), :] = total
            return carry

        lax.fori_loop(0, PACKS, body, 0)

    def arrange_back(pack, rows):
        feeds = FEED_SETS * FEEDS_HERE
        lane = lax.broadcasted_iota(jnp.int32, (FEED_SETS, feeds), 1)
        first = lax.broadcasted_iota(jnp.int32, (FEED_SETS, feeds), 0) * FEEDS_HERE
        mine = (lane >= first) & (lane < first + FEEDS_HERE)
        place = lax.broadcasted_iota(jnp.int32, (FEED_SETS, 128), 1)
        dims = (((1,), (1,)), ((), ()))
        for part in range(2):
            value = x[part, rows, :]
            for q in range(8):
                own = (place >= q * FEEDS_HERE) & (place < (q + 1) * FEEDS_HERE)
                lined_back[q * FEED_SETS : (q + 1) * FEED_SETS, :] = jnp.where(own, value, 0.0)
            rest = lined_back[...]
            total = jnp.zeros((8 * FEED_SETS, feeds), jnp.float32)
            for _ in range(3):
                piece = rest.astype(jnp.bfloat16)
                rest = rest - piece.astype(jnp.float32)
                total = total + lax.dot_general(
                    piece, repeat[...], dims, preferred_element_type=jnp.float32
                )
            for q in range(8):
                line = jnp.where(mine, total[q * FEED_SETS : (q + 1) * FEED_SETS], 0.0)
                out[part, pl.ds(pack * 8 + q, 1), :] = jnp.sum(line, axis=0, keepdims=True)

    section = lax.axis_index("section")
    chan = lax.axis_index("chan")
    core = lax.rem(chan, 2)
    before = 2 - core
    me = section * FEED_SETS + chan
    load = pltpu.make_async_copy(
        volt, ext.at[:, :, pl.ds(pl.multiple_of(before * CHANNELS, CHANNELS), LENGTH)], loads
    )
    load.start()
    barrier = pltpu.get_barrier_semaphore()

    def greet(there, column):
        pl.semaphore_signal(
            barrier, inc=1, device_id=(there, column), device_id_type=pl.DeviceIdType.MESH
        )

    visit(section, chan, greet)
    edges = []
    for kind in range(2):
        early, late = (2 - kind) * CHANNELS, (1 + kind) * CHANNELS
        pair = (edge_sems, edge_sems.at[pl.ds(2, 2)])
        edges.append((
            copy_at(
                volt.at[:, :, pl.ds(LENGTH - early, early)],
                ext.at[:, :, pl.ds(0, early)],
                pair,
                0,
                (lax.rem(section + 1, SECTIONS), chan),
            ),
            copy_at(
                volt.at[:, :, pl.ds(0, late)],
                ext.at[:, :, pl.ds(early + LENGTH, late)],
                pair,
                1,
                (lax.rem(section + SECTIONS - 1, SECTIONS), chan),
            ),
        ))
    pl.semaphore_wait(barrier, OWNERS - 1)
    for kind in range(2):

        @pl.when(core == kind)
        def _():
            edges[kind][0].start()
            edges[kind][1].start()

    load.wait()

    def clear(first, count):
        def body(at, inner):
            where = pl.ds(pl.multiple_of(first * CHANNELS + at * FINE, FINE), FINE)
            for part in range(2):
                ext[part, :, where] = jnp.zeros((FEEDS_HERE, FINE), jnp.bfloat16)
            return inner

        lax.fori_loop(0, count * COARSE, body, 0)

    def grouped(position, carry):
        group = lax.rem(position + 1, GROUPS)

        for kind in range(2):

            @pl.when((position == 2) & (core == kind))
            def _():
                edges[kind][1].wait()

            @pl.when((position == 3) & (core == kind))
            def _():
                edges[kind][0].wait()

        @pl.when((position == 3) & (section == 0))
        def _():
            clear(0, before)

        def step(at, inner):
            @pl.when((section == SECTIONS - 1) & (position == 2) & (at == GROUP - 1))
            def _():
                clear(BLOCKS_HERE - HALO + before, HALO)

            block = lax.rem(group * GROUP + at + core * (BLOCKS_HERE - 1), BLOCKS_HERE)
            first_transform(block, ext, taps, halfway)
            second_transform(twiddle, halfway, upper, lower)
            fine_transform(at, fine_upper, fine_lower, upper, lower, stage)
            return inner

        lax.fori_loop(0, GROUP, step, 0)

        def emit(owner, inner):
            rows = pl.ds(owner * STRIDE, 16)
            for pack in range(2):
                sent_pair[owner, group, pack] = stage[pack, rows, :].astype(jnp.bfloat16)
                sent_one[pack, owner, group] = stage[2 + pack, rows, :].astype(jnp.bfloat16)
            return inner

        lax.fori_loop(0, OWNERS, emit, 0, unroll=8)

        def send(there, column):
            pltpu.make_async_remote_copy(
                src_ref=sent_pair.at[there * FEED_SETS + column, group],
                dst_ref=held_pair.at[me, group],
                send_sem=send_sems.at[0],
                recv_sem=recv_sems.at[group],
                device_id=(there, column),
                device_id_type=pl.DeviceIdType.MESH,
            ).start()

        visit(section, chan, send)
        return carry

    lax.fori_loop(0, GROUPS, grouped, 0)

    def send_third(there, column):
        pltpu.make_async_remote_copy(
            src_ref=sent_one.at[0, there * FEED_SETS + column],
            dst_ref=held_one.at[0, me],
            send_sem=send_sems.at[1],
            recv_sem=recv_sems.at[2 * GROUPS],
            device_id=(there, column),
            device_id_type=pl.DeviceIdType.MESH,
        ).start()

    visit(section, chan, send_third)

    def rest(group, carry):
        def send(there, column):
            pltpu.make_async_remote_copy(
                src_ref=sent_one.at[1, there * FEED_SETS + column, group],
                dst_ref=held_one.at[1, me, group],
                send_sem=send_sems.at[2],
                recv_sem=recv_sems.at[GROUPS + group],
                device_id=(there, column),
                device_id_type=pl.DeviceIdType.MESH,
            ).start()

        visit(section, chan, send)
        return carry

    lax.fori_loop(0, GROUPS, rest, 0)
    arrange(usable, weight, False)
    arrange(auto_power, power, True)

    for group in range(GROUPS):
        for pack in range(2):
            held_pair[me, group, pack] = sent_pair[me, group, pack]
            held_one[pack, me, group] = sent_one[pack, me, group]

    others = pl.ds(0, OWNERS - 1)
    scratch = (weight, power, share, x, y, coeff, squares, diag)
    top_row = lax.broadcasted_iota(jnp.int32, (GROUP, 128), 0) == 0

    def tile(pack, slot, feed_set):
        at = (pack * SLOTS + slot) * FEED_SETS + feed_set
        return wide[at, 0], wide[at, 1]

    def begin(first, count):
        start_x(first, count, weight, x)
        diag[0 : count * FEED_SETS, :] = jnp.zeros((count * FEED_SETS, 128), jnp.float32)

    def take(read, group, count):
        def arrive(index, sums):
            sums = list(sums)
            for pack in range(count):
                for near in range(2):
                    feed_set = index * 2 + near
                    row = pl.ds(pack * FEED_SETS + feed_set, 1)
                    weight_row = x[0, row, :]
                    values = []
                    for at in range(SECTIONS):
                        value = read(at * FEED_SETS + feed_set, pack).astype(jnp.float32)
                        values.append((value[0:GROUP], value[GROUP:]))
                    if group == 0 and near == 1:
                        values = [
                            tuple(jnp.where(top_row, values[at - 1][c], values[at][c]) for c in range(2))
                            for at in range(SECTIONS)
                        ]
                    total = jnp.zeros((GROUP, 128), jnp.float32)
                    for at, (re, im) in enumerate(values):
                        place = (pack * SLOTS + at * GROUPS + group) * FEED_SETS + feed_set
                        wide[place, 0] = re
                        wide[place, 1] = im
                        total = total + (re * re + im * im)
                        own = 2 * (pack * SECTIONS + at)
                        sums[own] = sums[own] + re * weight_row
                        sums[own + 1] = sums[own + 1] - im * weight_row
                    diag[row, :] = diag[row, :] + jnp.sum(total, axis=0, keepdims=True)
            return tuple(sums)

        zero = jnp.zeros((GROUP, 128), jnp.float32)
        sums = lax.fori_loop(0, FEED_SETS // 2, arrive, (zero,) * (2 * SECTIONS * count))
        for pack in range(count):
            for at in range(SECTIONS):
                slot = pack * SLOTS + at * GROUPS + group
                own = 2 * (pack * SECTIONS + at)
                for part in range(2):
                    coeff[part, slot * GROUP : (slot + 1) * GROUP, :] = sums[own + part]

    begin(0, 2)
    for group in (1, 2, 3, 0):
        pltpu.make_async_copy(
            sent_pair.at[others, group], held_pair.at[others, group], recv_sems.at[group]
        ).wait()
        take(lambda source, pack: held_pair[source, group, pack], group, 2)
    solve_packs(tile, 0, 2, *scratch)
    for pack in range(2):
        arrange_back(pack, slice(pack * FEED_SETS, (pack + 1) * FEED_SETS))

    begin(2, 1)
    pltpu.make_async_copy(
        sent_one.at[0, others], held_one.at[0, others], recv_sems.at[2 * GROUPS]
    ).wait()
    for group in range(GROUPS):
        take(lambda source, pack: held_one[0, source, group], group, 1)
    solve_packs(tile, 2, 1, *scratch)
    arrange_back(2, slice(0, FEED_SETS))

    begin(3, 1)
    for group in range(GROUPS):
        pltpu.make_async_copy(
            sent_one.at[1, others, group],
            held_one.at[1, others, group],
            recv_sems.at[GROUPS + group],
        ).wait()
        take(lambda source, pack: held_one[1, source, group], group, 1)
    solve_packs(tile, 3, 1, *scratch)
    arrange_back(3, slice(0, FEED_SETS))
    pltpu.make_async_copy(sent_pair.at[others], held_pair.at[others], send_sems.at[0]).wait()
    for pack in range(2):
        pltpu.make_async_copy(
            sent_one.at[pack, others], held_one.at[pack, others], send_sems.at[1 + pack]
        ).wait()


def local(voltages, usable, auto_power):
    taps, twiddle, fine, share = tables()
    upper = fine.astype(jnp.bfloat16)
    lower = (fine - upper.astype(np.float32)).astype(jnp.bfloat16)
    rows = PACKS * FEED_SETS

    lane = np.arange(FEED_SETS * FEEDS_HERE)[:, None] % FEEDS_HERE
    repeat = (lane == np.arange(128)[None, :] % FEEDS_HERE).astype(jnp.bfloat16)
    vmem = pl.BlockSpec(memory_space=pltpu.VMEM)
    pair = pltpu.VMEM((OWNERS, GROUPS, 2, 16, 128), jnp.bfloat16)
    one = pltpu.VMEM((2, OWNERS, GROUPS, 16, 128), jnp.bfloat16)
    return pl.pallas_call(
        kernel,
        out_shape=jax.ShapeDtypeStruct((2, PACKS * 8, FEED_SETS * FEEDS_HERE), jnp.float32),
        in_specs=[pl.BlockSpec(memory_space=pl.ANY)] + [vmem] * 8,
        out_specs=vmem,
        scratch_shapes=[
            pltpu.VMEM((rows, 128), jnp.float32),
            pltpu.VMEM((rows, 128), jnp.float32),
            pltpu.VMEM((8 * FEED_SETS, FEED_SETS * FEEDS_HERE), jnp.float32),
            pltpu.VMEM((8 * FEED_SETS, 128), jnp.float32),
            pltpu.VMEM((2 * SLOTS * FEED_SETS, 2, GROUP, 128), jnp.float32),
            pltpu.VMEM((2, FEEDS_HERE, LENGTH + HALO * CHANNELS), jnp.bfloat16),
            pltpu.VMEM((4, 8, 2, FEEDS_HERE, FINE), jnp.float32),
            pltpu.VMEM((COARSE * FEEDS_HERE, 256), jnp.bfloat16),
            pltpu.VMEM((COARSE * FEEDS_HERE, 256), jnp.bfloat16),
            pltpu.VMEM((PACKS, OWNERS * STRIDE + 8, 128), jnp.float32),
            pair,
            one,
            pair,
            one,
            pltpu.VMEM((2, 2 * FEED_SETS, 128), jnp.float32),
            pltpu.VMEM((2, 2 * FEED_SETS, 128), jnp.float32),
            pltpu.VMEM((2, 2 * SLOTS * GROUP, 128), jnp.float32),
            pltpu.VMEM((16, 128), jnp.float32),
            pltpu.VMEM((2 * FEED_SETS, 128), jnp.float32),
            pltpu.SemaphoreType.DMA,
            pltpu.SemaphoreType.DMA((3,)),
            pltpu.SemaphoreType.DMA((1 + 2 * GROUPS,)),
            pltpu.SemaphoreType.DMA((4,)),
        ],
        compiler_params=pltpu.CompilerParams(
            collective_id=0, has_side_effects=True, vmem_limit_bytes=56 * 1024 * 1024
        ),
        cost_estimate=pl.CostEstimate(flops=10**10, bytes_accessed=2 * 10**7, transcendentals=0),
    )(
        voltages, taps, twiddle, upper, lower,
        usable, auto_power, share.astype(jnp.bfloat16), repeat,
    )


def solution(mesh):
    in_specs = (
        P(None, "chan", "section"),
        P(("section", "chan"), None),
        P(("section", "chan"), None),
    )
    out_specs = P(None, ("section", "chan"), None)
    return jax.shard_map(local, mesh=mesh, in_specs=in_specs, out_specs=out_specs, check_vma=False)
```

```python
import functools
import math

import jax
import jax.numpy as jnp
import numpy as np
from jax import lax
from jax.experimental import pallas as pl
from jax.experimental.pallas import tpu as pltpu
from jax.sharding import PartitionSpec as P

CHANNELS = 4096
TAPS = 4
ITERS = 5
EPSILON = 1e-06

COARSE = 32
FINE = 128
FEEDS_HERE = 16
BLOCKS_HERE = 32
GROUP = 8
GROUPS = BLOCKS_HERE // GROUP
PACKS = 4
OWNERS = 128
SECTIONS = 4
FEED_SETS = 32
SLOTS = SECTIONS * GROUPS
STRIDE = 17
LENGTH = BLOCKS_HERE * CHANNELS
HALO = TAPS - 1


def tables():
    position = np.arange(TAPS * CHANNELS, dtype=np.float64)
    offset = (position - 0.5 * TAPS * CHANNELS + 0.5) / CHANNELS
    window = 0.5 - 0.5 * np.cos(2.0 * np.pi * (position + 0.5) / (TAPS * CHANNELS))
    taps = np.sin(np.pi * offset) / (np.pi * offset) * window
    taps = taps.reshape(TAPS * COARSE, FINE).astype(np.float32)
    angle = 2.0 * np.pi * np.outer(np.arange(COARSE), np.arange(FINE)) / CHANNELS
    twiddle = np.concatenate([np.cos(angle), np.sin(angle)], axis=0).astype(np.float32)
    angle = 2.0 * np.pi * (np.outer(np.arange(FINE), np.arange(FINE)) % FINE) / FINE
    cosine = np.cos(angle) / math.sqrt(CHANNELS)
    sine = np.sin(angle) / math.sqrt(CHANNELS)
    fine = np.block([[cosine, sine], [-sine, cosine]]).astype(np.float32)
    lane = np.arange(128)
    share = (lane[:, None] // FEEDS_HERE == lane[None, :] // FEEDS_HERE).astype(np.float32)
    return taps, twiddle, fine, share


def butterfly_4(x):
    (ar, ai), (br, bi), (cr, ci), (dr, di) = x
    pr, pi, qr, qi = ar + cr, ai + ci, ar - cr, ai - ci
    sr, si, tr, ti = br + dr, bi + di, br - dr, bi - di
    return [(pr + sr, pi + si), (qr + ti, qi - tr), (pr - sr, pi - si), (qr - ti, qi + tr)]


def turn(x, eighths_of_32):
    n = eighths_of_32 % 32
    re, im = x
    if n == 0:
        return re, im
    if n == 8:
        return im, -re
    if n == 16:
        return -re, -im
    if n == 24:
        return -im, re
    cosine, sine = math.cos(2 * math.pi * n / 32), math.sin(2 * math.pi * n / 32)
    if n % 4 == 0:
        h = math.sqrt(0.5)
        if n == 4:
            return (re + im) * h, (im - re) * h
        if n == 12:
            return (im - re) * h, (re + im) * -h
    return re * cosine + im * sine, im * cosine - re * sine


def butterfly_8(x):
    even = butterfly_4([x[0], x[2], x[4], x[6]])
    odd = butterfly_4([x[1], x[3], x[5], x[7]])
    low, high = [], []
    for k in range(4):
        er, ei = even[k]
        tr, ti = turn(odd[k], 4 * k)
        low.append((er + tr, ei + ti))
        high.append((er - tr, ei - ti))
    return low + high


def first_transform(block, ext, taps, halfway):
    start = block * CHANNELS
    for low in range(8):
        points = []
        for high in range(4):
            tile = 8 * high + low
            pair = []
            for part in range(2):
                total = None
                for tap in range(TAPS):
                    at = pl.multiple_of(start + (tap * COARSE + tile) * FINE, FINE)
                    row = tap * COARSE + tile
                    term = taps[row : row + 1, :] * ext[part, :, pl.ds(at, FINE)].astype(jnp.float32)
                    total = term if total is None else total + term
                pair.append(total)
            points.append(tuple(pair))
        for q, point in enumerate(butterfly_4(points)):
            re, im = turn(point, low * q)
            halfway[q, low, 0] = re
            halfway[q, low, 1] = im


def second_transform(twiddle, halfway, upper, lower):
    for q1 in range(4):
        points = [(halfway[q1, low, 0], halfway[q1, low, 1]) for low in range(8)]
        for q2, (re, im) in enumerate(butterfly_8(points)):
            q = q1 + 4 * q2
            if q > 0:
                cosine = twiddle[q : q + 1, :]
                sine = twiddle[COARSE + q : COARSE + q + 1, :]
                re, im = re * cosine + im * sine, im * cosine - re * sine
            for part, value in enumerate((re, im)):
                high = value.astype(jnp.bfloat16)
                low = (value - high.astype(jnp.float32)).astype(jnp.bfloat16)
                rows = slice(q * FEEDS_HERE, (q + 1) * FEEDS_HERE)
                lanes = slice(part * FINE, (part + 1) * FINE)
                upper[rows, lanes] = high
                lower[rows, lanes] = low


def fine_transform(at, fine_upper, fine_lower, upper, lower, stage):
    dims = (((1,), (1,)), ((), ()))
    for half in range(2):
        rows = slice(half * 256, (half + 1) * 256)
        high = upper[rows, :]
        low = lower[rows, :]
        out = lax.dot_general(fine_upper[...], high, dims, preferred_element_type=jnp.float32)
        out += lax.dot_general(fine_lower[...], high, dims, preferred_element_type=jnp.float32)
        out += lax.dot_general(fine_upper[...], low, dims, preferred_element_type=jnp.float32)
        for pack in range(2):
            for part in range(2):
                piece = out[part * FINE : (part + 1) * FINE, pack * 128 : (pack + 1) * 128]
                stage[2 * half + pack, pl.ds(part * GROUP + at, OWNERS, stride=STRIDE), :] = piece


def visit(section, chan, action):
    row, column = lax.div(chan, 8), lax.rem(lax.div(chan, 2), 4)

    def turns(near, core):
        x = [lax.rem(section + near[0] + 2 * far, SECTIONS) for far in range(2)]
        y = [lax.rem(row + near[1] + 2 * far, 4) * 8 for far in range(2)]
        z = [lax.rem(column + near[2] + 2 * far, 4) * 2 + core for far in range(2)]
        return x, y, z

    def several(x, y, z, skip):
        for step in range(skip, 8):
            action(x[step % 2], y[step // 2 % 2] + z[step // 4])

    same = lax.rem(chan, 2)
    several(*turns((0, 0, 0), same), 1)

    def body(step, carry):
        near = [lax.rem(lax.div(step, 2), 2), lax.rem(lax.div(step, 4), 2), lax.rem(lax.div(step, 8), 2)]
        core = lax.rem(same + step, 2)
        several(*turns(near, core), 0)
        return carry

    lax.fori_loop(1, 16, body, 0)


def copy_at(source, target, sems, at, device):
    return pltpu.make_async_remote_copy(
        src_ref=source,
        dst_ref=target,
        send_sem=sems[0].at[at],
        recv_sem=sems[1].at[at],
        device_id=device,
        device_id_type=pl.DeviceIdType.MESH,
    )


def share_dot(value, share):
    high = value.astype(jnp.bfloat16)
    low = (value - high.astype(jnp.float32)).astype(jnp.bfloat16)
    total = jnp.dot(high, share, preferred_element_type=jnp.float32)
    return total + jnp.dot(low, share, preferred_element_type=jnp.float32)


def own_rows(pack, count=1):
    return pl.ds(pl.multiple_of(pack * FEED_SETS, FEED_SETS), count * FEED_SETS)


def forward_pass(tile, count, x, coeff):
    for pack in range(count):

        def forward(index, inner):
            pr = [jnp.zeros((GROUP, 128), jnp.float32) for _ in range(8)]
            pi = [jnp.zeros((GROUP, 128), jnp.float32) for _ in range(8)]
            for feed_set in range(FEED_SETS):
                at = pack * FEED_SETS + feed_set
                xr = x[0, at : at + 1, :]
                xi = x[1, at : at + 1, :]
                for two in range(4):
                    re, im = tile(pack, index * 4 + two, feed_set)
                    pr[two] = pr[two] + re * xr
                    pr[4 + two] = pr[4 + two] + im * xi
                    pi[two] = pi[two] + re * xi
                    pi[4 + two] = pi[4 + two] - im * xr
            at = pl.multiple_of((pack * SLOTS + index * 4) * GROUP, 4 * GROUP)
            for two in range(4):
                coeff[0, pl.ds(at + two * GROUP, GROUP), :] = pr[two] + pr[4 + two]
                coeff[1, pl.ds(at + two * GROUP, GROUP), :] = pi[two] + pi[4 + two]
            return inner

        lax.fori_loop(0, SLOTS // 4, forward, 0)


def start_x(first, count, weight, x):
    span = slice(0, count * FEED_SETS)
    x[0, span, :] = weight[own_rows(first, count), :]
    x[1, span, :] = jnp.zeros((count * FEED_SETS, 128), jnp.float32)


def solve_packs(tile, first, count, weight, power, share, x, y, coeff, squares, diag):
    span = slice(0, count * FEED_SETS)
    diag[span, :] = float(SLOTS * GROUP) * power[own_rows(first, count), :] - diag[span, :]
    squares[...] = jnp.zeros_like(squares)

    def lengths():
        total = share_dot(squares[...], share[...])
        return [jnp.sqrt(total[8 * pack : 8 * pack + 1] + EPSILON) for pack in range(count)]

    def iterate(iteration, carry):
        inverse = [jnp.where(iteration == 0, 1.0, 1.0 / length) for length in lengths()]
        for pack in range(count):
            rows = slice(pack * SLOTS * GROUP, (pack + 1) * SLOTS * GROUP)
            for part in range(2):
                coeff[part, rows, :] = share_dot(coeff[part, rows, :], share[...]) * inverse[pack]
        for pack in range(count):

            def backward(index, inner):
                yr = [jnp.zeros((GROUP, 128), jnp.float32) for _ in range(8)]
                yi = [jnp.zeros((GROUP, 128), jnp.float32) for _ in range(8)]
                for slot in range(SLOTS):
                    at = (pack * SLOTS + slot) * GROUP
                    pr = coeff[0, at : at + GROUP, :]
                    pi = coeff[1, at : at + GROUP, :]
                    for two in range(4):
                        re, im = tile(pack, slot, index * 4 + two)
                        yr[two] = yr[two] + re * pr
                        yr[4 + two] = yr[4 + two] - im * pi
                        yi[two] = yi[two] + re * pi
                        yi[4 + two] = yi[4 + two] + im * pr
                for two in range(4):
                    at = pl.ds(pack * FEED_SETS + index * 4 + two, 1)
                    y[0, at, :] = jnp.sum(yr[two] + yr[4 + two], axis=0, keepdims=True)
                    y[1, at, :] = jnp.sum(yi[two] + yi[4 + two], axis=0, keepdims=True)
                return inner

            lax.fori_loop(0, FEED_SETS // 4, backward, 0)
        for pack in range(count):
            here = slice(pack * FEED_SETS, (pack + 1) * FEED_SETS)
            w = weight[own_rows(first + pack), :]
            scaled = w * (diag[here, :] * (w * inverse[pack]))
            total = jnp.zeros((8, 128), jnp.float32)
            for part in range(2):
                value = w * y[part, here, :] + scaled * x[part, here, :]
                x[part, here, :] = value
                for row in range(0, FEED_SETS, 8):
                    total = total + value[row : row + 8] * value[row : row + 8]
            total = jnp.sum(total, axis=0, keepdims=True)
            squares[8 * pack : 8 * pack + 8, :] = jnp.broadcast_to(total, (8, 128))

        @pl.when(iteration < ITERS - 1)
        def _():
            forward_pass(tile, count, x, coeff)

        return carry

    lax.fori_loop(0, ITERS, iterate, 0)
    for pack, length in enumerate(lengths()):
        here = slice(pack * FEED_SETS, (pack + 1) * FEED_SETS)
        for part in range(2):
            x[part, here, :] = x[part, here, :] / jnp.sqrt(length)


def kernel(
    volt, taps, twiddle, fine_upper, fine_lower, usable, auto_power, share, repeat, out,
    weight, power, lined, lined_back, wide, ext, halfway, upper, lower, stage, sent_pair, sent_one, held_pair, held_one,
    x, y, coeff, squares, diag, loads, send_sems, recv_sems, edge_sems,
):
    def arrange(source, target, split):
        feeds = FEED_SETS * FEEDS_HERE
        lane = lax.broadcasted_iota(jnp.int32, (FEED_SETS, feeds), 1)
        first = lax.broadcasted_iota(jnp.int32, (FEED_SETS, feeds), 0) * FEEDS_HERE
        mine = (lane >= first) & (lane < first + FEEDS_HERE)
        place = lax.broadcasted_iota(jnp.int32, (FEED_SETS, 128), 1)

        def body(pack, carry):
            for q in range(8):
                row = source[pl.ds(pack * 8 + q, 1), :].astype(jnp.float32)
                lined[q * FEED_SETS : (q + 1) * FEED_SETS, :] = jnp.where(mine, row, 0.0)
            value = lined[...]
            high = value.astype(jnp.bfloat16)
            wide = jnp.dot(high, repeat[...], preferred_element_type=jnp.float32)
            if split:
                rest = value - high.astype(jnp.float32)
                middle = rest.astype(jnp.bfloat16)
                low = (rest - middle.astype(jnp.float32)).astype(jnp.bfloat16)
                wide = wide + jnp.dot(middle, repeat[...], preferred_element_type=jnp.float32)
                wide = wide + jnp.dot(low, repeat[...], preferred_element_type=jnp.float32)
            total = jnp.zeros((FEED_SETS, 128), jnp.float32)
            for q in range(8):
                part = wide[q * FEED_SETS : (q + 1) * FEED_SETS]
                own = (place >= q * FEEDS_HERE) & (place < (q + 1) * FEEDS_HERE)
                total = total + jnp.where(own, part, 0.0)
            target[pl.ds(pl.multiple_of(pack * FEED_SETS, FEED_SETS), FEED_SETS), :] = total
            return carry

        lax.fori_loop(0, PACKS, body, 0)

    def arrange_back(pack, rows):
        feeds = FEED_SETS * FEEDS_HERE
        lane = lax.broadcasted_iota(jnp.int32, (FEED_SETS, feeds), 1)
        first = lax.broadcasted_iota(jnp.int32, (FEED_SETS, feeds), 0) * FEEDS_HERE
        mine = (lane >= first) & (lane < first + FEEDS_HERE)
        place = lax.broadcasted_iota(jnp.int32, (FEED_SETS, 128), 1)
        dims = (((1,), (1,)), ((), ()))
        for part in range(2):
            value = x[part, rows, :]
            for q in range(8):
                own = (place >= q * FEEDS_HERE) & (place < (q + 1) * FEEDS_HERE)
                lined_back[q * FEED_SETS : (q + 1) * FEED_SETS, :] = jnp.where(own, value, 0.0)
            rest = lined_back[...]
            total = jnp.zeros((8 * FEED_SETS, feeds), jnp.float32)
            for _ in range(2):
                piece = rest.astype(jnp.bfloat16)
                rest = rest - piece.astype(jnp.float32)
                total = total + lax.dot_general(
                    piece, repeat[...], dims, preferred_element_type=jnp.float32
                )
            for q in range(8):
                line = jnp.where(mine, total[q * FEED_SETS : (q + 1) * FEED_SETS], 0.0)
                out[part, pl.ds(pack * 8 + q, 1), :] = jnp.sum(line, axis=0, keepdims=True)

    section = lax.axis_index("section")
    chan = lax.axis_index("chan")
    core = lax.rem(chan, 2)
    before = 2 - core
    me = section * FEED_SETS + chan
    load = pltpu.make_async_copy(
        volt, ext.at[:, :, pl.ds(pl.multiple_of(before * CHANNELS, CHANNELS), LENGTH)], loads
    )
    load.start()
    barrier = pltpu.get_barrier_semaphore()

    def greet(there, column):
        pl.semaphore_signal(
            barrier, inc=1, device_id=(there, column), device_id_type=pl.DeviceIdType.MESH
        )

    visit(section, chan, greet)
    edges = []
    for kind in range(2):
        early, late = (2 - kind) * CHANNELS, (1 + kind) * CHANNELS
        pair = (edge_sems, edge_sems.at[pl.ds(2, 2)])
        edges.append((
            copy_at(
                volt.at[:, :, pl.ds(LENGTH - early, early)],
                ext.at[:, :, pl.ds(0, early)],
                pair,
                0,
                (lax.rem(section + 1, SECTIONS), chan),
            ),
            copy_at(
                volt.at[:, :, pl.ds(0, late)],
                ext.at[:, :, pl.ds(early + LENGTH, late)],
                pair,
                1,
                (lax.rem(section + SECTIONS - 1, SECTIONS), chan),
            ),
        ))
    pl.semaphore_wait(barrier, OWNERS - 1)
    for kind in range(2):

        @pl.when(core == kind)
        def _():
            edges[kind][0].start()
            edges[kind][1].start()

    load.wait()

    def clear(first, count):
        def body(at, inner):
            where = pl.ds(pl.multiple_of(first * CHANNELS + at * FINE, FINE), FINE)
            for part in range(2):
                ext[part, :, where] = jnp.zeros((FEEDS_HERE, FINE), jnp.bfloat16)
            return inner

        lax.fori_loop(0, count * COARSE, body, 0)

    def grouped(position, carry):
        group = lax.rem(position + 1, GROUPS)

        for kind in range(2):

            @pl.when((position == 2) & (core == kind))
            def _():
                edges[kind][1].wait()

            @pl.when((position == 3) & (core == kind))
            def _():
                edges[kind][0].wait()

        @pl.when((position == 3) & (section == 0))
        def _():
            clear(0, before)

        def step(at, inner):
            @pl.when((section == SECTIONS - 1) & (position == 2) & (at == GROUP - 1))
            def _():
                clear(BLOCKS_HERE - HALO + before, HALO)

            block = lax.rem(group * GROUP + at + core * (BLOCKS_HERE - 1), BLOCKS_HERE)
            first_transform(block, ext, taps, halfway)
            second_transform(twiddle, halfway, upper, lower)
            fine_transform(at, fine_upper, fine_lower, upper, lower, stage)
            return inner

        lax.fori_loop(0, GROUP, step, 0)

        def emit(owner, inner):
            rows = pl.ds(owner * STRIDE, 16)
            for pack in range(2):
                sent_pair[owner, group, pack] = stage[pack, rows, :].astype(jnp.bfloat16)
                sent_one[pack, owner, group] = stage[2 + pack, rows, :].astype(jnp.bfloat16)
            return inner

        lax.fori_loop(0, OWNERS, emit, 0, unroll=8)

        def send(there, column):
            pltpu.make_async_remote_copy(
                src_ref=sent_pair.at[there * FEED_SETS + column, group],
                dst_ref=held_pair.at[me, group],
                send_sem=send_sems.at[0],
                recv_sem=recv_sems.at[group],
                device_id=(there, column),
                device_id_type=pl.DeviceIdType.MESH,
            ).start()

        visit(section, chan, send)
        return carry

    lax.fori_loop(0, GROUPS, grouped, 0)

    def send_third(there, column):
        pltpu.make_async_remote_copy(
            src_ref=sent_one.at[0, there * FEED_SETS + column],
            dst_ref=held_one.at[0, me],
            send_sem=send_sems.at[1],
            recv_sem=recv_sems.at[2 * GROUPS],
            device_id=(there, column),
            device_id_type=pl.DeviceIdType.MESH,
        ).start()

    visit(section, chan, send_third)

    def rest(group, carry):
        def send(there, column):
            pltpu.make_async_remote_copy(
                src_ref=sent_one.at[1, there * FEED_SETS + column, group],
                dst_ref=held_one.at[1, me, group],
                send_sem=send_sems.at[2],
                recv_sem=recv_sems.at[GROUPS + group],
                device_id=(there, column),
                device_id_type=pl.DeviceIdType.MESH,
            ).start()

        visit(section, chan, send)
        return carry

    lax.fori_loop(0, GROUPS, rest, 0)
    arrange(usable, weight, False)
    arrange(auto_power, power, True)

    for group in range(GROUPS):
        for pack in range(2):
            held_pair[me, group, pack] = sent_pair[me, group, pack]
            held_one[pack, me, group] = sent_one[pack, me, group]

    others = pl.ds(0, OWNERS - 1)
    scratch = (weight, power, share, x, y, coeff, squares, diag)
    top_row = lax.broadcasted_iota(jnp.int32, (GROUP, 128), 0) == 0

    def tile(pack, slot, feed_set):
        at = (pack * SLOTS + slot) * FEED_SETS + feed_set
        return wide[at, 0], wide[at, 1]

    def begin(first, count):
        start_x(first, count, weight, x)
        diag[0 : count * FEED_SETS, :] = jnp.zeros((count * FEED_SETS, 128), jnp.float32)

    def take(read, group, count):
        def arrive(index, sums):
            sums = list(sums)
            for pack in range(count):
                for near in range(2):
                    feed_set = index * 2 + near
                    row = pl.ds(pack * FEED_SETS + feed_set, 1)
                    weight_row = x[0, row, :]
                    values = []
                    for at in range(SECTIONS):
                        value = read(at * FEED_SETS + feed_set, pack).astype(jnp.float32)
                        values.append((value[0:GROUP], value[GROUP:]))
                    if group == 0 and near == 1:
                        values = [
                            tuple(jnp.where(top_row, values[at - 1][c], values[at][c]) for c in range(2))
                            for at in range(SECTIONS)
                        ]
                    total = jnp.zeros((GROUP, 128), jnp.float32)
                    for at, (re, im) in enumerate(values):
                        place = (pack * SLOTS + at * GROUPS + group) * FEED_SETS + feed_set
                        wide[place, 0] = re
                        wide[place, 1] = im
                        total = total + (re * re + im * im)
                        own = 2 * (pack * SECTIONS + at)
                        sums[own] = sums[own] + re * weight_row
                        sums[own + 1] = sums[own + 1] - im * weight_row
                    diag[row, :] = diag[row, :] + jnp.sum(total, axis=0, keepdims=True)
            return tuple(sums)

        zero = jnp.zeros((GROUP, 128), jnp.float32)
        sums = lax.fori_loop(0, FEED_SETS // 2, arrive, (zero,) * (2 * SECTIONS * count))
        for pack in range(count):
            for at in range(SECTIONS):
                slot = pack * SLOTS + at * GROUPS + group
                own = 2 * (pack * SECTIONS + at)
                for part in range(2):
                    coeff[part, slot * GROUP : (slot + 1) * GROUP, :] = sums[own + part]

    begin(0, 2)
    for group in (1, 2, 3, 0):
        pltpu.make_async_copy(
            sent_pair.at[others, group], held_pair.at[others, group], recv_sems.at[group]
        ).wait()
        take(lambda source, pack: held_pair[source, group, pack], group, 2)
    solve_packs(tile, 0, 2, *scratch)
    for pack in range(2):
        arrange_back(pack, slice(pack * FEED_SETS, (pack + 1) * FEED_SETS))

    begin(2, 1)
    pltpu.make_async_copy(
        sent_one.at[0, others], held_one.at[0, others], recv_sems.at[2 * GROUPS]
    ).wait()
    for group in range(GROUPS):
        take(lambda source, pack: held_one[0, source, group], group, 1)
    solve_packs(tile, 2, 1, *scratch)
    arrange_back(2, slice(0, FEED_SETS))

    begin(3, 1)
    for group in range(GROUPS):
        pltpu.make_async_copy(
            sent_one.at[1, others, group],
            held_one.at[1, others, group],
            recv_sems.at[GROUPS + group],
        ).wait()
        take(lambda source, pack: held_one[1, source, group], group, 1)
    solve_packs(tile, 3, 1, *scratch)
    arrange_back(3, slice(0, FEED_SETS))
    pltpu.make_async_copy(sent_pair.at[others], held_pair.at[others], send_sems.at[0]).wait()
    for pack in range(2):
        pltpu.make_async_copy(
            sent_one.at[pack, others], held_one.at[pack, others], send_sems.at[1 + pack]
        ).wait()


def local(voltages, usable, auto_power):
    taps, twiddle, fine, share = tables()
    upper = fine.astype(jnp.bfloat16)
    lower = (fine - upper.astype(np.float32)).astype(jnp.bfloat16)
    rows = PACKS * FEED_SETS

    lane = np.arange(FEED_SETS * FEEDS_HERE)[:, None] % FEEDS_HERE
    repeat = (lane == np.arange(128)[None, :] % FEEDS_HERE).astype(jnp.bfloat16)
    vmem = pl.BlockSpec(memory_space=pltpu.VMEM)
    pair = pltpu.VMEM((OWNERS, GROUPS, 2, 16, 128), jnp.bfloat16)
    one = pltpu.VMEM((2, OWNERS, GROUPS, 16, 128), jnp.bfloat16)
    return pl.pallas_call(
        kernel,
        out_shape=jax.ShapeDtypeStruct((2, PACKS * 8, FEED_SETS * FEEDS_HERE), jnp.float32),
        in_specs=[pl.BlockSpec(memory_space=pl.ANY)] + [vmem] * 8,
        out_specs=vmem,
        scratch_shapes=[
            pltpu.VMEM((rows, 128), jnp.float32),
            pltpu.VMEM((rows, 128), jnp.float32),
            pltpu.VMEM((8 * FEED_SETS, FEED_SETS * FEEDS_HERE), jnp.float32),
            pltpu.VMEM((8 * FEED_SETS, 128), jnp.float32),
            pltpu.VMEM((2 * SLOTS * FEED_SETS, 2, GROUP, 128), jnp.float32),
            pltpu.VMEM((2, FEEDS_HERE, LENGTH + HALO * CHANNELS), jnp.bfloat16),
            pltpu.VMEM((4, 8, 2, FEEDS_HERE, FINE), jnp.float32),
            pltpu.VMEM((COARSE * FEEDS_HERE, 256), jnp.bfloat16),
            pltpu.VMEM((COARSE * FEEDS_HERE, 256), jnp.bfloat16),
            pltpu.VMEM((PACKS, OWNERS * STRIDE + 8, 128), jnp.float32),
            pair,
            one,
            pair,
            one,
            pltpu.VMEM((2, 2 * FEED_SETS, 128), jnp.float32),
            pltpu.VMEM((2, 2 * FEED_SETS, 128), jnp.float32),
            pltpu.VMEM((2, 2 * SLOTS * GROUP, 128), jnp.float32),
            pltpu.VMEM((16, 128), jnp.float32),
            pltpu.VMEM((2 * FEED_SETS, 128), jnp.float32),
            pltpu.SemaphoreType.DMA,
            pltpu.SemaphoreType.DMA((3,)),
            pltpu.SemaphoreType.DMA((1 + 2 * GROUPS,)),
            pltpu.SemaphoreType.DMA((4,)),
        ],
        compiler_params=pltpu.CompilerParams(
            collective_id=0, has_side_effects=True, vmem_limit_bytes=56 * 1024 * 1024
        ),
        cost_estimate=pl.CostEstimate(flops=10**10, bytes_accessed=2 * 10**7, transcendentals=0),
    )(
        voltages, taps, twiddle, upper, lower,
        usable, auto_power, share.astype(jnp.bfloat16), repeat,
    )


def solution(mesh):
    in_specs = (
        P(None, "chan", "section"),
        P(("section", "chan"), None),
        P(("section", "chan"), None),
    )
    out_specs = P(None, ("section", "chan"), None)
    return jax.shard_map(local, mesh=mesh, in_specs=in_specs, out_specs=out_specs, check_vma=False)
```

```python
import functools
import math

import jax
import jax.numpy as jnp
import numpy as np
from jax import lax
from jax.experimental import pallas as pl
from jax.experimental.pallas import tpu as pltpu
from jax.sharding import PartitionSpec as P

CHANNELS = 4096
TAPS = 4
ITERS = 5
EPSILON = 1e-06

COARSE = 32
FINE = 128
FEEDS_HERE = 16
BLOCKS_HERE = 32
GROUP = 8
GROUPS = BLOCKS_HERE // GROUP
PACKS = 4
OWNERS = 128
SECTIONS = 4
FEED_SETS = 32
SLOTS = SECTIONS * GROUPS
STRIDE = 17
LENGTH = BLOCKS_HERE * CHANNELS
HALO = TAPS - 1


def tables():
    position = np.arange(TAPS * CHANNELS, dtype=np.float64)
    offset = (position - 0.5 * TAPS * CHANNELS + 0.5) / CHANNELS
    window = 0.5 - 0.5 * np.cos(2.0 * np.pi * (position + 0.5) / (TAPS * CHANNELS))
    taps = np.sin(np.pi * offset) / (np.pi * offset) * window
    taps = taps.reshape(TAPS * COARSE, FINE).astype(np.float32)
    angle = 2.0 * np.pi * np.outer(np.arange(COARSE), np.arange(FINE)) / CHANNELS
    twiddle = np.concatenate([np.cos(angle), np.sin(angle)], axis=0).astype(np.float32)
    angle = 2.0 * np.pi * (np.outer(np.arange(FINE), np.arange(FINE)) % FINE) / FINE
    cosine = np.cos(angle) / math.sqrt(CHANNELS)
    sine = np.sin(angle) / math.sqrt(CHANNELS)
    fine = np.block([[cosine, sine], [-sine, cosine]]).astype(np.float32)
    lane = np.arange(128)
    share = (lane[:, None] // FEEDS_HERE == lane[None, :] // FEEDS_HERE).astype(np.float32)
    return taps, twiddle, fine, share


def butterfly_4(x):
    (ar, ai), (br, bi), (cr, ci), (dr, di) = x
    pr, pi, qr, qi = ar + cr, ai + ci, ar - cr, ai - ci
    sr, si, tr, ti = br + dr, bi + di, br - dr, bi - di
    return [(pr + sr, pi + si), (qr + ti, qi - tr), (pr - sr, pi - si), (qr - ti, qi + tr)]


def turn(x, eighths_of_32):
    n = eighths_of_32 % 32
    re, im = x
    if n == 0:
        return re, im
    if n == 8:
        return im, -re
    if n == 16:
        return -re, -im
    if n == 24:
        return -im, re
    cosine, sine = math.cos(2 * math.pi * n / 32), math.sin(2 * math.pi * n / 32)
    if n % 4 == 0:
        h = math.sqrt(0.5)
        if n == 4:
            return (re + im) * h, (im - re) * h
        if n == 12:
            return (im - re) * h, (re + im) * -h
    return re * cosine + im * sine, im * cosine - re * sine


def butterfly_8(x):
    even = butterfly_4([x[0], x[2], x[4], x[6]])
    odd = butterfly_4([x[1], x[3], x[5], x[7]])
    low, high = [], []
    for k in range(4):
        er, ei = even[k]
        tr, ti = turn(odd[k], 4 * k)
        low.append((er + tr, ei + ti))
        high.append((er - tr, ei - ti))
    return low + high


def first_transform(block, ext, taps, halfway):
    start = block * CHANNELS
    for low in range(8):
        points = []
        for high in range(4):
            tile = 8 * high + low
            pair = []
            for part in range(2):
                total = None
                for tap in range(TAPS):
                    at = pl.multiple_of(start + (tap * COARSE + tile) * FINE, FINE)
                    row = tap * COARSE + tile
                    term = taps[row : row + 1, :] * ext[part, :, pl.ds(at, FINE)].astype(jnp.float32)
                    total = term if total is None else total + term
                pair.append(total)
            points.append(tuple(pair))
        for q, point in enumerate(butterfly_4(points)):
            re, im = turn(point, low * q)
            halfway[q, low, 0] = re
            halfway[q, low, 1] = im


def second_transform(twiddle, halfway, upper, lower):
    for q1 in range(4):
        points = [(halfway[q1, low, 0], halfway[q1, low, 1]) for low in range(8)]
        for q2, (re, im) in enumerate(butterfly_8(points)):
            q = q1 + 4 * q2
            if q > 0:
                cosine = twiddle[q : q + 1, :]
                sine = twiddle[COARSE + q : COARSE + q + 1, :]
                re, im = re * cosine + im * sine, im * cosine - re * sine
            for part, value in enumerate((re, im)):
                high = value.astype(jnp.bfloat16)
                low = (value - high.astype(jnp.float32)).astype(jnp.bfloat16)
                rows = slice(q * FEEDS_HERE, (q + 1) * FEEDS_HERE)
                lanes = slice(part * FINE, (part + 1) * FINE)
                upper[rows, lanes] = high
                lower[rows, lanes] = low


def fine_transform(at, fine_upper, fine_lower, upper, lower, stage):
    dims = (((1,), (1,)), ((), ()))
    for half in range(2):
        rows = slice(half * 256, (half + 1) * 256)
        high = upper[rows, :]
        low = lower[rows, :]
        out = lax.dot_general(fine_upper[...], high, dims, preferred_element_type=jnp.float32)
        out += lax.dot_general(fine_lower[...], high, dims, preferred_element_type=jnp.float32)
        out += lax.dot_general(fine_upper[...], low, dims, preferred_element_type=jnp.float32)
        for pack in range(2):
            for part in range(2):
                piece = out[part * FINE : (part + 1) * FINE, pack * 128 : (pack + 1) * 128]
                stage[2 * half + pack, pl.ds(part * GROUP + at, OWNERS, stride=STRIDE), :] = piece


def visit(section, chan, action):
    row, column = lax.div(chan, 8), lax.rem(lax.div(chan, 2), 4)

    def turns(near, core):
        x = [lax.rem(section + near[0] + 2 * far, SECTIONS) for far in range(2)]
        y = [lax.rem(row + near[1] + 2 * far, 4) * 8 for far in range(2)]
        z = [lax.rem(column + near[2] + 2 * far, 4) * 2 + core for far in range(2)]
        return x, y, z

    def several(x, y, z, skip):
        for step in range(skip, 8):
            action(x[step % 2], y[step // 2 % 2] + z[step // 4])

    same = lax.rem(chan, 2)
    several(*turns((0, 0, 0), same), 1)

    def body(step, carry):
        near = [lax.rem(lax.div(step, 2), 2), lax.rem(lax.div(step, 4), 2), lax.rem(lax.div(step, 8), 2)]
        core = lax.rem(same + step, 2)
        several(*turns(near, core), 0)
        return carry

    lax.fori_loop(1, 16, body, 0)


def copy_at(source, target, sems, at, device):
    return pltpu.make_async_remote_copy(
        src_ref=source,
        dst_ref=target,
        send_sem=sems[0].at[at],
        recv_sem=sems[1].at[at],
        device_id=device,
        device_id_type=pl.DeviceIdType.MESH,
    )


def share_dot(value, share):
    high = value.astype(jnp.bfloat16)
    low = (value - high.astype(jnp.float32)).astype(jnp.bfloat16)
    total = jnp.dot(high, share, preferred_element_type=jnp.float32)
    return total + jnp.dot(low, share, preferred_element_type=jnp.float32)


def own_rows(pack, count=1):
    return pl.ds(pl.multiple_of(pack * FEED_SETS, FEED_SETS), count * FEED_SETS)


def forward_pass(tile, count, x, coeff, slots):
    for pack in range(count):

        def forward(index, inner):
            pr = [jnp.zeros((GROUP, 128), jnp.float32) for _ in range(8)]
            pi = [jnp.zeros((GROUP, 128), jnp.float32) for _ in range(8)]
            for feed_set in range(FEED_SETS):
                at = pack * FEED_SETS + feed_set
                xr = x[0, at : at + 1, :]
                xi = x[1, at : at + 1, :]
                for two in range(4):
                    re, im = tile(pack, index * 4 + two, feed_set)
                    pr[two] = pr[two] + re * xr
                    pr[4 + two] = pr[4 + two] + im * xi
                    pi[two] = pi[two] + re * xi
                    pi[4 + two] = pi[4 + two] - im * xr
            at = pl.multiple_of((pack * SLOTS + index * 4) * GROUP, 4 * GROUP)
            for two in range(4):
                coeff[0, pl.ds(at + two * GROUP, GROUP), :] = pr[two] + pr[4 + two]
                coeff[1, pl.ds(at + two * GROUP, GROUP), :] = pi[two] + pi[4 + two]
            return inner

        lax.fori_loop(0, slots // 4, forward, 0)


def start_x(first, count, weight, x):
    span = slice(0, count * FEED_SETS)
    x[0, span, :] = weight[own_rows(first, count), :]
    x[1, span, :] = jnp.zeros((count * FEED_SETS, 128), jnp.float32)


def solve_packs(
    tile, first, count, weight, power, share, x, y, coeff, squares, diag, slots=SLOTS
):
    span = slice(0, count * FEED_SETS)

    def whole(value):
        return value if slots == SLOTS else value + pltpu.roll(value, 64, 1)

    diag[span, :] = float(SLOTS * GROUP) * power[own_rows(first, count), :] - whole(diag[span, :])
    squares[...] = jnp.zeros_like(squares)

    def lengths():
        total = share_dot(squares[...], share[...])
        return [jnp.sqrt(total[8 * pack : 8 * pack + 1] + EPSILON) for pack in range(count)]

    def iterate(iteration, carry):
        inverse = [jnp.where(iteration == 0, 1.0, 1.0 / length) for length in lengths()]
        for pack in range(count):
            rows = slice(pack * SLOTS * GROUP, (pack * SLOTS + slots) * GROUP)
            for part in range(2):
                coeff[part, rows, :] = share_dot(coeff[part, rows, :], share[...]) * inverse[pack]
        for pack in range(count):

            def backward(index, inner):
                yr = [jnp.zeros((GROUP, 128), jnp.float32) for _ in range(8)]
                yi = [jnp.zeros((GROUP, 128), jnp.float32) for _ in range(8)]
                for slot in range(slots):
                    at = (pack * SLOTS + slot) * GROUP
                    pr = coeff[0, at : at + GROUP, :]
                    pi = coeff[1, at : at + GROUP, :]
                    for two in range(4):
                        re, im = tile(pack, slot, index * 4 + two)
                        yr[two] = yr[two] + re * pr
                        yr[4 + two] = yr[4 + two] - im * pi
                        yi[two] = yi[two] + re * pi
                        yi[4 + two] = yi[4 + two] + im * pr
                for two in range(4):
                    at = pl.ds(pack * FEED_SETS + index * 4 + two, 1)
                    y[0, at, :] = jnp.sum(yr[two] + yr[4 + two], axis=0, keepdims=True)
                    y[1, at, :] = jnp.sum(yi[two] + yi[4 + two], axis=0, keepdims=True)
                return inner

            lax.fori_loop(0, FEED_SETS // 4, backward, 0)
        for pack in range(count):
            here = slice(pack * FEED_SETS, (pack + 1) * FEED_SETS)
            w = weight[own_rows(first + pack), :]
            scaled = w * (diag[here, :] * (w * inverse[pack]))
            total = jnp.zeros((8, 128), jnp.float32)
            for part in range(2):
                value = w * whole(y[part, here, :]) + scaled * x[part, here, :]
                x[part, here, :] = value
                for row in range(0, FEED_SETS, 8):
                    total = total + value[row : row + 8] * value[row : row + 8]
            total = jnp.sum(total, axis=0, keepdims=True)
            squares[8 * pack : 8 * pack + 8, :] = jnp.broadcast_to(total, (8, 128))

        @pl.when(iteration < ITERS - 1)
        def _():
            forward_pass(tile, count, x, coeff, slots)

        return carry

    lax.fori_loop(0, ITERS, iterate, 0)
    for pack, length in enumerate(lengths()):
        here = slice(pack * FEED_SETS, (pack + 1) * FEED_SETS)
        for part in range(2):
            x[part, here, :] = x[part, here, :] / jnp.sqrt(length)


def kernel(
    volt, taps, twiddle, fine_upper, fine_lower, usable, auto_power, share, repeat, out,
    weight, power, lined, lined_back, wide, sent_half, held_half, kept, ext, halfway, upper, lower, stage, sent_pair, sent_one, held_pair, held_one,
    x, y, coeff, squares, diag, loads, send_sems, recv_sems, edge_sems,
):
    def arrange(source, target, split):
        feeds = FEED_SETS * FEEDS_HERE
        lane = lax.broadcasted_iota(jnp.int32, (FEED_SETS, feeds), 1)
        first = lax.broadcasted_iota(jnp.int32, (FEED_SETS, feeds), 0) * FEEDS_HERE
        mine = (lane >= first) & (lane < first + FEEDS_HERE)
        place = lax.broadcasted_iota(jnp.int32, (FEED_SETS, 128), 1)

        def body(pack, carry):
            for q in range(8):
                row = source[pl.ds(pack * 8 + q, 1), :].astype(jnp.float32)
                lined[q * FEED_SETS : (q + 1) * FEED_SETS, :] = jnp.where(mine, row, 0.0)
            value = lined[...]
            high = value.astype(jnp.bfloat16)
            wide = jnp.dot(high, repeat[...], preferred_element_type=jnp.float32)
            if split:
                rest = value - high.astype(jnp.float32)
                middle = rest.astype(jnp.bfloat16)
                low = (rest - middle.astype(jnp.float32)).astype(jnp.bfloat16)
                wide = wide + jnp.dot(middle, repeat[...], preferred_element_type=jnp.float32)
                wide = wide + jnp.dot(low, repeat[...], preferred_element_type=jnp.float32)
            total = jnp.zeros((FEED_SETS, 128), jnp.float32)
            for q in range(8):
                part = wide[q * FEED_SETS : (q + 1) * FEED_SETS]
                own = (place >= q * FEEDS_HERE) & (place < (q + 1) * FEEDS_HERE)
                total = total + jnp.where(own, part, 0.0)
            target[pl.ds(pl.multiple_of(pack * FEED_SETS, FEED_SETS), FEED_SETS), :] = total
            return carry

        lax.fori_loop(0, PACKS, body, 0)

    def arrange_back(pack, rows):
        feeds = FEED_SETS * FEEDS_HERE
        lane = lax.broadcasted_iota(jnp.int32, (FEED_SETS, feeds), 1)
        first = lax.broadcasted_iota(jnp.int32, (FEED_SETS, feeds), 0) * FEEDS_HERE
        mine = (lane >= first) & (lane < first + FEEDS_HERE)
        place = lax.broadcasted_iota(jnp.int32, (FEED_SETS, 128), 1)
        dims = (((1,), (1,)), ((), ()))
        for part in range(2):
            value = x[part, rows, :]
            for q in range(8):
                own = (place >= q * FEEDS_HERE) & (place < (q + 1) * FEEDS_HERE)
                lined_back[q * FEED_SETS : (q + 1) * FEED_SETS, :] = jnp.where(own, value, 0.0)
            rest = lined_back[...]
            total = jnp.zeros((8 * FEED_SETS, feeds), jnp.float32)
            for _ in range(2):
                piece = rest.astype(jnp.bfloat16)
                rest = rest - piece.astype(jnp.float32)
                total = total + lax.dot_general(
                    piece, repeat[...], dims, preferred_element_type=jnp.float32
                )
            for q in range(8):
                line = jnp.where(mine, total[q * FEED_SETS : (q + 1) * FEED_SETS], 0.0)
                out[part, pl.ds(pack * 8 + q, 1), :] = jnp.sum(line, axis=0, keepdims=True)

    section = lax.axis_index("section")
    chan = lax.axis_index("chan")
    core = lax.rem(chan, 2)
    before = 2 - core
    me = section * FEED_SETS + chan
    load = pltpu.make_async_copy(
        volt, ext.at[:, :, pl.ds(pl.multiple_of(before * CHANNELS, CHANNELS), LENGTH)], loads
    )
    load.start()
    barrier = pltpu.get_barrier_semaphore()

    def greet(there, column):
        pl.semaphore_signal(
            barrier, inc=1, device_id=(there, column), device_id_type=pl.DeviceIdType.MESH
        )

    visit(section, chan, greet)
    edges = []
    for kind in range(2):
        early, late = (2 - kind) * CHANNELS, (1 + kind) * CHANNELS
        pair = (edge_sems, edge_sems.at[pl.ds(2, 2)])
        edges.append((
            copy_at(
                volt.at[:, :, pl.ds(LENGTH - early, early)],
                ext.at[:, :, pl.ds(0, early)],
                pair,
                0,
                (lax.rem(section + 1, SECTIONS), chan),
            ),
            copy_at(
                volt.at[:, :, pl.ds(0, late)],
                ext.at[:, :, pl.ds(early + LENGTH, late)],
                pair,
                1,
                (lax.rem(section + SECTIONS - 1, SECTIONS), chan),
            ),
        ))
    pl.semaphore_wait(barrier, OWNERS - 1)
    for kind in range(2):

        @pl.when(core == kind)
        def _():
            edges[kind][0].start()
            edges[kind][1].start()

    load.wait()

    def clear(first, count):
        def body(at, inner):
            where = pl.ds(pl.multiple_of(first * CHANNELS + at * FINE, FINE), FINE)
            for part in range(2):
                ext[part, :, where] = jnp.zeros((FEEDS_HERE, FINE), jnp.bfloat16)
            return inner

        lax.fori_loop(0, count * COARSE, body, 0)

    def grouped(position, carry):
        group = lax.rem(position + 1, GROUPS)

        for kind in range(2):

            @pl.when((position == 2) & (core == kind))
            def _():
                edges[kind][1].wait()

            @pl.when((position == 3) & (core == kind))
            def _():
                edges[kind][0].wait()

        @pl.when((position == 3) & (section == 0))
        def _():
            clear(0, before)

        def step(at, inner):
            @pl.when((section == SECTIONS - 1) & (position == 2) & (at == GROUP - 1))
            def _():
                clear(BLOCKS_HERE - HALO + before, HALO)

            block = lax.rem(group * GROUP + at + core * (BLOCKS_HERE - 1), BLOCKS_HERE)
            first_transform(block, ext, taps, halfway)
            second_transform(twiddle, halfway, upper, lower)
            fine_transform(at, fine_upper, fine_lower, upper, lower, stage)
            return inner

        lax.fori_loop(0, GROUP, step, 0)

        def emit(owner, inner):
            rows = pl.ds(owner * STRIDE, 16)
            for pack in range(2):
                sent_pair[owner, group, pack] = stage[pack, rows, :].astype(jnp.bfloat16)
                sent_one[pack, owner, group] = stage[2 + pack, rows, :].astype(jnp.bfloat16)
            return inner

        lax.fori_loop(0, OWNERS, emit, 0, unroll=8)

        def send(there, column):
            pltpu.make_async_remote_copy(
                src_ref=sent_pair.at[there * FEED_SETS + column, group],
                dst_ref=held_pair.at[me, group],
                send_sem=send_sems.at[0],
                recv_sem=recv_sems.at[group],
                device_id=(there, column),
                device_id_type=pl.DeviceIdType.MESH,
            ).start()

        visit(section, chan, send)
        return carry

    lax.fori_loop(0, GROUPS, grouped, 0)

    def send_third(there, column):
        pltpu.make_async_remote_copy(
            src_ref=sent_one.at[0, there * FEED_SETS + column],
            dst_ref=held_one.at[0, me],
            send_sem=send_sems.at[1],
            recv_sem=recv_sems.at[2 * GROUPS],
            device_id=(there, column),
            device_id_type=pl.DeviceIdType.MESH,
        ).start()

    visit(section, chan, send_third)

    def low_lanes(shape):
        return lax.broadcasted_iota(jnp.int32, shape, 1) < 64

    def repack(owner, carry):
        low = low_lanes((16, 128))
        for pair in range(GROUPS // 2):
            one, two = [
                sent_one[1, owner, 2 * pair + at].astype(jnp.float32) for at in range(2)
            ]
            first = jnp.where(low, one, pltpu.roll(two, 64, 1))
            second = jnp.where(low, pltpu.roll(one, 64, 1), two)
            sent_half[0, owner, pair] = first.astype(jnp.bfloat16)
            sent_half[1, owner, pair] = second.astype(jnp.bfloat16)
        return carry

    lax.fori_loop(0, OWNERS, repack, 0, unroll=4)

    def rest(index, carry):
        half, pair = lax.div(index, 2), lax.rem(index, 2)

        def send(there, column):
            pltpu.make_async_remote_copy(
                src_ref=sent_half.at[half, there * FEED_SETS + column, pair],
                dst_ref=held_half.at[half, me, pair],
                send_sem=send_sems.at[2],
                recv_sem=recv_sems.at[GROUPS + index],
                device_id=(there, column),
                device_id_type=pl.DeviceIdType.MESH,
            ).start()

        visit(section, chan, send)
        return carry

    lax.fori_loop(0, 4, rest, 0)
    arrange(usable, weight, False)
    arrange(auto_power, power, True)
    for ref in (weight, power):
        value = ref[own_rows(3), :]
        other = pltpu.roll(value, 64, 1)
        low = low_lanes((FEED_SETS, 128))
        ref[own_rows(4), :] = jnp.where(low, value, other)
        ref[own_rows(5), :] = jnp.where(low, other, value)

    for group in range(GROUPS):
        for pack in range(2):
            held_pair[me, group, pack] = sent_pair[me, group, pack]
            held_half[pack, me, group // 2] = sent_half[pack, me, group // 2]
        held_one[0, me, group] = sent_one[0, me, group]

    others = pl.ds(0, OWNERS - 1)
    scratch = (weight, power, share, x, y, coeff, squares, diag)
    top_row = lax.broadcasted_iota(jnp.int32, (GROUP, 128), 0) == 0

    def tile(pack, slot, feed_set):
        at = (pack * SLOTS + slot) * FEED_SETS + feed_set
        return wide[at, 0], wide[at, 1]

    def begin(first, count):
        start_x(first, count, weight, x)
        diag[0 : count * FEED_SETS, :] = jnp.zeros((count * FEED_SETS, 128), jnp.float32)

    def take(read, group, count, mend, per=GROUPS):
        def arrive(index, sums):
            sums = list(sums)
            for pack in range(count):
                for near in range(2):
                    feed_set = index * 2 + near
                    row = pl.ds(pack * FEED_SETS + feed_set, 1)
                    weight_row = x[0, row, :]
                    values = []
                    for at in range(SECTIONS):
                        value = read(at * FEED_SETS + feed_set, pack).astype(jnp.float32)
                        values.append((value[0:GROUP], value[GROUP:]))
                    if group == 0 and near == 1:
                        values = [
                            tuple(jnp.where(mend, values[at - 1][c], values[at][c]) for c in range(2))
                            for at in range(SECTIONS)
                        ]
                    total = jnp.zeros((GROUP, 128), jnp.float32)
                    for at, (re, im) in enumerate(values):
                        place = (pack * SLOTS + at * per + group) * FEED_SETS + feed_set
                        wide[place, 0] = re
                        wide[place, 1] = im
                        total = total + (re * re + im * im)
                        own = 2 * (pack * SECTIONS + at)
                        sums[own] = sums[own] + re * weight_row
                        sums[own + 1] = sums[own + 1] - im * weight_row
                    diag[row, :] = diag[row, :] + jnp.sum(total, axis=0, keepdims=True)
            return tuple(sums)

        zero = jnp.zeros((GROUP, 128), jnp.float32)
        sums = lax.fori_loop(0, FEED_SETS // 2, arrive, (zero,) * (2 * SECTIONS * count))
        for pack in range(count):
            for at in range(SECTIONS):
                slot = pack * SLOTS + at * per + group
                own = 2 * (pack * SECTIONS + at)
                for part in range(2):
                    coeff[part, slot * GROUP : (slot + 1) * GROUP, :] = sums[own + part]

    begin(0, 2)
    for group in (1, 2, 3, 0):
        pltpu.make_async_copy(
            sent_pair.at[others, group], held_pair.at[others, group], recv_sems.at[group]
        ).wait()
        take(lambda source, pack: held_pair[source, group, pack], group, 2, top_row)
    solve_packs(tile, 0, 2, *scratch)
    for pack in range(2):
        arrange_back(pack, slice(pack * FEED_SETS, (pack + 1) * FEED_SETS))

    begin(2, 1)
    pltpu.make_async_copy(
        sent_one.at[0, others], held_one.at[0, others], recv_sems.at[2 * GROUPS]
    ).wait()
    for group in range(GROUPS):
        take(lambda source, pack: held_one[0, source, group], group, 1, top_row)
    solve_packs(tile, 2, 1, *scratch)
    arrange_back(2, slice(0, FEED_SETS))

    for half in range(2):
        begin(4 + half, 1)
        for pair in range(2):
            pltpu.make_async_copy(
                sent_half.at[half, others, pair],
                held_half.at[half, others, pair],
                recv_sems.at[GROUPS + 2 * half + pair],
            ).wait()
            low = top_row & low_lanes((GROUP, 128))
            take(lambda source, pack: held_half[half, source, pair], pair, 1, low, GROUPS // 2)
        solve_packs(tile, 4 + half, 1, *scratch, slots=SLOTS // 2)
        own = slice(0, FEED_SETS)
        for part in range(2):
            if half == 0:
                kept[part] = x[part, own, :]
            else:
                x[part, own, :] = jnp.where(low_lanes((FEED_SETS, 128)), kept[part], x[part, own, :])
    arrange_back(3, slice(0, FEED_SETS))
    pltpu.make_async_copy(sent_pair.at[others], held_pair.at[others], send_sems.at[0]).wait()
    for pack in range(2):
        pltpu.make_async_copy(
            sent_one.at[pack, others], held_one.at[pack, others], send_sems.at[1 + pack]
        ).wait()


def local(voltages, usable, auto_power):
    taps, twiddle, fine, share = tables()
    upper = fine.astype(jnp.bfloat16)
    lower = (fine - upper.astype(np.float32)).astype(jnp.bfloat16)
    rows = PACKS * FEED_SETS

    lane = np.arange(FEED_SETS * FEEDS_HERE)[:, None] % FEEDS_HERE
    repeat = (lane == np.arange(128)[None, :] % FEEDS_HERE).astype(jnp.bfloat16)
    vmem = pl.BlockSpec(memory_space=pltpu.VMEM)
    pair = pltpu.VMEM((OWNERS, GROUPS, 2, 16, 128), jnp.bfloat16)
    half = pltpu.VMEM((2, OWNERS, GROUPS // 2, 16, 128), jnp.bfloat16)
    one = pltpu.VMEM((2, OWNERS, GROUPS, 16, 128), jnp.bfloat16)
    return pl.pallas_call(
        kernel,
        out_shape=jax.ShapeDtypeStruct((2, PACKS * 8, FEED_SETS * FEEDS_HERE), jnp.float32),
        in_specs=[pl.BlockSpec(memory_space=pl.ANY)] + [vmem] * 8,
        out_specs=vmem,
        scratch_shapes=[
            pltpu.VMEM((rows + 2 * FEED_SETS, 128), jnp.float32),
            pltpu.VMEM((rows + 2 * FEED_SETS, 128), jnp.float32),
            pltpu.VMEM((8 * FEED_SETS, FEED_SETS * FEEDS_HERE), jnp.float32),
            pltpu.VMEM((8 * FEED_SETS, 128), jnp.float32),
            pltpu.VMEM((2 * SLOTS * FEED_SETS, 2, GROUP, 128), jnp.float32),
            half,
            half,
            pltpu.VMEM((2, FEED_SETS, 128), jnp.float32),
            pltpu.VMEM((2, FEEDS_HERE, LENGTH + HALO * CHANNELS), jnp.bfloat16),
            pltpu.VMEM((4, 8, 2, FEEDS_HERE, FINE), jnp.float32),
            pltpu.VMEM((COARSE * FEEDS_HERE, 256), jnp.bfloat16),
            pltpu.VMEM((COARSE * FEEDS_HERE, 256), jnp.bfloat16),
            pltpu.VMEM((PACKS, OWNERS * STRIDE + 8, 128), jnp.float32),
            pair,
            one,
            pair,
            one,
            pltpu.VMEM((2, 2 * FEED_SETS, 128), jnp.float32),
            pltpu.VMEM((2, 2 * FEED_SETS, 128), jnp.float32),
            pltpu.VMEM((2, 2 * SLOTS * GROUP, 128), jnp.float32),
            pltpu.VMEM((16, 128), jnp.float32),
            pltpu.VMEM((2 * FEED_SETS, 128), jnp.float32),
            pltpu.SemaphoreType.DMA,
            pltpu.SemaphoreType.DMA((3,)),
            pltpu.SemaphoreType.DMA((1 + 2 * GROUPS,)),
            pltpu.SemaphoreType.DMA((4,)),
        ],
        compiler_params=pltpu.CompilerParams(
            collective_id=0, has_side_effects=True, vmem_limit_bytes=56 * 1024 * 1024
        ),
        cost_estimate=pl.CostEstimate(flops=10**10, bytes_accessed=2 * 10**7, transcendentals=0),
    )(
        voltages, taps, twiddle, upper, lower,
        usable, auto_power, share.astype(jnp.bfloat16), repeat,
    )


def solution(mesh):
    in_specs = (
        P(None, "chan", "section"),
        P(("section", "chan"), None),
        P(("section", "chan"), None),
    )
    out_specs = P(None, ("section", "chan"), None)
    return jax.shard_map(local, mesh=mesh, in_specs=in_specs, out_specs=out_specs, check_vma=False)
```

```python
import functools
import math

import jax
import jax.numpy as jnp
import numpy as np
from jax import lax
from jax.experimental import pallas as pl
from jax.experimental.pallas import tpu as pltpu
from jax.sharding import PartitionSpec as P

CHANNELS = 4096
TAPS = 4
ITERS = 5
EPSILON = 1e-06

COARSE = 32
FINE = 128
FEEDS_HERE = 16
BLOCKS_HERE = 32
GROUP = 8
GROUPS = BLOCKS_HERE // GROUP
PACKS = 4
OWNERS = 128
SECTIONS = 4
FEED_SETS = 32
SLOTS = SECTIONS * GROUPS
STRIDE = 17
LENGTH = BLOCKS_HERE * CHANNELS
HALO = TAPS - 1


def tables():
    position = np.arange(TAPS * CHANNELS, dtype=np.float64)
    offset = (position - 0.5 * TAPS * CHANNELS + 0.5) / CHANNELS
    window = 0.5 - 0.5 * np.cos(2.0 * np.pi * (position + 0.5) / (TAPS * CHANNELS))
    taps = np.sin(np.pi * offset) / (np.pi * offset) * window
    taps = taps.reshape(TAPS * COARSE, FINE).astype(np.float32)
    angle = 2.0 * np.pi * np.outer(np.arange(COARSE), np.arange(FINE)) / CHANNELS
    twiddle = np.concatenate([np.cos(angle), np.sin(angle)], axis=0).astype(np.float32)
    angle = 2.0 * np.pi * (np.outer(np.arange(FINE), np.arange(FINE)) % FINE) / FINE
    cosine = np.cos(angle) / math.sqrt(CHANNELS)
    sine = np.sin(angle) / math.sqrt(CHANNELS)
    fine = np.block([[cosine, sine], [-sine, cosine]]).astype(np.float32)
    lane = np.arange(128)
    share = (lane[:, None] // FEEDS_HERE == lane[None, :] // FEEDS_HERE).astype(np.float32)
    return taps, twiddle, fine, share


def butterfly_4(x):
    (ar, ai), (br, bi), (cr, ci), (dr, di) = x
    pr, pi, qr, qi = ar + cr, ai + ci, ar - cr, ai - ci
    sr, si, tr, ti = br + dr, bi + di, br - dr, bi - di
    return [(pr + sr, pi + si), (qr + ti, qi - tr), (pr - sr, pi - si), (qr - ti, qi + tr)]


def turn(x, eighths_of_32):
    n = eighths_of_32 % 32
    re, im = x
    if n == 0:
        return re, im
    if n == 8:
        return im, -re
    if n == 16:
        return -re, -im
    if n == 24:
        return -im, re
    cosine, sine = math.cos(2 * math.pi * n / 32), math.sin(2 * math.pi * n / 32)
    if n % 4 == 0:
        h = math.sqrt(0.5)
        if n == 4:
            return (re + im) * h, (im - re) * h
        if n == 12:
            return (im - re) * h, (re + im) * -h
    return re * cosine + im * sine, im * cosine - re * sine


def butterfly_8(x):
    even = butterfly_4([x[0], x[2], x[4], x[6]])
    odd = butterfly_4([x[1], x[3], x[5], x[7]])
    low, high = [], []
    for k in range(4):
        er, ei = even[k]
        tr, ti = turn(odd[k], 4 * k)
        low.append((er + tr, ei + ti))
        high.append((er - tr, ei - ti))
    return low + high


def first_transform(block, ext, taps, halfway):
    start = block * CHANNELS
    for low in range(8):
        points = []
        for high in range(4):
            tile = 8 * high + low
            pair = []
            for part in range(2):
                total = None
                for tap in range(TAPS):
                    at = pl.multiple_of(start + (tap * COARSE + tile) * FINE, FINE)
                    row = tap * COARSE + tile
                    term = taps[row : row + 1, :] * ext[part, :, pl.ds(at, FINE)].astype(jnp.float32)
                    total = term if total is None else total + term
                pair.append(total)
            points.append(tuple(pair))
        for q, point in enumerate(butterfly_4(points)):
            re, im = turn(point, low * q)
            halfway[q, low, 0] = re
            halfway[q, low, 1] = im


def second_transform(twiddle, halfway, upper, lower):
    for q1 in range(4):
        points = [(halfway[q1, low, 0], halfway[q1, low, 1]) for low in range(8)]
        for q2, (re, im) in enumerate(butterfly_8(points)):
            q = q1 + 4 * q2
            if q > 0:
                cosine = twiddle[q : q + 1, :]
                sine = twiddle[COARSE + q : COARSE + q + 1, :]
                re, im = re * cosine + im * sine, im * cosine - re * sine
            for part, value in enumerate((re, im)):
                high = value.astype(jnp.bfloat16)
                low = (value - high.astype(jnp.float32)).astype(jnp.bfloat16)
                rows = slice(q * FEEDS_HERE, (q + 1) * FEEDS_HERE)
                lanes = slice(part * FINE, (part + 1) * FINE)
                upper[rows, lanes] = high
                lower[rows, lanes] = low


def fine_transform(at, fine_upper, fine_lower, upper, lower, stage):
    dims = (((1,), (1,)), ((), ()))
    for half in range(2):
        rows = slice(half * 256, (half + 1) * 256)
        high = upper[rows, :]
        low = lower[rows, :]
        out = lax.dot_general(fine_upper[...], high, dims, preferred_element_type=jnp.float32)
        out += lax.dot_general(fine_lower[...], high, dims, preferred_element_type=jnp.float32)
        out += lax.dot_general(fine_upper[...], low, dims, preferred_element_type=jnp.float32)
        for pack in range(2):
            for part in range(2):
                piece = out[part * FINE : (part + 1) * FINE, pack * 128 : (pack + 1) * 128]
                stage[2 * half + pack, pl.ds(part * GROUP + at, OWNERS, stride=STRIDE), :] = piece


def visit(section, chan, action):
    row, column = lax.div(chan, 8), lax.rem(lax.div(chan, 2), 4)

    def turns(near, core):
        x = [lax.rem(section + near[0] + 2 * far, SECTIONS) for far in range(2)]
        y = [lax.rem(row + near[1] + 2 * far, 4) * 8 for far in range(2)]
        z = [lax.rem(column + near[2] + 2 * far, 4) * 2 + core for far in range(2)]
        return x, y, z

    def several(x, y, z, skip):
        for step in range(skip, 8):
            action(x[step % 2], y[step // 2 % 2] + z[step // 4])

    same = lax.rem(chan, 2)
    several(*turns((0, 0, 0), same), 1)

    def body(index, carry):
        step = index + same * (16 - 2 * index)
        near = [lax.rem(lax.div(step, 2), 2), lax.rem(lax.div(step, 4), 2), lax.rem(lax.div(step, 8), 2)]
        core = lax.rem(same + step, 2)
        several(*turns(near, core), 0)
        return carry

    lax.fori_loop(1, 16, body, 0)


def copy_at(source, target, sems, at, device):
    return pltpu.make_async_remote_copy(
        src_ref=source,
        dst_ref=target,
        send_sem=sems[0].at[at],
        recv_sem=sems[1].at[at],
        device_id=device,
        device_id_type=pl.DeviceIdType.MESH,
    )


def share_dot(value, share):
    high = value.astype(jnp.bfloat16)
    low = (value - high.astype(jnp.float32)).astype(jnp.bfloat16)
    total = jnp.dot(high, share, preferred_element_type=jnp.float32)
    return total + jnp.dot(low, share, preferred_element_type=jnp.float32)


def own_rows(pack, count=1):
    return pl.ds(pl.multiple_of(pack * FEED_SETS, FEED_SETS), count * FEED_SETS)


def forward_pass(tile, count, x, coeff, slots):
    for pack in range(count):

        def forward(index, inner):
            pr = [jnp.zeros((GROUP, 128), jnp.float32) for _ in range(8)]
            pi = [jnp.zeros((GROUP, 128), jnp.float32) for _ in range(8)]
            for feed_set in range(FEED_SETS):
                at = pack * FEED_SETS + feed_set
                xr = x[0, at : at + 1, :]
                xi = x[1, at : at + 1, :]
                for two in range(4):
                    re, im = tile(pack, index * 4 + two, feed_set)
                    pr[two] = pr[two] + re * xr
                    pr[4 + two] = pr[4 + two] + im * xi
                    pi[two] = pi[two] + re * xi
                    pi[4 + two] = pi[4 + two] - im * xr
            at = pl.multiple_of((pack * SLOTS + index * 4) * GROUP, 4 * GROUP)
            for two in range(4):
                coeff[0, pl.ds(at + two * GROUP, GROUP), :] = pr[two] + pr[4 + two]
                coeff[1, pl.ds(at + two * GROUP, GROUP), :] = pi[two] + pi[4 + two]
            return inner

        lax.fori_loop(0, slots // 4, forward, 0)


def start_x(first, count, weight, x):
    span = slice(0, count * FEED_SETS)
    x[0, span, :] = weight[own_rows(first, count), :]
    x[1, span, :] = jnp.zeros((count * FEED_SETS, 128), jnp.float32)


def solve_packs(
    tile, first, count, weight, power, share, x, y, coeff, squares, diag, slots=SLOTS
):
    span = slice(0, count * FEED_SETS)

    def whole(value):
        return value if slots == SLOTS else value + pltpu.roll(value, 64, 1)

    diag[span, :] = float(SLOTS * GROUP) * power[own_rows(first, count), :] - whole(diag[span, :])
    squares[...] = jnp.zeros_like(squares)

    def lengths():
        total = share_dot(squares[...], share[...])
        return [jnp.sqrt(total[8 * pack : 8 * pack + 1] + EPSILON) for pack in range(count)]

    def iterate(iteration, carry):
        inverse = [jnp.where(iteration == 0, 1.0, 1.0 / length) for length in lengths()]
        for pack in range(count):
            rows = slice(pack * SLOTS * GROUP, (pack * SLOTS + slots) * GROUP)
            for part in range(2):
                coeff[part, rows, :] = share_dot(coeff[part, rows, :], share[...]) * inverse[pack]
        for pack in range(count):

            def backward(index, inner):
                yr = [jnp.zeros((GROUP, 128), jnp.float32) for _ in range(8)]
                yi = [jnp.zeros((GROUP, 128), jnp.float32) for _ in range(8)]
                for slot in range(slots):
                    at = (pack * SLOTS + slot) * GROUP
                    pr = coeff[0, at : at + GROUP, :]
                    pi = coeff[1, at : at + GROUP, :]
                    for two in range(4):
                        re, im = tile(pack, slot, index * 4 + two)
                        yr[two] = yr[two] + re * pr
                        yr[4 + two] = yr[4 + two] - im * pi
                        yi[two] = yi[two] + re * pi
                        yi[4 + two] = yi[4 + two] + im * pr
                for two in range(4):
                    at = pl.ds(pack * FEED_SETS + index * 4 + two, 1)
                    y[0, at, :] = jnp.sum(yr[two] + yr[4 + two], axis=0, keepdims=True)
                    y[1, at, :] = jnp.sum(yi[two] + yi[4 + two], axis=0, keepdims=True)
                return inner

            lax.fori_loop(0, FEED_SETS // 4, backward, 0)
        for pack in range(count):
            here = slice(pack * FEED_SETS, (pack + 1) * FEED_SETS)
            w = weight[own_rows(first + pack), :]
            scaled = w * (diag[here, :] * (w * inverse[pack]))
            total = jnp.zeros((8, 128), jnp.float32)
            for part in range(2):
                value = w * whole(y[part, here, :]) + scaled * x[part, here, :]
                x[part, here, :] = value
                for row in range(0, FEED_SETS, 8):
                    total = total + value[row : row + 8] * value[row : row + 8]
            total = jnp.sum(total, axis=0, keepdims=True)
            squares[8 * pack : 8 * pack + 8, :] = jnp.broadcast_to(total, (8, 128))

        @pl.when(iteration < ITERS - 1)
        def _():
            forward_pass(tile, count, x, coeff, slots)

        return carry

    lax.fori_loop(0, ITERS, iterate, 0)
    for pack, length in enumerate(lengths()):
        here = slice(pack * FEED_SETS, (pack + 1) * FEED_SETS)
        for part in range(2):
            x[part, here, :] = x[part, here, :] / jnp.sqrt(length)


def kernel(
    volt, taps, twiddle, fine_upper, fine_lower, usable, auto_power, share, repeat, out,
    weight, power, lined, lined_back, wide, sent_half, held_half, kept, ext, halfway, upper, lower, stage, sent_pair, sent_one, held_pair, held_one,
    x, y, coeff, squares, diag, loads, send_sems, recv_sems, edge_sems,
):
    def arrange(source, target, split):
        feeds = FEED_SETS * FEEDS_HERE
        lane = lax.broadcasted_iota(jnp.int32, (FEED_SETS, feeds), 1)
        first = lax.broadcasted_iota(jnp.int32, (FEED_SETS, feeds), 0) * FEEDS_HERE
        mine = (lane >= first) & (lane < first + FEEDS_HERE)
        place = lax.broadcasted_iota(jnp.int32, (FEED_SETS, 128), 1)

        def body(pack, carry):
            for q in range(8):
                row = source[pl.ds(pack * 8 + q, 1), :].astype(jnp.float32)
                lined[q * FEED_SETS : (q + 1) * FEED_SETS, :] = jnp.where(mine, row, 0.0)
            value = lined[...]
            high = value.astype(jnp.bfloat16)
            wide = jnp.dot(high, repeat[...], preferred_element_type=jnp.float32)
            if split:
                rest = value - high.astype(jnp.float32)
                middle = rest.astype(jnp.bfloat16)
                low = (rest - middle.astype(jnp.float32)).astype(jnp.bfloat16)
                wide = wide + jnp.dot(middle, repeat[...], preferred_element_type=jnp.float32)
                wide = wide + jnp.dot(low, repeat[...], preferred_element_type=jnp.float32)
            total = jnp.zeros((FEED_SETS, 128), jnp.float32)
            for q in range(8):
                part = wide[q * FEED_SETS : (q + 1) * FEED_SETS]
                own = (place >= q * FEEDS_HERE) & (place < (q + 1) * FEEDS_HERE)
                total = total + jnp.where(own, part, 0.0)
            target[pl.ds(pl.multiple_of(pack * FEED_SETS, FEED_SETS), FEED_SETS), :] = total
            return carry

        lax.fori_loop(0, PACKS, body, 0)

    def arrange_back(pack, rows):
        feeds = FEED_SETS * FEEDS_HERE
        lane = lax.broadcasted_iota(jnp.int32, (FEED_SETS, feeds), 1)
        first = lax.broadcasted_iota(jnp.int32, (FEED_SETS, feeds), 0) * FEEDS_HERE
        mine = (lane >= first) & (lane < first + FEEDS_HERE)
        place = lax.broadcasted_iota(jnp.int32, (FEED_SETS, 128), 1)
        dims = (((1,), (1,)), ((), ()))
        for part in range(2):
            value = x[part, rows, :]
            for q in range(8):
                own = (place >= q * FEEDS_HERE) & (place < (q + 1) * FEEDS_HERE)
                lined_back[q * FEED_SETS : (q + 1) * FEED_SETS, :] = jnp.where(own, value, 0.0)
            rest = lined_back[...]
            total = jnp.zeros((8 * FEED_SETS, feeds), jnp.float32)
            for _ in range(2):
                piece = rest.astype(jnp.bfloat16)
                rest = rest - piece.astype(jnp.float32)
                total = total + lax.dot_general(
                    piece, repeat[...], dims, preferred_element_type=jnp.float32
                )
            for q in range(8):
                line = jnp.where(mine, total[q * FEED_SETS : (q + 1) * FEED_SETS], 0.0)
                out[part, pl.ds(pack * 8 + q, 1), :] = jnp.sum(line, axis=0, keepdims=True)

    section = lax.axis_index("section")
    chan = lax.axis_index("chan")
    core = lax.rem(chan, 2)
    before = 2 - core
    me = section * FEED_SETS + chan
    load = pltpu.make_async_copy(
        volt, ext.at[:, :, pl.ds(pl.multiple_of(before * CHANNELS, CHANNELS), LENGTH)], loads
    )
    load.start()
    barrier = pltpu.get_barrier_semaphore()

    def greet(there, column):
        pl.semaphore_signal(
            barrier, inc=1, device_id=(there, column), device_id_type=pl.DeviceIdType.MESH
        )

    visit(section, chan, greet)
    edges = []
    for kind in range(2):
        early, late = (2 - kind) * CHANNELS, (1 + kind) * CHANNELS
        pair = (edge_sems, edge_sems.at[pl.ds(2, 2)])
        edges.append((
            copy_at(
                volt.at[:, :, pl.ds(LENGTH - early, early)],
                ext.at[:, :, pl.ds(0, early)],
                pair,
                0,
                (lax.rem(section + 1, SECTIONS), chan),
            ),
            copy_at(
                volt.at[:, :, pl.ds(0, late)],
                ext.at[:, :, pl.ds(early + LENGTH, late)],
                pair,
                1,
                (lax.rem(section + SECTIONS - 1, SECTIONS), chan),
            ),
        ))
    pl.semaphore_wait(barrier, OWNERS - 1)
    for kind in range(2):

        @pl.when(core == kind)
        def _():
            edges[kind][0].start()
            edges[kind][1].start()

    load.wait()

    def clear(first, count):
        def body(at, inner):
            where = pl.ds(pl.multiple_of(first * CHANNELS + at * FINE, FINE), FINE)
            for part in range(2):
                ext[part, :, where] = jnp.zeros((FEEDS_HERE, FINE), jnp.bfloat16)
            return inner

        lax.fori_loop(0, count * COARSE, body, 0)

    def grouped(position, carry):
        group = lax.rem(position + 1, GROUPS)

        for kind in range(2):

            @pl.when((position == 2) & (core == kind))
            def _():
                edges[kind][1].wait()

            @pl.when((position == 3) & (core == kind))
            def _():
                edges[kind][0].wait()

        @pl.when((position == 3) & (section == 0))
        def _():
            clear(0, before)

        def step(at, inner):
            @pl.when((section == SECTIONS - 1) & (position == 2) & (at == GROUP - 1))
            def _():
                clear(BLOCKS_HERE - HALO + before, HALO)

            block = lax.rem(group * GROUP + at + core * (BLOCKS_HERE - 1), BLOCKS_HERE)
            first_transform(block, ext, taps, halfway)
            second_transform(twiddle, halfway, upper, lower)
            fine_transform(at, fine_upper, fine_lower, upper, lower, stage)
            return inner

        lax.fori_loop(0, GROUP, step, 0)

        def emit(owner, inner):
            rows = pl.ds(owner * STRIDE, 16)
            for pack in range(2):
                sent_pair[owner, group, pack] = stage[pack, rows, :].astype(jnp.bfloat16)
                sent_one[pack, owner, group] = stage[2 + pack, rows, :].astype(jnp.bfloat16)
            return inner

        lax.fori_loop(0, OWNERS, emit, 0, unroll=8)

        def send(there, column):
            pltpu.make_async_remote_copy(
                src_ref=sent_pair.at[there * FEED_SETS + column, group],
                dst_ref=held_pair.at[me, group],
                send_sem=send_sems.at[0],
                recv_sem=recv_sems.at[group],
                device_id=(there, column),
                device_id_type=pl.DeviceIdType.MESH,
            ).start()

        visit(section, chan, send)
        return carry

    lax.fori_loop(0, GROUPS, grouped, 0)

    def send_third(there, column):
        pltpu.make_async_remote_copy(
            src_ref=sent_one.at[0, there * FEED_SETS + column],
            dst_ref=held_one.at[0, me],
            send_sem=send_sems.at[1],
            recv_sem=recv_sems.at[2 * GROUPS],
            device_id=(there, column),
            device_id_type=pl.DeviceIdType.MESH,
        ).start()

    visit(section, chan, send_third)

    def low_lanes(shape):
        return lax.broadcasted_iota(jnp.int32, shape, 1) < 64

    def repack(owner, carry):
        low = low_lanes((16, 128))
        for pair in range(GROUPS // 2):
            one, two = [
                sent_one[1, owner, 2 * pair + at].astype(jnp.float32) for at in range(2)
            ]
            first = jnp.where(low, one, pltpu.roll(two, 64, 1))
            second = jnp.where(low, pltpu.roll(one, 64, 1), two)
            sent_half[0, owner, pair] = first.astype(jnp.bfloat16)
            sent_half[1, owner, pair] = second.astype(jnp.bfloat16)
        return carry

    lax.fori_loop(0, OWNERS, repack, 0, unroll=4)

    def rest(index, carry):
        half, pair = lax.div(index, 2), lax.rem(index, 2)

        def send(there, column):
            pltpu.make_async_remote_copy(
                src_ref=sent_half.at[half, there * FEED_SETS + column, pair],
                dst_ref=held_half.at[half, me, pair],
                send_sem=send_sems.at[2],
                recv_sem=recv_sems.at[GROUPS + index],
                device_id=(there, column),
                device_id_type=pl.DeviceIdType.MESH,
            ).start()

        visit(section, chan, send)
        return carry

    lax.fori_loop(0, 4, rest, 0)
    arrange(usable, weight, False)
    arrange(auto_power, power, True)
    for ref in (weight, power):
        value = ref[own_rows(3), :]
        other = pltpu.roll(value, 64, 1)
        low = low_lanes((FEED_SETS, 128))
        ref[own_rows(4), :] = jnp.where(low, value, other)
        ref[own_rows(5), :] = jnp.where(low, other, value)

    for group in range(GROUPS):
        for pack in range(2):
            held_pair[me, group, pack] = sent_pair[me, group, pack]
            held_half[pack, me, group // 2] = sent_half[pack, me, group // 2]
        held_one[0, me, group] = sent_one[0, me, group]

    others = pl.ds(0, OWNERS - 1)
    scratch = (weight, power, share, x, y, coeff, squares, diag)
    top_row = lax.broadcasted_iota(jnp.int32, (GROUP, 128), 0) == 0

    def tile(pack, slot, feed_set):
        at = (pack * SLOTS + slot) * FEED_SETS + feed_set
        return wide[at, 0], wide[at, 1]

    def begin(first, count):
        start_x(first, count, weight, x)
        diag[0 : count * FEED_SETS, :] = jnp.zeros((count * FEED_SETS, 128), jnp.float32)

    def take(read, group, count, mend, per=GROUPS):
        def arrive(index, sums):
            sums = list(sums)
            for pack in range(count):
                for near in range(2):
                    feed_set = index * 2 + near
                    row = pl.ds(pack * FEED_SETS + feed_set, 1)
                    weight_row = x[0, row, :]
                    values = []
                    for at in range(SECTIONS):
                        value = read(at * FEED_SETS + feed_set, pack).astype(jnp.float32)
                        values.append((value[0:GROUP], value[GROUP:]))
                    if group == 0 and near == 1:
                        values = [
                            tuple(jnp.where(mend, values[at - 1][c], values[at][c]) for c in range(2))
                            for at in range(SECTIONS)
                        ]
                    total = jnp.zeros((GROUP, 128), jnp.float32)
                    for at, (re, im) in enumerate(values):
                        place = (pack * SLOTS + at * per + group) * FEED_SETS + feed_set
                        wide[place, 0] = re
                        wide[place, 1] = im
                        total = total + (re * re + im * im)
                        own = 2 * (pack * SECTIONS + at)
                        sums[own] = sums[own] + re * weight_row
                        sums[own + 1] = sums[own + 1] - im * weight_row
                    diag[row, :] = diag[row, :] + jnp.sum(total, axis=0, keepdims=True)
            return tuple(sums)

        zero = jnp.zeros((GROUP, 128), jnp.float32)
        sums = lax.fori_loop(0, FEED_SETS // 2, arrive, (zero,) * (2 * SECTIONS * count))
        for pack in range(count):
            for at in range(SECTIONS):
                slot = pack * SLOTS + at * per + group
                own = 2 * (pack * SECTIONS + at)
                for part in range(2):
                    coeff[part, slot * GROUP : (slot + 1) * GROUP, :] = sums[own + part]

    begin(0, 2)
    for group in (1, 2, 3, 0):
        pltpu.make_async_copy(
            sent_pair.at[others, group], held_pair.at[others, group], recv_sems.at[group]
        ).wait()
        take(lambda source, pack: held_pair[source, group, pack], group, 2, top_row)
    solve_packs(tile, 0, 2, *scratch)
    for pack in range(2):
        arrange_back(pack, slice(pack * FEED_SETS, (pack + 1) * FEED_SETS))

    begin(2, 1)
    pltpu.make_async_copy(
        sent_one.at[0, others], held_one.at[0, others], recv_sems.at[2 * GROUPS]
    ).wait()
    for group in range(GROUPS):
        take(lambda source, pack: held_one[0, source, group], group, 1, top_row)
    solve_packs(tile, 2, 1, *scratch)
    arrange_back(2, slice(0, FEED_SETS))

    for half in range(2):
        begin(4 + half, 1)
        for pair in range(2):
            pltpu.make_async_copy(
                sent_half.at[half, others, pair],
                held_half.at[half, others, pair],
                recv_sems.at[GROUPS + 2 * half + pair],
            ).wait()
            low = top_row & low_lanes((GROUP, 128))
            take(lambda source, pack: held_half[half, source, pair], pair, 1, low, GROUPS // 2)
        solve_packs(tile, 4 + half, 1, *scratch, slots=SLOTS // 2)
        own = slice(0, FEED_SETS)
        for part in range(2):
            if half == 0:
                kept[part] = x[part, own, :]
            else:
                x[part, own, :] = jnp.where(low_lanes((FEED_SETS, 128)), kept[part], x[part, own, :])
    arrange_back(3, slice(0, FEED_SETS))
    pltpu.make_async_copy(sent_pair.at[others], held_pair.at[others], send_sems.at[0]).wait()
    for pack in range(2):
        pltpu.make_async_copy(
            sent_one.at[pack, others], held_one.at[pack, others], send_sems.at[1 + pack]
        ).wait()


def local(voltages, usable, auto_power):
    taps, twiddle, fine, share = tables()
    upper = fine.astype(jnp.bfloat16)
    lower = (fine - upper.astype(np.float32)).astype(jnp.bfloat16)
    rows = PACKS * FEED_SETS

    lane = np.arange(FEED_SETS * FEEDS_HERE)[:, None] % FEEDS_HERE
    repeat = (lane == np.arange(128)[None, :] % FEEDS_HERE).astype(jnp.bfloat16)
    vmem = pl.BlockSpec(memory_space=pltpu.VMEM)
    pair = pltpu.VMEM((OWNERS, GROUPS, 2, 16, 128), jnp.bfloat16)
    half = pltpu.VMEM((2, OWNERS, GROUPS // 2, 16, 128), jnp.bfloat16)
    one = pltpu.VMEM((2, OWNERS, GROUPS, 16, 128), jnp.bfloat16)
    return pl.pallas_call(
        kernel,
        out_shape=jax.ShapeDtypeStruct((2, PACKS * 8, FEED_SETS * FEEDS_HERE), jnp.float32),
        in_specs=[pl.BlockSpec(memory_space=pl.ANY)] + [vmem] * 8,
        out_specs=vmem,
        scratch_shapes=[
            pltpu.VMEM((rows + 2 * FEED_SETS, 128), jnp.float32),
            pltpu.VMEM((rows + 2 * FEED_SETS, 128), jnp.float32),
            pltpu.VMEM((8 * FEED_SETS, FEED_SETS * FEEDS_HERE), jnp.float32),
            pltpu.VMEM((8 * FEED_SETS, 128), jnp.float32),
            pltpu.VMEM((2 * SLOTS * FEED_SETS, 2, GROUP, 128), jnp.float32),
            half,
            half,
            pltpu.VMEM((2, FEED_SETS, 128), jnp.float32),
            pltpu.VMEM((2, FEEDS_HERE, LENGTH + HALO * CHANNELS), jnp.bfloat16),
            pltpu.VMEM((4, 8, 2, FEEDS_HERE, FINE), jnp.float32),
            pltpu.VMEM((COARSE * FEEDS_HERE, 256), jnp.bfloat16),
            pltpu.VMEM((COARSE * FEEDS_HERE, 256), jnp.bfloat16),
            pltpu.VMEM((PACKS, OWNERS * STRIDE + 8, 128), jnp.float32),
            pair,
            one,
            pair,
            one,
            pltpu.VMEM((2, 2 * FEED_SETS, 128), jnp.float32),
            pltpu.VMEM((2, 2 * FEED_SETS, 128), jnp.float32),
            pltpu.VMEM((2, 2 * SLOTS * GROUP, 128), jnp.float32),
            pltpu.VMEM((16, 128), jnp.float32),
            pltpu.VMEM((2 * FEED_SETS, 128), jnp.float32),
            pltpu.SemaphoreType.DMA,
            pltpu.SemaphoreType.DMA((3,)),
            pltpu.SemaphoreType.DMA((1 + 2 * GROUPS,)),
            pltpu.SemaphoreType.DMA((4,)),
        ],
        compiler_params=pltpu.CompilerParams(
            collective_id=0, has_side_effects=True, vmem_limit_bytes=56 * 1024 * 1024
        ),
        cost_estimate=pl.CostEstimate(flops=10**10, bytes_accessed=2 * 10**7, transcendentals=0),
    )(
        voltages, taps, twiddle, upper, lower,
        usable, auto_power, share.astype(jnp.bfloat16), repeat,
    )


def solution(mesh):
    in_specs = (
        P(None, "chan", "section"),
        P(("section", "chan"), None),
        P(("section", "chan"), None),
    )
    out_specs = P(None, ("section", "chan"), None)
    return jax.shard_map(local, mesh=mesh, in_specs=in_specs, out_specs=out_specs, check_vma=False)
```

```python
import functools
import math

import jax
import jax.numpy as jnp
import numpy as np
from jax import lax
from jax.experimental import pallas as pl
from jax.experimental.pallas import tpu as pltpu
from jax.sharding import PartitionSpec as P

CHANNELS = 4096
TAPS = 4
ITERS = 5
EPSILON = 1e-06

COARSE = 32
FINE = 128
FEEDS_HERE = 16
BLOCKS_HERE = 32
GROUP = 8
GROUPS = BLOCKS_HERE // GROUP
PACKS = 4
OWNERS = 128
SECTIONS = 4
FEED_SETS = 32
SLOTS = SECTIONS * GROUPS
STRIDE = 17
LENGTH = BLOCKS_HERE * CHANNELS
HALO = TAPS - 1


def tables():
    position = np.arange(TAPS * CHANNELS, dtype=np.float64)
    offset = (position - 0.5 * TAPS * CHANNELS + 0.5) / CHANNELS
    window = 0.5 - 0.5 * np.cos(2.0 * np.pi * (position + 0.5) / (TAPS * CHANNELS))
    taps = np.sin(np.pi * offset) / (np.pi * offset) * window
    taps = taps.reshape(TAPS * COARSE, FINE).astype(np.float32)
    angle = 2.0 * np.pi * np.outer(np.arange(COARSE), np.arange(FINE)) / CHANNELS
    twiddle = np.concatenate([np.cos(angle), np.sin(angle)], axis=0).astype(np.float32)
    angle = 2.0 * np.pi * (np.outer(np.arange(FINE), np.arange(FINE)) % FINE) / FINE
    cosine = np.cos(angle) / math.sqrt(CHANNELS)
    sine = np.sin(angle) / math.sqrt(CHANNELS)
    fine = np.block([[cosine, sine], [-sine, cosine]]).astype(np.float32)
    lane = np.arange(128)
    share = (lane[:, None] // FEEDS_HERE == lane[None, :] // FEEDS_HERE).astype(np.float32)
    return taps, twiddle, fine, share


def butterfly_4(x):
    (ar, ai), (br, bi), (cr, ci), (dr, di) = x
    pr, pi, qr, qi = ar + cr, ai + ci, ar - cr, ai - ci
    sr, si, tr, ti = br + dr, bi + di, br - dr, bi - di
    return [(pr + sr, pi + si), (qr + ti, qi - tr), (pr - sr, pi - si), (qr - ti, qi + tr)]


def turn(x, eighths_of_32):
    n = eighths_of_32 % 32
    re, im = x
    if n == 0:
        return re, im
    if n == 8:
        return im, -re
    if n == 16:
        return -re, -im
    if n == 24:
        return -im, re
    cosine, sine = math.cos(2 * math.pi * n / 32), math.sin(2 * math.pi * n / 32)
    if n % 4 == 0:
        h = math.sqrt(0.5)
        if n == 4:
            return (re + im) * h, (im - re) * h
        if n == 12:
            return (im - re) * h, (re + im) * -h
    return re * cosine + im * sine, im * cosine - re * sine


def butterfly_8(x):
    even = butterfly_4([x[0], x[2], x[4], x[6]])
    odd = butterfly_4([x[1], x[3], x[5], x[7]])
    low, high = [], []
    for k in range(4):
        er, ei = even[k]
        tr, ti = turn(odd[k], 4 * k)
        low.append((er + tr, ei + ti))
        high.append((er - tr, ei - ti))
    return low + high


def first_transform(block, ext, taps, halfway):
    start = block * CHANNELS
    for low in range(8):
        points = []
        for high in range(4):
            tile = 8 * high + low
            pair = []
            for part in range(2):
                total = None
                for tap in range(TAPS):
                    at = pl.multiple_of(start + (tap * COARSE + tile) * FINE, FINE)
                    row = tap * COARSE + tile
                    term = taps[row : row + 1, :] * ext[part, :, pl.ds(at, FINE)].astype(jnp.float32)
                    total = term if total is None else total + term
                pair.append(total)
            points.append(tuple(pair))
        for q, point in enumerate(butterfly_4(points)):
            re, im = turn(point, low * q)
            halfway[q, low, 0] = re
            halfway[q, low, 1] = im


def second_transform(twiddle, halfway, upper, lower):
    for q1 in range(4):
        points = [(halfway[q1, low, 0], halfway[q1, low, 1]) for low in range(8)]
        for q2, (re, im) in enumerate(butterfly_8(points)):
            q = q1 + 4 * q2
            if q > 0:
                cosine = twiddle[q : q + 1, :]
                sine = twiddle[COARSE + q : COARSE + q + 1, :]
                re, im = re * cosine + im * sine, im * cosine - re * sine
            for part, value in enumerate((re, im)):
                high = value.astype(jnp.bfloat16)
                low = (value - high.astype(jnp.float32)).astype(jnp.bfloat16)
                rows = slice(q * FEEDS_HERE, (q + 1) * FEEDS_HERE)
                lanes = slice(part * FINE, (part + 1) * FINE)
                upper[rows, lanes] = high
                lower[rows, lanes] = low


def fine_transform(at, fine_upper, fine_lower, upper, lower, stage):
    dims = (((1,), (1,)), ((), ()))
    for half in range(2):
        rows = slice(half * 256, (half + 1) * 256)
        high = upper[rows, :]
        low = lower[rows, :]
        out = lax.dot_general(fine_upper[...], high, dims, preferred_element_type=jnp.float32)
        out += lax.dot_general(fine_lower[...], high, dims, preferred_element_type=jnp.float32)
        out += lax.dot_general(fine_upper[...], low, dims, preferred_element_type=jnp.float32)
        for pack in range(2):
            for part in range(2):
                piece = out[part * FINE : (part + 1) * FINE, pack * 128 : (pack + 1) * 128]
                stage[2 * half + pack, pl.ds(part * GROUP + at, OWNERS, stride=STRIDE), :] = piece


def visit(section, chan, action):
    row, column = lax.div(chan, 8), lax.rem(lax.div(chan, 2), 4)

    def turns(near, core):
        x = [lax.rem(section + near[0] + 2 * far, SECTIONS) for far in range(2)]
        y = [lax.rem(row + near[1] + 2 * far, 4) * 8 for far in range(2)]
        z = [lax.rem(column + near[2] + 2 * far, 4) * 2 + core for far in range(2)]
        return x, y, z

    def several(x, y, z, skip):
        for step in range(skip, 8):
            action(x[step % 2], y[step // 2 % 2] + z[step // 4])

    same = lax.rem(chan, 2)
    several(*turns((0, 0, 0), same), 1)

    def body(index, carry):
        mixed = lax.rem(index * 5, 16)
        step = mixed + same * (16 - 2 * mixed)
        near = [lax.rem(lax.div(step, 2), 2), lax.rem(lax.div(step, 4), 2), lax.rem(lax.div(step, 8), 2)]
        core = lax.rem(same + step, 2)
        several(*turns(near, core), 0)
        return carry

    lax.fori_loop(1, 16, body, 0)


def copy_at(source, target, sems, at, device):
    return pltpu.make_async_remote_copy(
        src_ref=source,
        dst_ref=target,
        send_sem=sems[0].at[at],
        recv_sem=sems[1].at[at],
        device_id=device,
        device_id_type=pl.DeviceIdType.MESH,
    )


def share_dot(value, share):
    high = value.astype(jnp.bfloat16)
    low = (value - high.astype(jnp.float32)).astype(jnp.bfloat16)
    total = jnp.dot(high, share, preferred_element_type=jnp.float32)
    return total + jnp.dot(low, share, preferred_element_type=jnp.float32)


def own_rows(pack, count=1):
    return pl.ds(pl.multiple_of(pack * FEED_SETS, FEED_SETS), count * FEED_SETS)


def forward_pass(tile, count, x, coeff, slots):
    for pack in range(count):

        def forward(index, inner):
            pr = [jnp.zeros((GROUP, 128), jnp.float32) for _ in range(8)]
            pi = [jnp.zeros((GROUP, 128), jnp.float32) for _ in range(8)]
            for feed_set in range(FEED_SETS):
                at = pack * FEED_SETS + feed_set
                xr = x[0, at : at + 1, :]
                xi = x[1, at : at + 1, :]
                for two in range(4):
                    re, im = tile(pack, index * 4 + two, feed_set)
                    pr[two] = pr[two] + re * xr
                    pr[4 + two] = pr[4 + two] + im * xi
                    pi[two] = pi[two] + re * xi
                    pi[4 + two] = pi[4 + two] - im * xr
            at = pl.multiple_of((pack * SLOTS + index * 4) * GROUP, 4 * GROUP)
            for two in range(4):
                coeff[0, pl.ds(at + two * GROUP, GROUP), :] = pr[two] + pr[4 + two]
                coeff[1, pl.ds(at + two * GROUP, GROUP), :] = pi[two] + pi[4 + two]
            return inner

        lax.fori_loop(0, slots // 4, forward, 0)


def start_x(first, count, weight, x):
    span = slice(0, count * FEED_SETS)
    x[0, span, :] = weight[own_rows(first, count), :]
    x[1, span, :] = jnp.zeros((count * FEED_SETS, 128), jnp.float32)


def solve_packs(
    tile, first, count, weight, power, share, x, y, coeff, squares, diag, slots=SLOTS
):
    span = slice(0, count * FEED_SETS)

    def whole(value):
        return value if slots == SLOTS else value + pltpu.roll(value, 64, 1)

    diag[span, :] = float(SLOTS * GROUP) * power[own_rows(first, count), :] - whole(diag[span, :])
    squares[...] = jnp.zeros_like(squares)

    def lengths():
        total = share_dot(squares[...], share[...])
        return [jnp.sqrt(total[8 * pack : 8 * pack + 1] + EPSILON) for pack in range(count)]

    def iterate(iteration, carry):
        inverse = [jnp.where(iteration == 0, 1.0, 1.0 / length) for length in lengths()]
        for pack in range(count):
            rows = slice(pack * SLOTS * GROUP, (pack * SLOTS + slots) * GROUP)
            for part in range(2):
                coeff[part, rows, :] = share_dot(coeff[part, rows, :], share[...]) * inverse[pack]
        for pack in range(count):

            def backward(index, inner):
                yr = [jnp.zeros((GROUP, 128), jnp.float32) for _ in range(8)]
                yi = [jnp.zeros((GROUP, 128), jnp.float32) for _ in range(8)]
                for slot in range(slots):
                    at = (pack * SLOTS + slot) * GROUP
                    pr = coeff[0, at : at + GROUP, :]
                    pi = coeff[1, at : at + GROUP, :]
                    for two in range(4):
                        re, im = tile(pack, slot, index * 4 + two)
                        yr[two] = yr[two] + re * pr
                        yr[4 + two] = yr[4 + two] - im * pi
                        yi[two] = yi[two] + re * pi
                        yi[4 + two] = yi[4 + two] + im * pr
                for two in range(4):
                    at = pl.ds(pack * FEED_SETS + index * 4 + two, 1)
                    y[0, at, :] = jnp.sum(yr[two] + yr[4 + two], axis=0, keepdims=True)
                    y[1, at, :] = jnp.sum(yi[two] + yi[4 + two], axis=0, keepdims=True)
                return inner

            lax.fori_loop(0, FEED_SETS // 4, backward, 0)
        for pack in range(count):
            here = slice(pack * FEED_SETS, (pack + 1) * FEED_SETS)
            w = weight[own_rows(first + pack), :]
            scaled = w * (diag[here, :] * (w * inverse[pack]))
            total = jnp.zeros((8, 128), jnp.float32)
            for part in range(2):
                value = w * whole(y[part, here, :]) + scaled * x[part, here, :]
                x[part, here, :] = value
                for row in range(0, FEED_SETS, 8):
                    total = total + value[row : row + 8] * value[row : row + 8]
            total = jnp.sum(total, axis=0, keepdims=True)
            squares[8 * pack : 8 * pack + 8, :] = jnp.broadcast_to(total, (8, 128))

        @pl.when(iteration < ITERS - 1)
        def _():
            forward_pass(tile, count, x, coeff, slots)

        return carry

    lax.fori_loop(0, ITERS, iterate, 0)
    for pack, length in enumerate(lengths()):
        here = slice(pack * FEED_SETS, (pack + 1) * FEED_SETS)
        for part in range(2):
            x[part, here, :] = x[part, here, :] / jnp.sqrt(length)


def kernel(
    volt, taps, twiddle, fine_upper, fine_lower, usable, auto_power, share, repeat, out,
    weight, power, lined, lined_back, wide, sent_half, held_half, kept, ext, halfway, upper, lower, stage, sent_pair, sent_one, held_pair, held_one,
    x, y, coeff, squares, diag, loads, send_sems, recv_sems, edge_sems,
):
    def arrange(source, target, split):
        feeds = FEED_SETS * FEEDS_HERE
        lane = lax.broadcasted_iota(jnp.int32, (FEED_SETS, feeds), 1)
        first = lax.broadcasted_iota(jnp.int32, (FEED_SETS, feeds), 0) * FEEDS_HERE
        mine = (lane >= first) & (lane < first + FEEDS_HERE)
        place = lax.broadcasted_iota(jnp.int32, (FEED_SETS, 128), 1)

        def body(pack, carry):
            for q in range(8):
                row = source[pl.ds(pack * 8 + q, 1), :].astype(jnp.float32)
                lined[q * FEED_SETS : (q + 1) * FEED_SETS, :] = jnp.where(mine, row, 0.0)
            value = lined[...]
            high = value.astype(jnp.bfloat16)
            wide = jnp.dot(high, repeat[...], preferred_element_type=jnp.float32)
            if split:
                rest = value - high.astype(jnp.float32)
                middle = rest.astype(jnp.bfloat16)
                low = (rest - middle.astype(jnp.float32)).astype(jnp.bfloat16)
                wide = wide + jnp.dot(middle, repeat[...], preferred_element_type=jnp.float32)
                wide = wide + jnp.dot(low, repeat[...], preferred_element_type=jnp.float32)
            total = jnp.zeros((FEED_SETS, 128), jnp.float32)
            for q in range(8):
                part = wide[q * FEED_SETS : (q + 1) * FEED_SETS]
                own = (place >= q * FEEDS_HERE) & (place < (q + 1) * FEEDS_HERE)
                total = total + jnp.where(own, part, 0.0)
            target[pl.ds(pl.multiple_of(pack * FEED_SETS, FEED_SETS), FEED_SETS), :] = total
            return carry

        lax.fori_loop(0, PACKS, body, 0)

    def arrange_back(pack, rows):
        feeds = FEED_SETS * FEEDS_HERE
        lane = lax.broadcasted_iota(jnp.int32, (FEED_SETS, feeds), 1)
        first = lax.broadcasted_iota(jnp.int32, (FEED_SETS, feeds), 0) * FEEDS_HERE
        mine = (lane >= first) & (lane < first + FEEDS_HERE)
        place = lax.broadcasted_iota(jnp.int32, (FEED_SETS, 128), 1)
        dims = (((1,), (1,)), ((), ()))
        for part in range(2):
            value = x[part, rows, :]
            for q in range(8):
                own = (place >= q * FEEDS_HERE) & (place < (q + 1) * FEEDS_HERE)
                lined_back[q * FEED_SETS : (q + 1) * FEED_SETS, :] = jnp.where(own, value, 0.0)
            rest = lined_back[...]
            total = jnp.zeros((8 * FEED_SETS, feeds), jnp.float32)
            for _ in range(2):
                piece = rest.astype(jnp.bfloat16)
                rest = rest - piece.astype(jnp.float32)
                total = total + lax.dot_general(
                    piece, repeat[...], dims, preferred_element_type=jnp.float32
                )
            for q in range(8):
                line = jnp.where(mine, total[q * FEED_SETS : (q + 1) * FEED_SETS], 0.0)
                out[part, pl.ds(pack * 8 + q, 1), :] = jnp.sum(line, axis=0, keepdims=True)

    section = lax.axis_index("section")
    chan = lax.axis_index("chan")
    core = lax.rem(chan, 2)
    before = 2 - core
    me = section * FEED_SETS + chan
    load = pltpu.make_async_copy(
        volt, ext.at[:, :, pl.ds(pl.multiple_of(before * CHANNELS, CHANNELS), LENGTH)], loads
    )
    load.start()
    barrier = pltpu.get_barrier_semaphore()

    def greet(there, column):
        pl.semaphore_signal(
            barrier, inc=1, device_id=(there, column), device_id_type=pl.DeviceIdType.MESH
        )

    visit(section, chan, greet)
    edges = []
    for kind in range(2):
        early, late = (2 - kind) * CHANNELS, (1 + kind) * CHANNELS
        pair = (edge_sems, edge_sems.at[pl.ds(2, 2)])
        edges.append((
            copy_at(
                volt.at[:, :, pl.ds(LENGTH - early, early)],
                ext.at[:, :, pl.ds(0, early)],
                pair,
                0,
                (lax.rem(section + 1, SECTIONS), chan),
            ),
            copy_at(
                volt.at[:, :, pl.ds(0, late)],
                ext.at[:, :, pl.ds(early + LENGTH, late)],
                pair,
                1,
                (lax.rem(section + SECTIONS - 1, SECTIONS), chan),
            ),
        ))
    pl.semaphore_wait(barrier, OWNERS - 1)
    for kind in range(2):

        @pl.when(core == kind)
        def _():
            edges[kind][0].start()
            edges[kind][1].start()

    load.wait()

    def clear(first, count):
        def body(at, inner):
            where = pl.ds(pl.multiple_of(first * CHANNELS + at * FINE, FINE), FINE)
            for part in range(2):
                ext[part, :, where] = jnp.zeros((FEEDS_HERE, FINE), jnp.bfloat16)
            return inner

        lax.fori_loop(0, count * COARSE, body, 0)

    def grouped(position, carry):
        group = lax.rem(position + 1, GROUPS)

        for kind in range(2):

            @pl.when((position == 2) & (core == kind))
            def _():
                edges[kind][1].wait()

            @pl.when((position == 3) & (core == kind))
            def _():
                edges[kind][0].wait()

        @pl.when((position == 3) & (section == 0))
        def _():
            clear(0, before)

        def step(at, inner):
            @pl.when((section == SECTIONS - 1) & (position == 2) & (at == GROUP - 1))
            def _():
                clear(BLOCKS_HERE - HALO + before, HALO)

            block = lax.rem(group * GROUP + at + core * (BLOCKS_HERE - 1), BLOCKS_HERE)
            first_transform(block, ext, taps, halfway)
            second_transform(twiddle, halfway, upper, lower)
            fine_transform(at, fine_upper, fine_lower, upper, lower, stage)
            return inner

        lax.fori_loop(0, GROUP, step, 0)

        def emit(owner, inner):
            rows = pl.ds(owner * STRIDE, 16)
            for pack in range(2):
                sent_pair[owner, group, pack] = stage[pack, rows, :].astype(jnp.bfloat16)
                sent_one[pack, owner, group] = stage[2 + pack, rows, :].astype(jnp.bfloat16)
            return inner

        lax.fori_loop(0, OWNERS, emit, 0, unroll=8)

        def send(there, column):
            pltpu.make_async_remote_copy(
                src_ref=sent_pair.at[there * FEED_SETS + column, group],
                dst_ref=held_pair.at[me, group],
                send_sem=send_sems.at[0],
                recv_sem=recv_sems.at[group],
                device_id=(there, column),
                device_id_type=pl.DeviceIdType.MESH,
            ).start()

        visit(section, chan, send)
        return carry

    lax.fori_loop(0, GROUPS, grouped, 0)

    def send_third(there, column):
        pltpu.make_async_remote_copy(
            src_ref=sent_one.at[0, there * FEED_SETS + column],
            dst_ref=held_one.at[0, me],
            send_sem=send_sems.at[1],
            recv_sem=recv_sems.at[2 * GROUPS],
            device_id=(there, column),
            device_id_type=pl.DeviceIdType.MESH,
        ).start()

    visit(section, chan, send_third)

    def low_lanes(shape):
        return lax.broadcasted_iota(jnp.int32, shape, 1) < 64

    def repack(owner, carry):
        low = low_lanes((16, 128))
        for pair in range(GROUPS // 2):
            one, two = [
                sent_one[1, owner, 2 * pair + at].astype(jnp.float32) for at in range(2)
            ]
            first = jnp.where(low, one, pltpu.roll(two, 64, 1))
            second = jnp.where(low, pltpu.roll(one, 64, 1), two)
            sent_half[0, owner, pair] = first.astype(jnp.bfloat16)
            sent_half[1, owner, pair] = second.astype(jnp.bfloat16)
        return carry

    lax.fori_loop(0, OWNERS, repack, 0, unroll=4)

    def rest(index, carry):
        half, pair = lax.div(index, 2), lax.rem(index, 2)

        def send(there, column):
            pltpu.make_async_remote_copy(
                src_ref=sent_half.at[half, there * FEED_SETS + column, pair],
                dst_ref=held_half.at[half, me, pair],
                send_sem=send_sems.at[2],
                recv_sem=recv_sems.at[GROUPS + index],
                device_id=(there, column),
                device_id_type=pl.DeviceIdType.MESH,
            ).start()

        visit(section, chan, send)
        return carry

    lax.fori_loop(0, 4, rest, 0)
    arrange(usable, weight, False)
    arrange(auto_power, power, True)
    for ref in (weight, power):
        value = ref[own_rows(3), :]
        other = pltpu.roll(value, 64, 1)
        low = low_lanes((FEED_SETS, 128))
        ref[own_rows(4), :] = jnp.where(low, value, other)
        ref[own_rows(5), :] = jnp.where(low, other, value)

    for group in range(GROUPS):
        for pack in range(2):
            held_pair[me, group, pack] = sent_pair[me, group, pack]
            held_half[pack, me, group // 2] = sent_half[pack, me, group // 2]
        held_one[0, me, group] = sent_one[0, me, group]

    others = pl.ds(0, OWNERS - 1)
    scratch = (weight, power, share, x, y, coeff, squares, diag)
    top_row = lax.broadcasted_iota(jnp.int32, (GROUP, 128), 0) == 0

    def tile(pack, slot, feed_set):
        at = (pack * SLOTS + slot) * FEED_SETS + feed_set
        return wide[at, 0], wide[at, 1]

    def begin(first, count):
        start_x(first, count, weight, x)
        diag[0 : count * FEED_SETS, :] = jnp.zeros((count * FEED_SETS, 128), jnp.float32)

    def take(read, group, count, mend, per=GROUPS):
        def arrive(index, sums):
            sums = list(sums)
            for pack in range(count):
                for near in range(2):
                    feed_set = index * 2 + near
                    row = pl.ds(pack * FEED_SETS + feed_set, 1)
                    weight_row = x[0, row, :]
                    values = []
                    for at in range(SECTIONS):
                        value = read(at * FEED_SETS + feed_set, pack).astype(jnp.float32)
                        values.append((value[0:GROUP], value[GROUP:]))
                    if group == 0 and near == 1:
                        values = [
                            tuple(jnp.where(mend, values[at - 1][c], values[at][c]) for c in range(2))
                            for at in range(SECTIONS)
                        ]
                    total = jnp.zeros((GROUP, 128), jnp.float32)
                    for at, (re, im) in enumerate(values):
                        place = (pack * SLOTS + at * per + group) * FEED_SETS + feed_set
                        wide[place, 0] = re
                        wide[place, 1] = im
                        total = total + (re * re + im * im)
                        own = 2 * (pack * SECTIONS + at)
                        sums[own] = sums[own] + re * weight_row
                        sums[own + 1] = sums[own + 1] - im * weight_row
                    diag[row, :] = diag[row, :] + jnp.sum(total, axis=0, keepdims=True)
            return tuple(sums)

        zero = jnp.zeros((GROUP, 128), jnp.float32)
        sums = lax.fori_loop(0, FEED_SETS // 2, arrive, (zero,) * (2 * SECTIONS * count))
        for pack in range(count):
            for at in range(SECTIONS):
                slot = pack * SLOTS + at * per + group
                own = 2 * (pack * SECTIONS + at)
                for part in range(2):
                    coeff[part, slot * GROUP : (slot + 1) * GROUP, :] = sums[own + part]

    begin(0, 2)
    for group in (1, 2, 3, 0):
        pltpu.make_async_copy(
            sent_pair.at[others, group], held_pair.at[others, group], recv_sems.at[group]
        ).wait()
        take(lambda source, pack: held_pair[source, group, pack], group, 2, top_row)
    solve_packs(tile, 0, 2, *scratch)
    for pack in range(2):
        arrange_back(pack, slice(pack * FEED_SETS, (pack + 1) * FEED_SETS))

    begin(2, 1)
    pltpu.make_async_copy(
        sent_one.at[0, others], held_one.at[0, others], recv_sems.at[2 * GROUPS]
    ).wait()
    for group in range(GROUPS):
        take(lambda source, pack: held_one[0, source, group], group, 1, top_row)
    solve_packs(tile, 2, 1, *scratch)
    arrange_back(2, slice(0, FEED_SETS))

    for half in range(2):
        begin(4 + half, 1)
        for pair in range(2):
            pltpu.make_async_copy(
                sent_half.at[half, others, pair],
                held_half.at[half, others, pair],
                recv_sems.at[GROUPS + 2 * half + pair],
            ).wait()
            low = top_row & low_lanes((GROUP, 128))
            take(lambda source, pack: held_half[half, source, pair], pair, 1, low, GROUPS // 2)
        solve_packs(tile, 4 + half, 1, *scratch, slots=SLOTS // 2)
        own = slice(0, FEED_SETS)
        for part in range(2):
            if half == 0:
                kept[part] = x[part, own, :]
            else:
                x[part, own, :] = jnp.where(low_lanes((FEED_SETS, 128)), kept[part], x[part, own, :])
    arrange_back(3, slice(0, FEED_SETS))
    pltpu.make_async_copy(sent_pair.at[others], held_pair.at[others], send_sems.at[0]).wait()
    for pack in range(2):
        pltpu.make_async_copy(
            sent_one.at[pack, others], held_one.at[pack, others], send_sems.at[1 + pack]
        ).wait()


def local(voltages, usable, auto_power):
    taps, twiddle, fine, share = tables()
    upper = fine.astype(jnp.bfloat16)
    lower = (fine - upper.astype(np.float32)).astype(jnp.bfloat16)
    rows = PACKS * FEED_SETS

    lane = np.arange(FEED_SETS * FEEDS_HERE)[:, None] % FEEDS_HERE
    repeat = (lane == np.arange(128)[None, :] % FEEDS_HERE).astype(jnp.bfloat16)
    vmem = pl.BlockSpec(memory_space=pltpu.VMEM)
    pair = pltpu.VMEM((OWNERS, GROUPS, 2, 16, 128), jnp.bfloat16)
    half = pltpu.VMEM((2, OWNERS, GROUPS // 2, 16, 128), jnp.bfloat16)
    one = pltpu.VMEM((2, OWNERS, GROUPS, 16, 128), jnp.bfloat16)
    return pl.pallas_call(
        kernel,
        out_shape=jax.ShapeDtypeStruct((2, PACKS * 8, FEED_SETS * FEEDS_HERE), jnp.float32),
        in_specs=[pl.BlockSpec(memory_space=pl.ANY)] + [vmem] * 8,
        out_specs=vmem,
        scratch_shapes=[
            pltpu.VMEM((rows + 2 * FEED_SETS, 128), jnp.float32),
            pltpu.VMEM((rows + 2 * FEED_SETS, 128), jnp.float32),
            pltpu.VMEM((8 * FEED_SETS, FEED_SETS * FEEDS_HERE), jnp.float32),
            pltpu.VMEM((8 * FEED_SETS, 128), jnp.float32),
            pltpu.VMEM((2 * SLOTS * FEED_SETS, 2, GROUP, 128), jnp.float32),
            half,
            half,
            pltpu.VMEM((2, FEED_SETS, 128), jnp.float32),
            pltpu.VMEM((2, FEEDS_HERE, LENGTH + HALO * CHANNELS), jnp.bfloat16),
            pltpu.VMEM((4, 8, 2, FEEDS_HERE, FINE), jnp.float32),
            pltpu.VMEM((COARSE * FEEDS_HERE, 256), jnp.bfloat16),
            pltpu.VMEM((COARSE * FEEDS_HERE, 256), jnp.bfloat16),
            pltpu.VMEM((PACKS, OWNERS * STRIDE + 8, 128), jnp.float32),
            pair,
            one,
            pair,
            one,
            pltpu.VMEM((2, 2 * FEED_SETS, 128), jnp.float32),
            pltpu.VMEM((2, 2 * FEED_SETS, 128), jnp.float32),
            pltpu.VMEM((2, 2 * SLOTS * GROUP, 128), jnp.float32),
            pltpu.VMEM((16, 128), jnp.float32),
            pltpu.VMEM((2 * FEED_SETS, 128), jnp.float32),
            pltpu.SemaphoreType.DMA,
            pltpu.SemaphoreType.DMA((3,)),
            pltpu.SemaphoreType.DMA((1 + 2 * GROUPS,)),
            pltpu.SemaphoreType.DMA((4,)),
        ],
        compiler_params=pltpu.CompilerParams(
            collective_id=0, has_side_effects=True, vmem_limit_bytes=56 * 1024 * 1024
        ),
        cost_estimate=pl.CostEstimate(flops=10**10, bytes_accessed=2 * 10**7, transcendentals=0),
    )(
        voltages, taps, twiddle, upper, lower,
        usable, auto_power, share.astype(jnp.bfloat16), repeat,
    )


def solution(mesh):
    in_specs = (
        P(None, "chan", "section"),
        P(("section", "chan"), None),
        P(("section", "chan"), None),
    )
    out_specs = P(None, ("section", "chan"), None)
    return jax.shard_map(local, mesh=mesh, in_specs=in_specs, out_specs=out_specs, check_vma=False)
```
